512 devices in a mesh: period: 2 (over y), gx: 16 (over z), gy: 8 (over x), gz: 2 (over core).
Axes of the slice: x: 8, y: 2, z: 16, core: 2. Of those that a mesh axis runs over, the one named last changes fastest.
The devices are a block of a 8x8x16 slice.
Arguments:
- residual: float32 [4, 3, 64, 64, 256], P('period', None, 'gx', 'gy', 'gz'), parts along dimension 0, may hold values from -6 to 6
- classes: int32 [64, 64, 256], P('gx', 'gy', 'gz'), may hold values from 0 to 15
- edge_mask: int32 [3, 64, 64, 256], P(None, 'gx', 'gy', 'gz'), may hold values from 0 to 1
- class_weight: float32 [32], P('period'), parts along dimension 0, may hold values from 0.01 to 1
Outputs:
- preconditioned: float32 [4, 3, 64, 64, 256], P('period', None, 'gx', 'gy', 'gz'), parts along dimension 0
The draws below stay inside these ranges and needn't reach their ends.
There are 2 independent parts, one for each index of `period`. The reference program is written for one: setup_inputs(seed, part) draws one part's arguments, and reference() takes and returns one part's arrays. A program takes and returns all parts, laid end to end along the dimension named above; an argument that names none is the same for every part. Nothing has to cross between parts.
All inputs are finite; a program needn't handle non-finite values.
Results may differ from the reference program's by a relative error of at most 0.00025.
Values sent between devices are 32-bit elements; how exact they have to be, the bound alone decides.
No kernel may reach another device: no remote copies, remote signals or barrier semaphores. Data moves between devices by JAX's collectives and lax.ppermute only.
A program may use at most 64 MiB of HBM per device.

```python
import math
import jax
import jax.numpy as jnp
from jax import lax

COARSE_SWEEPS = 2
NCLASS = 16
NX = 64
NY = 64
NZ = 256


def draw_edge_mask(key, part):
    base_key, row_key, depth_key, row_pick, depth_pick = jax.random.split(jax.random.fold_in(key, 11), 5)
    scattered = (jax.random.randint(base_key, (3, NX, NY, NZ), 0, 16) == 0).astype(jnp.int32)
    row_blocks = (jax.random.randint(row_key, (NY // 4,), 0, 4) == 0).astype(jnp.int32)
    row_forced = (jnp.arange(NY // 4, dtype=jnp.int32) == jax.random.randint(row_pick, (), 0, NY // 4)).astype(jnp.int32)
    row_quiet = jnp.repeat(jnp.maximum(row_blocks, row_forced), 4)
    depth_blocks = (jax.random.randint(depth_key, (NZ // 4,), 0, 4) == 0).astype(jnp.int32)
    depth_forced = (jnp.arange(NZ // 4, dtype=jnp.int32) == jax.random.randint(depth_pick, (), 0, NZ // 4)).astype(jnp.int32)
    depth_quiet = jnp.repeat(jnp.maximum(depth_blocks, depth_forced), 4)
    quiet_cells = row_quiet[:, None] * depth_quiet[None, :]
    along_edges = scattered[0] * (1 - quiet_cells)[None]
    across_edges = jnp.maximum(scattered[1:], quiet_cells[None, None])
    return jnp.concatenate([along_edges[None], across_edges], axis=0)


def set_ends(values, key, low, top_value):
    longest = values.shape.index(max(values.shape))
    spots = []
    for shift in (0, 1):
        where = [jax.random.randint(jax.random.fold_in(key, axis), (), 0, length) for axis, length in enumerate(values.shape)]
        where[longest] = (where[longest] + shift) % values.shape[longest]
        spots.append(tuple(where))
    return values.at[spots[0]].set(low).at[spots[1]].set(top_value)


def block_levels(stream_key, extent, pieces, smallest, top_value):
    level, own = 1.0, jax.random.fold_in(stream_key, 6)
    for position, blocks in pieces:
        heights = jnp.exp(jax.random.uniform(jax.random.fold_in(own, position), (blocks,), jnp.float32, smallest / len(pieces), top_value / len(pieces)))
        level = level * jnp.repeat(heights, extent[position] // blocks).reshape([-1 if axis == position else 1 for axis in range(len(extent))])
    return level


def bell_draw(stream_key, shape, deviation, bound, cuts=(), held_as=jnp.bfloat16):
    gain = block_levels(stream_key, shape, cuts, -0.22, 0.18) if cuts else 1.0
    values = jax.random.normal(stream_key, shape, jnp.float32) * deviation * gain
    return jnp.minimum(jnp.maximum(values, -bound), bound).astype(held_as)


def setup_inputs(seed: int = 0, part: int = 0) -> dict:
    splits = jax.random.split(jax.random.key(seed), 5)
    own_keys = jax.random.split(jax.random.fold_in(splits[4], part), 5)
    residual = bell_draw(own_keys[0], (2, 3, NX, NY, NZ), 1.0, 6.0, ((2, 16), (3, 8), (4, 2)), jnp.float32)
    classes = set_ends(jax.random.randint(splits[1], (NX, NY, NZ), 0, NCLASS), jax.random.fold_in(splits[1], 1), 0, NCLASS - 1).astype(jnp.int32)
    edge_mask = draw_edge_mask(jax.random.fold_in(splits[4], 71), part)
    class_weight = jnp.clip(jnp.exp(jax.random.uniform(own_keys[3], (NCLASS,), jnp.float32, math.log(0.01), math.log(1.0))), 0.01, 1.0)
    return dict(residual=residual, classes=classes, edge_mask=edge_mask, class_weight=class_weight)


aspect = 2.0
face_weight = (1.0 / (aspect * aspect), 1.0, 1.0)
mass_factor = (aspect * aspect, 1.0, 1.0)
stiff_weight = (2.0 * (face_weight[1] + face_weight[2]), 2.0 * (face_weight[0] + face_weight[2]), 2.0 * (face_weight[0] + face_weight[1]))
edge_damping = 0.6
shift_ratio = 1.0e-4
shift_added = 0.05
coarse_along = 0.5625
coarse_across = 0.1875


def shifted(values, axis_index, offset):
    axis_index = axis_index % values.ndim
    length = values.shape[axis_index]
    widths = [(0, 0)] * values.ndim
    if offset > 0:
        widths[axis_index] = (0, 1)
        return lax.slice_in_dim(jnp.pad(values, widths), 1, length + 1, axis=axis_index)
    widths[axis_index] = (1, 0)
    return lax.slice_in_dim(jnp.pad(values, widths), 0, length, axis=axis_index)


def spread(per_kind):
    scalar_kind = per_kind[0:1]
    vector_kind = per_kind[1:2]
    return jnp.concatenate([scalar_kind, vector_kind, vector_kind, vector_kind], axis=0)


def edge_coefficients(cell_values, free_edges):
    cells_west = shifted(cell_values, 0, -1)
    cells_south = shifted(cell_values, 1, -1)
    cells_above = shifted(cell_values, 2, -1)
    first_edges = 0.25 * (((cell_values + cells_south) + cells_above) + shifted(cells_above, 1, -1))
    second_edges = 0.25 * (((cell_values + cells_west) + cells_above) + shifted(cells_above, 0, -1))
    third_edges = 0.25 * (((cell_values + cells_west) + cells_south) + shifted(cells_south, 0, -1))
    averages = jnp.stack([first_edges, second_edges, third_edges])
    factors = jnp.array(mass_factor, jnp.float32).reshape(3, 1, 1, 1)
    stiffness = jnp.array(stiff_weight, jnp.float32).reshape(3, 1, 1, 1)
    masses = factors * averages * free_edges
    edge_diagonal = stiffness + masses
    kind_weights = jnp.stack([masses, edge_diagonal * free_edges])
    return masses, edge_diagonal, kind_weights


def make_level(kind_weights):
    to_east = kind_weights[:, 0]
    to_north = kind_weights[:, 1]
    to_deep = kind_weights[:, 2]
    to_west = shifted(to_east, -3, -1)
    to_south = shifted(to_north, -2, -1)
    to_shallow = shifted(to_deep, -1, -1)
    weight_sum = ((((to_east + to_west) + to_north) + to_south) + to_deep) + to_shallow
    return (to_east, to_north, to_deep, to_west, to_south, to_shallow, (1.0 + shift_ratio) * weight_sum + shift_added)


def coarse_weights(kind_weights):
    grouped = kind_weights.reshape(kind_weights.shape[:3] + (kind_weights.shape[3] // 2, 2, kind_weights.shape[4] // 2, 2))
    summed = (grouped[:, :, :, :, 0, :, 0] + grouped[:, :, :, :, 1, :, 0]) + (grouped[:, :, :, :, 0, :, 1] + grouped[:, :, :, :, 1, :, 1])
    factors = jnp.array([coarse_along, coarse_across, coarse_across], jnp.float32).reshape(1, 3, 1, 1, 1)
    return summed * factors


def pad_space(values):
    return jnp.pad(values, ((0, 0), (0, 0), (1, 1), (1, 1), (1, 1)))


def curl_apply(padded, masses):
    extent_east = padded.shape[2] - 2
    extent_north = padded.shape[3] - 2
    extent_deep = padded.shape[4] - 2

    def region(values, move_east, move_north, move_deep, extra_cells):
        return values[:, move_east:move_east + extent_east + extra_cells, move_north:move_north + extent_north + extra_cells, move_deep:move_deep + extent_deep + extra_cells]

    field_east = padded[:, 0]
    field_north = padded[:, 1]
    field_deep = padded[:, 2]
    flux_east = face_weight[0] * ((region(field_deep, 0, 1, 0, 1) - region(field_deep, 0, 0, 0, 1)) - (region(field_north, 0, 0, 1, 1) - region(field_north, 0, 0, 0, 1)))
    flux_north = face_weight[1] * ((region(field_east, 0, 0, 1, 1) - region(field_east, 0, 0, 0, 1)) - (region(field_deep, 1, 0, 0, 1) - region(field_deep, 0, 0, 0, 1)))
    flux_deep = face_weight[2] * ((region(field_north, 1, 0, 0, 1) - region(field_north, 0, 0, 0, 1)) - (region(field_east, 0, 1, 0, 1) - region(field_east, 0, 0, 0, 1)))
    out_east = ((region(flux_north, 1, 1, 0, 0) - region(flux_north, 1, 1, 1, 0)) - (region(flux_deep, 1, 0, 1, 0) - region(flux_deep, 1, 1, 1, 0))) + masses[0] * region(field_east, 1, 1, 1, 0)
    out_north = ((region(flux_deep, 0, 1, 1, 0) - region(flux_deep, 1, 1, 1, 0)) - (region(flux_east, 1, 1, 0, 0) - region(flux_east, 1, 1, 1, 0))) + masses[1] * region(field_north, 1, 1, 1, 0)
    out_deep = ((region(flux_east, 1, 0, 1, 0) - region(flux_east, 1, 1, 1, 0)) - (region(flux_north, 0, 1, 1, 0) - region(flux_north, 1, 1, 1, 0))) + masses[2] * region(field_deep, 1, 1, 1, 0)
    return jnp.stack([out_east, out_north, out_deep], axis=1)


def side_padded(plane_pad, grid_level):
    return ((spread(grid_level[1]) * plane_pad[..., 2:, 1:-1] + spread(grid_level[4]) * plane_pad[..., :-2, 1:-1]) + spread(grid_level[2]) * plane_pad[..., 1:-1, 2:]) + spread(grid_level[5]) * plane_pad[..., 1:-1, :-2]


def apply_padded(padded, grid_level):
    center = padded[:, :, 1:-1, 1:-1, 1:-1]
    along_line = spread(grid_level[0]) * padded[:, :, 2:, 1:-1, 1:-1] + spread(grid_level[3]) * padded[:, :, :-2, 1:-1, 1:-1]
    return spread(grid_level[6]) * center - (along_line + side_padded(padded[:, :, 1:-1], grid_level))


def gradient_adjoint(padded):
    interior = padded[:, :, 1:-1, 1:-1, 1:-1]
    from_west = padded[:, 0, :-2, 1:-1, 1:-1]
    from_south = padded[:, 1, 1:-1, :-2, 1:-1]
    from_above = padded[:, 2, 1:-1, 1:-1, :-2]
    total_flow = ((from_west - interior[:, 0]) + (from_south - interior[:, 1])) + (from_above - interior[:, 2])
    return total_flow[:, None]


def average_adjoint(padded):
    interior = padded[:, :, 1:-1, 1:-1, 1:-1]
    return jnp.stack([0.5 * (interior[:, 0] + padded[:, 0, :-2, 1:-1, 1:-1]), 0.5 * (interior[:, 1] + padded[:, 1, 1:-1, :-2, 1:-1]), 0.5 * (interior[:, 2] + padded[:, 2, 1:-1, 1:-1, :-2])], axis=1)


def gradient_edges(padded):
    interior = padded[:, 0, 1:-1, 1:-1, 1:-1]
    return jnp.stack([padded[:, 0, 2:, 1:-1, 1:-1] - interior, padded[:, 0, 1:-1, 2:, 1:-1] - interior, padded[:, 0, 1:-1, 1:-1, 2:] - interior], axis=1)


def average_edges(padded):
    return jnp.stack([0.5 * (padded[:, 1, 1:-1, 1:-1, 1:-1] + padded[:, 1, 2:, 1:-1, 1:-1]), 0.5 * (padded[:, 2, 1:-1, 1:-1, 1:-1] + padded[:, 2, 1:-1, 2:, 1:-1]), 0.5 * (padded[:, 3, 1:-1, 1:-1, 1:-1] + padded[:, 3, 1:-1, 1:-1, 2:])], axis=1)


def restrict_plane(padded):
    extent_north = padded.shape[3] - 2
    extent_deep = padded.shape[4] - 2
    halved = padded[:, :, :, 1:extent_north + 1:2] + 0.5 * (padded[:, :, :, 0:extent_north:2] + padded[:, :, :, 2:extent_north + 2:2])
    return halved[..., 1:extent_deep + 1:2] + 0.5 * (halved[..., 0:extent_deep:2] + halved[..., 2:extent_deep + 2:2])


def prolong_plane(padded):
    extent_north = padded.shape[3] - 2
    extent_deep = padded.shape[4] - 2
    even_rows = padded[:, :, :, 1:extent_north + 1]
    odd_rows = 0.5 * (even_rows + padded[:, :, :, 2:extent_north + 2])
    widened = jnp.stack([even_rows, odd_rows], axis=4)
    widened = widened.reshape(widened.shape[:3] + (2 * extent_north, extent_deep + 2))
    even_layers = widened[..., 1:extent_deep + 1]
    odd_layers = 0.5 * (even_layers + widened[..., 2:extent_deep + 2])
    joined = jnp.stack([even_layers, odd_layers], axis=5)
    return joined.reshape(joined.shape[:4] + (2 * extent_deep,))


def factor_lines(below_diagonal, main_diagonal, above_diagonal, entering):
    def forward(factor_before, row_items):
        below_row, main_row, above_row = row_items
        pivots = main_row - below_row * factor_before
        factor = above_row / pivots
        return factor, (pivots, factor)

    ignored, (pivot_rows, factor_rows) = lax.scan(forward, entering, (jnp.moveaxis(below_diagonal, 1, 0), jnp.moveaxis(main_diagonal, 1, 0), jnp.moveaxis(above_diagonal, 1, 0)))
    return jnp.moveaxis(pivot_rows, 0, 1), jnp.moveaxis(factor_rows, 0, 1)


def eliminate_rows(source, below_diagonal, pivots):
    def forward(earlier_row, row_items):
        below_row, pivot_row, source_row = row_items
        eliminated = (source_row - spread(below_row) * earlier_row) / spread(pivot_row)
        return eliminated, eliminated

    ignored, rows_out = lax.scan(forward, jnp.zeros(source[:, :, 0].shape, jnp.float32), (jnp.moveaxis(below_diagonal, 1, 0), jnp.moveaxis(pivots, 1, 0), jnp.moveaxis(source, 2, 0)))
    return jnp.moveaxis(rows_out, 0, 2)


def substitute_rows(eliminated, factors):
    def backward(next_value, row_items):
        factor_row, reduced_row = row_items
        solved = reduced_row - spread(factor_row) * next_value
        return solved, solved

    ignored, rows_out = lax.scan(backward, jnp.zeros(eliminated[:, :, 0].shape, jnp.float32), (jnp.moveaxis(factors, 1, 0), jnp.moveaxis(eliminated, 2, 0)), reverse=True)
    return jnp.moveaxis(rows_out, 0, 2)


def line_solve(source, grid_level):
    below_diagonal = -grid_level[3]
    pivots, factors = factor_lines(below_diagonal, grid_level[6], -grid_level[0], jnp.zeros(grid_level[6][:, 0].shape, jnp.float32))
    return substitute_rows(eliminate_rows(source, below_diagonal, pivots), factors)


def cycle_reference(nodal_source, fine_level, coarse_level):
    smoothed = line_solve(nodal_source, fine_level)
    residue = nodal_source - apply_padded(pad_space(smoothed), fine_level)
    coarse_source = restrict_plane(pad_space(residue)[:, :, 1:-1])
    correction = line_solve(coarse_source, coarse_level)
    for repeat in range(COARSE_SWEEPS - 1):
        correction = line_solve(coarse_source + side_padded(pad_space(correction)[:, :, 1:-1], coarse_level), coarse_level)
    smoothed = smoothed + prolong_plane(pad_space(correction)[:, :, 1:-1])
    return line_solve(nodal_source + side_padded(pad_space(smoothed)[:, :, 1:-1], fine_level), fine_level)


def reference(residual, classes, edge_mask, class_weight):
    cell_values = class_weight[classes]
    free_edges = (1 - edge_mask).astype(jnp.float32)
    masses, edge_diagonal, kind_weights = edge_coefficients(cell_values, free_edges)
    fine_level = make_level(kind_weights)
    coarse_level = make_level(coarse_weights(kind_weights))
    source = residual * free_edges
    first = edge_damping * source / edge_diagonal * free_edges
    remainder = source - curl_apply(pad_space(first), masses) * free_edges
    rimmed = pad_space(remainder)
    nodal_source = jnp.concatenate([gradient_adjoint(rimmed), average_adjoint(rimmed)], axis=1)
    potential = cycle_reference(nodal_source, fine_level, coarse_level)
    rimmed = pad_space(potential)
    second = first + (gradient_edges(rimmed) + average_edges(rimmed)) * free_edges
    remainder = source - curl_apply(pad_space(second), masses) * free_edges
    return second + edge_damping * remainder / edge_diagonal * free_edges
```

```python
import functools

import jax
import jax.numpy as jnp
from jax import lax
from jax.experimental import pallas as pl
from jax.experimental.pallas import tpu as pltpu
from jax.sharding import PartitionSpec as P

aspect = 2.0
face_weight = (1.0 / (aspect * aspect), 1.0, 1.0)
mass_factor = (aspect * aspect, 1.0, 1.0)
stiff_weight = (
    2.0 * (face_weight[1] + face_weight[2]),
    2.0 * (face_weight[0] + face_weight[2]),
    2.0 * (face_weight[0] + face_weight[1]),
)
edge_damping = 0.6
shift_ratio = 0.0001
shift_added = 0.05
coarse_scale = (0.5625, 0.1875, 0.1875)

f32 = jnp.float32
TILE = 8
ROWS = 3 * TILE
GROUPS = 4
DEPTH = 32


def lanes(shape):
    return lax.broadcasted_iota(jnp.int32, shape, 1)


def block_transpose(values, width):
    values = list(values)
    count = len(values)
    group = lanes(values[0].shape) // width
    bit = 1
    while bit < count:
        clear = (group & bit) == 0
        for low in range(count):
            if low & bit:
                continue
            high = low | bit
            first, second = values[low], values[high]
            values[low] = jnp.where(clear, first, pltpu.roll(second, bit * width, 1))
            values[high] = jnp.where(clear, pltpu.roll(first, 128 - bit * width, 1), second)
        bit *= 2
    return values


def loop(count, body, carry, unroll=1, reverse=False):
    def step(turn, state):
        for part in range(unroll):
            index = turn * unroll + part
            state = body(count - 1 - index if reverse else index, state)
        return state

    return lax.fori_loop(0, count // unroll, step, carry)


def y_next(v, by=1):
    return pltpu.roll(v, v.shape[0] - by, 0)


def y_back(v, by=1):
    return pltpu.roll(v, by, 0)


def z_next(v, by=1):
    return pltpu.roll(v, 128 - by, 1)


def z_back(v, by=1):
    return pltpu.roll(v, by, 1)


def pack_body(residual, classes, edge_mask, class_weight, out):
    thick = classes.shape[0]
    slots = []
    for part in range(2):
        for comp in range(3):
            slots += [residual[part, comp, i] for i in range(thick)]
    for i in range(thick):
        labels = classes[i]
        cells = jnp.zeros(labels.shape, f32)
        for label in range(class_weight.shape[0]):
            cells = jnp.where(labels == label, class_weight[label], cells)
        slots.append(cells)
    for comp in range(3):
        slots += [(1 - edge_mask[comp, i]).astype(f32) for i in range(thick)]
    zero = jnp.zeros((TILE, 128), f32)
    while len(slots) % 16:
        slots.append(zero)
    for part in range(len(slots) // 16):
        moved = block_transpose(slots[16 * part : 16 * part + 16], TILE)
        for target in range(16):
            out[target, TILE * part : TILE * part + TILE, :] = moved[target]


def unpack_body(packed, out):
    zero = jnp.zeros((TILE, 128), f32)
    for part in range(2):
        moved = block_transpose(
            [packed[source, TILE * part : TILE * part + TILE, :] for source in range(16)], TILE
        )
        for slot in range(16):
            field, i = divmod(16 * part + slot, 4)
            if field < 6:
                out[field // 3, field % 3, i] = moved[slot]


def line_body(
    place,
    middle,
    shallow,
    deep,
    out,
    W,
    E,
    M,
    Dm,
    Rm,
    KW,
    CW,
    FI,
    FB,
    FQ,
    CI,
    CB,
    CQ,
    NS,
    SM,
    CS,
    TY,
    OUT,
):
    extent_y, extent_z = place[2], place[3]
    shape = (ROWS, 128)
    lane = lanes(shape)
    row = lax.broadcasted_iota(jnp.int32, shape, 0)
    at_y = row + place[0]
    at_z = lane % DEPTH + place[1]
    inside = jnp.where(
        (at_y >= 0) & (at_y < extent_y) & (at_z >= 0) & (at_z < extent_z), 1.0, 0.0
    ).astype(f32)
    not_first = jnp.where(lane < DEPTH, 0.0, 1.0).astype(f32)
    not_last = jnp.where(lane >= 128 - DEPTH, 0.0, 1.0).astype(f32)
    even_row = row % 2 == 0
    even_lane = lane % 2 == 0

    def pad_low(ref, field):
        ref[field, 0] = pltpu.roll(ref[field, 16], DEPTH, 1) * not_first

    def pad_high(ref, field):
        ref[field, 17] = pltpu.roll(ref[field, 1], 128 - DEPTH, 1) * not_last

    zero8 = jnp.zeros((TILE, 128), f32)
    windows = (shallow, middle, deep)

    def spread_out(a, state):
        for y in range(3):
            for part in range(3):
                pieces = []
                for p in range(16):
                    g, t = divmod(p, 4)
                    if t == 3:
                        pieces.append(zero8)
                    else:
                        pieces.append(
                            windows[t][y * 16 + 4 * g + a, TILE * part : TILE * part + TILE, :]
                        )
                moved = block_transpose(pieces, TILE)
                for slot in range(16):
                    field, i = divmod(16 * part + slot, 4)
                    if field < 10:
                        W[field, 4 * a + i + 1, TILE * y : TILE * y + TILE, :] = moved[slot]
        return state

    loop(4, spread_out, 0)
    pad_low(W, 6)

    def coefficients(l, state):
        c = W[6, l + 1]
        cx = W[6, l]
        cy = y_back(c)
        cz = z_back(c)
        averages = (
            0.25 * (((c + cy) + cz) + z_back(cy)),
            0.25 * (((c + cx) + cz) + z_back(cx)),
            0.25 * (((c + cx) + cy) + y_back(cx)),
        )
        for d in range(3):
            free = W[7 + d, l + 1]
            masses = mass_factor[d] * averages[d] * free
            diagonal = stiff_weight[d] + masses
            damp = edge_damping * free / diagonal
            M[d, l] = masses
            Dm[d, l] = damp
            for part in range(2):
                source = W[3 * part + d, l + 1] * free
                W[3 * part + d, l + 1] = source
                E[3 * part + d, l + 1] = source * damp
            stiff = diagonal * free
            for g, values in enumerate(block_transpose([masses, stiff, stiff, stiff], DEPTH)):
                KW[d, 16 * g + l + 1] = values
        return state

    loop(16, coefficients, 0)

    for d in range(3):
        KW[d, 0] = jnp.zeros(shape, f32)

    def side_fluxes(part, l):
        e1, e2, e3 = (E[3 * part + d, l] for d in range(3))
        b2 = face_weight[1] * ((z_next(e1) - e1) - (E[3 * part + 2, l + 1] - e3))
        b3 = face_weight[2] * ((E[3 * part + 1, l + 1] - e2) - (y_next(e1) - e1))
        return b2, b3

    def curl(part, l, before):
        e1, e2, e3 = (E[3 * part + d, l] for d in range(3))
        b2, b3 = side_fluxes(part, l)
        b1 = face_weight[0] * ((y_next(e3) - e3) - (z_next(e2) - e2))
        b2_before, b3_before = before
        results = (
            (z_back(b2) - b2) - (y_back(b3) - b3) + M[0, l - 1] * e1,
            (b3_before - b3) - (z_back(b1) - b1) + M[1, l - 1] * e2,
            (y_back(b1) - b1) - (b2_before - b2) + M[2, l - 1] * e3,
        )
        return results, (b2, b3)

    for field in range(6):
        pad_low(E, field)
        pad_high(E, field)

    def first_remainder(l, state):
        after = []
        for part in range(2):
            results, fluxes = curl(part, l + 1, state[part])
            after.append(fluxes)
            for d in range(3):
                Rm[3 * part + d, l + 1] = (
                    W[3 * part + d, l + 1] - results[d] * W[7 + d, l + 1]
                )
        return tuple(after)

    loop(16, first_remainder, (side_fluxes(0, 0), side_fluxes(1, 0)))
    pad_low(Rm, 0)
    pad_low(Rm, 3)

    def to_nodes(l, state):
        for part in range(2):
            r1, r2, r3 = (Rm[3 * part + d, l + 1] for d in range(3))
            r1b = Rm[3 * part, l]
            r2b = y_back(r2)
            r3b = z_back(r3)
            members = [
                ((r1b - r1) + (r2b - r2)) + (r3b - r3),
                0.5 * (r1 + r1b),
                0.5 * (r2 + r2b),
                0.5 * (r3 + r3b),
            ]
            for g, values in enumerate(block_transpose(members, DEPTH)):
                NS[part, 16 * g + l] = values
        return state

    loop(16, to_nodes, 0)

    def factors(x, state):
        fine_before, coarse_before, cw1_before = state
        w1b, w1, w2, w3 = KW[0, x], KW[0, x + 1], KW[1, x + 1], KW[2, x + 1]
        total = ((((w1 + w1b) + w2) + y_back(w2)) + w3) + z_back(w3)
        pivot = ((1.0 + shift_ratio) * total + shift_added) - w1b * fine_before
        inverse = inside / pivot
        quotient = w1 * inverse
        FI[x] = inverse
        FB[x] = w1b * inverse
        FQ[x] = quotient
        cw = []
        for d, w in enumerate((w1, w2, w3)):
            pair = w + y_next(w)
            cw.append(coarse_scale[d] * (pair + z_next(pair)))
        CW[0, x] = cw[1]
        CW[1, x] = cw[2]
        total = ((((cw[0] + cw1_before) + cw[1]) + y_back(cw[1], 2)) + cw[2]) + z_back(cw[2], 2)
        pivot = ((1.0 + shift_ratio) * total + shift_added) - cw1_before * coarse_before
        inverse = inside / pivot
        coarse_quotient = cw[0] * inverse
        CI[x] = inverse
        CB[x] = cw1_before * inverse
        CQ[x] = coarse_quotient
        return quotient, coarse_quotient, cw[0]

    nothing = jnp.zeros(shape, f32)
    loop(64, factors, (nothing, nothing, nothing))

    def eliminate(source, inverse, back):
        def step(x, state):
            scale, couple = inverse[x], back[x]
            after = []
            for part in range(2):
                value = source[part, x] * scale + couple * state[part]
                TY[part, x] = value
                after.append(value)
            return tuple(after)

        loop(64, step, (nothing, nothing), unroll=4)

    def substitute(quotient, then):
        def step(x, state):
            factor = quotient[x]
            after = []
            for part in range(2):
                value = TY[part, x] + factor * state[part]
                after.append(value)
                then(part, x, value)
            return tuple(after)

        loop(64, step, (nothing, nothing), unroll=2, reverse=True)

    def sides(v, w2, w3, by):
        return ((w2 * y_next(v, by) + y_back(w2 * v, by)) + w3 * z_next(v, by)) + z_back(
            w3 * v, by
        )

    def after_smoothing(part, x, value):
        SM[part, x] = value
        residue = sides(value, KW[1, x + 1], KW[2, x + 1], 1)
        halved = residue + 0.5 * (y_back(residue) + y_next(residue))
        CS[part, x] = halved + 0.5 * (z_back(halved) + z_next(halved))

    def after_coarse(part, x, value):
        CS[part, x] = CS[part, x] + sides(value, CW[0, x], CW[1, x], 2)

    def after_correction(part, x, value):
        rows = jnp.where(even_row, value, 0.5 * (y_back(value) + y_next(value)))
        both = jnp.where(even_lane, rows, 0.5 * (z_back(rows) + z_next(rows)))
        smoothed = SM[part, x] + both
        CS[part, x] = NS[part, x] + sides(smoothed, KW[1, x + 1], KW[2, x + 1], 1)

    def after_potential(part, x, value):
        NS[part, x] = value

    eliminate(NS, FI, FB)
    substitute(FQ, after_smoothing)
    eliminate(CS, CI, CB)
    substitute(CQ, after_coarse)
    eliminate(CS, CI, CB)
    substitute(CQ, after_correction)
    eliminate(CS, FI, FB)
    substitute(FQ, after_potential)

    def from_nodes(l, state):
        for part in range(2):
            members = block_transpose([NS[part, 16 * g + l] for g in range(4)], DEPTH)
            p0, p1, p2, p3 = members
            Rm[3 * part, l + 1] = p0
            Rm[3 * part + 1, l + 1] = p1
            for d, (g_part, h_part) in (
                (1, (y_next(p0) - p0, 0.5 * (p2 + y_next(p2)))),
                (2, (z_next(p0) - p0, 0.5 * (p3 + z_next(p3)))),
            ):
                E[3 * part + d, l + 1] = (
                    E[3 * part + d, l + 1] + (g_part + h_part) * W[7 + d, l + 1]
                )
        return state

    loop(16, from_nodes, 0)
    for part in range(2):
        pad_high(Rm, 3 * part)
        pad_high(Rm, 3 * part + 1)

    def second_first(l, state):
        for part in range(2):
            p0, p1 = Rm[3 * part, l + 1], Rm[3 * part + 1, l + 1]
            g_part = Rm[3 * part, l + 2] - p0
            h_part = 0.5 * (p1 + Rm[3 * part + 1, l + 2])
            E[3 * part, l + 1] = E[3 * part, l + 1] + (g_part + h_part) * W[7, l + 1]
        return state

    loop(16, second_first, 0)
    for field in range(6):
        pad_low(E, field)
        pad_high(E, field)

    def last_step(l, state):
        after = []
        for part in range(2):
            results, fluxes = curl(part, l + 1, state[part])
            after.append(fluxes)
            for d in range(3):
                field = 3 * part + d
                remainder = W[field, l + 1] - results[d] * W[7 + d, l + 1]
                value = E[field, l + 1] + Dm[d, l] * remainder
                OUT[field, l] = value[TILE : 2 * TILE]
        return tuple(after)

    loop(16, last_step, (side_fluxes(0, 0), side_fluxes(1, 0)))

    def gather_up(a, state):
        for part in range(2):
            pieces = []
            for slot in range(16):
                field, i = divmod(16 * part + slot, 4)
                pieces.append(OUT[field, 4 * a + i] if field < 6 else zero8)
            moved = block_transpose(pieces, TILE)
            for g in range(4):
                out[4 * g + a, TILE * part : TILE * part + TILE, :] = moved[4 * g + 1]
        return state

    loop(4, gather_up, 0)


def vmem():
    return pl.BlockSpec(memory_space=pltpu.VMEM)


def smem():
    return pl.BlockSpec(memory_space=pltpu.SMEM)


def pack(residual, classes, edge_mask, class_weight, **options):
    return pl.pallas_call(
        pack_body,
        out_shape=jax.ShapeDtypeStruct((16, ROWS, 128), f32),
        in_specs=[vmem(), vmem(), vmem(), smem()],
        out_specs=vmem(),
        name="pack",
        **options,
    )(residual, classes, edge_mask, class_weight)


def unpack(packed, shape, **options):
    return pl.pallas_call(
        unpack_body,
        out_shape=jax.ShapeDtypeStruct(shape, f32),
        in_specs=[vmem()],
        out_specs=vmem(),
        name="unpack",
        **options,
    )(packed)


def lines(place, middle, shallow, deep, **options):
    edge = lambda count, levels: pltpu.VMEM((count, levels, ROWS, 128), f32)
    line = pltpu.VMEM((64, ROWS, 128), f32)
    pair = pltpu.VMEM((2, 64, ROWS, 128), f32)
    return pl.pallas_call(
        line_body,
        out_shape=jax.ShapeDtypeStruct((16, 2 * TILE, 128), f32),
        in_specs=[smem(), vmem(), vmem(), vmem()],
        out_specs=vmem(),
        scratch_shapes=[
            edge(10, 18),
            edge(6, 18),
            edge(3, 16),
            edge(3, 16),
            edge(6, 18),
            pltpu.VMEM((3, 65, ROWS, 128), f32),
            pair,
            line,
            line,
            line,
            line,
            line,
            line,
            pair,
            pair,
            pair,
            pair,
            pltpu.VMEM((6, 16, TILE, 128), f32),
        ],
        name="lines",
        **options,
    )(place, middle, shallow, deep)


def swap(values):
    return lax.all_to_all(values, "gx", 0, 0, tiled=True)


def per_device(residual, classes, edge_mask, class_weight):
    size_x, size_y, size_z = (lax.axis_size(name) for name in ("gx", "gy", "gz"))
    axes = ("gx", "gy", "gz")
    tiles = size_x * size_z

    def position(y, tile):
        z, x = divmod(tile, size_x)
        return (x * size_y + y) * size_z + z

    def from_side(values, step_y, step_tile):
        pairs = [
            (position(y, tile), position(y + step_y, tile + step_tile))
            for y in range(size_y)
            for tile in range(tiles)
            if 0 <= y + step_y < size_y and 0 <= tile + step_tile < tiles
        ]
        return lax.ppermute(values, axes, pairs)

    own = swap(
        pack(
            residual,
            classes,
            edge_mask,
            class_weight,
        )
    )
    middle = jnp.concatenate([from_side(own, 1, 0), own, from_side(own, -1, 0)], axis=0)
    shallow = from_side(middle, 0, 1)
    deep = from_side(middle, 0, -1)
    tile = lax.axis_index("gz") * size_x + lax.axis_index("gx")
    place = jnp.stack(
        [
            lax.axis_index("gy") * TILE - TILE,
            tile * TILE - TILE,
            jnp.int32(size_y * TILE),
            jnp.int32(tiles * TILE),
        ]
    ).astype(jnp.int32)
    options = dict(compiler_params=pltpu.CompilerParams(vmem_limit_bytes=50 * 2**20))
    result = swap(lines(place, middle, shallow, deep, **options))
    return unpack(result, residual.shape)


def solution(mesh):
    return jax.shard_map(
        per_device,
        mesh=mesh,
        in_specs=(
            P("period", None, "gx", "gy", "gz"),
            P("gx", "gy", "gz"),
            P(None, "gx", "gy", "gz"),
            P("period"),
        ),
        out_specs=P("period", None, "gx", "gy", "gz"),
        check_vma=False,
    )
```

```python
import functools

import jax
import jax.numpy as jnp
from jax import lax
from jax.experimental import pallas as pl
from jax.experimental.pallas import tpu as pltpu
from jax.sharding import PartitionSpec as P

aspect = 2.0
face_weight = (1.0 / (aspect * aspect), 1.0, 1.0)
mass_factor = (aspect * aspect, 1.0, 1.0)
stiff_weight = (
    2.0 * (face_weight[1] + face_weight[2]),
    2.0 * (face_weight[0] + face_weight[2]),
    2.0 * (face_weight[0] + face_weight[1]),
)
edge_damping = 0.6
shift_ratio = 0.0001
shift_added = 0.05
coarse_scale = (0.5625, 0.1875, 0.1875)

f32 = jnp.float32
TILE = 8
ROWS = 3 * TILE
GROUPS = 4
DEPTH = 32


def lanes(shape):
    return lax.broadcasted_iota(jnp.int32, shape, 1)


def turned(values):
    gap = jnp.zeros((DEPTH - ROWS, 128), f32)
    stacked = jnp.concatenate([piece for value in values for piece in (value, gap)], axis=0).T
    return [stacked[DEPTH * g : DEPTH * g + ROWS] for g in range(4)]


def loop(count, body, carry, unroll=1, reverse=False):
    def step(turn, state):
        for part in range(unroll):
            index = turn * unroll + part
            state = body(count - 1 - index if reverse else index, state)
        return state

    return lax.fori_loop(0, count // unroll, step, carry)


def y_next(v, by=1):
    return pltpu.roll(v, v.shape[0] - by, 0)


def y_back(v, by=1):
    return pltpu.roll(v, by, 0)


def z_next(v, by=1):
    return pltpu.roll(v, 128 - by, 1)


def z_back(v, by=1):
    return pltpu.roll(v, by, 1)


row_next, row_back, lane_next, lane_back = y_next, y_back, z_next, z_back


def pack_body(residual, classes, edge_mask, class_weight, out):
    thick = classes.shape[0]
    slots = []
    for part in range(2):
        for comp in range(3):
            slots += [residual[part, comp, i] for i in range(thick)]
    for i in range(thick):
        labels = classes[i]
        cells = jnp.zeros(labels.shape, f32)
        for label in range(class_weight.shape[0]):
            cells = jnp.where(labels == label, class_weight[label], cells)
        slots.append(cells)
    for comp in range(3):
        slots += [(1 - edge_mask[comp, i]).astype(f32) for i in range(thick)]
    zero = jnp.zeros((TILE, 128), f32)
    while len(slots) % 16:
        slots.append(zero)
    for part in range(len(slots) // 16):
        moved = jnp.concatenate(slots[16 * part : 16 * part + 16], axis=0).T
        for target in range(16):
            out[target, TILE * part : TILE * part + TILE, :] = moved[
                TILE * target : TILE * target + TILE
            ]


def unpack_body(packed, out):
    for part in range(2):
        moved = jnp.concatenate(
            [packed[source, TILE * part : TILE * part + TILE, :] for source in range(16)], axis=0
        ).T
        for slot in range(16):
            field, i = divmod(16 * part + slot, 4)
            if field < 6:
                out[field // 3, field % 3, i] = moved[TILE * slot : TILE * slot + TILE]


def line_body(
    place,
    middle,
    shallow,
    deep,
    out,
    W,
    E,
    M,
    Dm,
    Rm,
    KW,
    CW,
    FI,
    FB,
    FQ,
    CI,
    CB,
    CQ,
    NS,
    SM,
    CS,
    TY,
    RH,
    OUT,
):
    extent_y, extent_z = place[2], place[3]
    shape = (ROWS, 128)
    lane = lanes(shape)
    row = lax.broadcasted_iota(jnp.int32, shape, 0)
    at_y = lane % DEPTH + place[0]
    at_z = row + place[1]
    inside = jnp.where(
        (at_y >= 0) & (at_y < extent_y) & (at_z >= 0) & (at_z < extent_z), 1.0, 0.0
    ).astype(f32)
    coarse_inside = jnp.where(row % 2 == 0, inside, row_back(inside))
    not_first = jnp.where(lane < DEPTH, 0.0, 1.0).astype(f32)
    not_last = jnp.where(lane >= 128 - DEPTH, 0.0, 1.0).astype(f32)
    even_row = row % 2 == 0
    even_lane = lane % 2 == 0

    def pad_low(ref, field):
        ref[field, 0] = pltpu.roll(ref[field, 16], DEPTH, 1) * not_first

    def pad_high(ref, field):
        ref[field, 17] = pltpu.roll(ref[field, 1], 128 - DEPTH, 1) * not_last

    zero8 = jnp.zeros((TILE, 128), f32)
    windows = (shallow, middle, deep)

    def spread_out(a, state):
        for y in range(3):
            for part in range(3):
                pieces = []
                for p in range(16):
                    g, t = divmod(p, 4)
                    if t == 3:
                        pieces.append(zero8)
                    else:
                        pieces.append(
                            windows[t][y * 16 + 4 * g + a, TILE * part : TILE * part + TILE, :]
                        )
                moved = jnp.concatenate(pieces, axis=0).T
                for slot in range(16):
                    field, i = divmod(16 * part + slot, 4)
                    if field < 10:
                        W[field, 4 * a + i + 1, TILE * y : TILE * y + TILE, :] = moved[
                            TILE * slot : TILE * slot + TILE
                        ]
        return state

    loop(4, spread_out, 0)
    pad_low(W, 6)

    def coefficients(l, state):
        c = W[6, l + 1]
        cx = W[6, l]
        cy = y_back(c)
        cz = z_back(c)
        averages = (
            0.25 * (((c + cy) + cz) + z_back(cy)),
            0.25 * (((c + cx) + cz) + z_back(cx)),
            0.25 * (((c + cx) + cy) + y_back(cx)),
        )
        for d in range(3):
            free = W[7 + d, l + 1]
            masses = mass_factor[d] * averages[d] * free
            diagonal = stiff_weight[d] + masses
            damp = edge_damping * free / diagonal
            M[d, l] = masses
            Dm[d, l] = damp
            for part in range(2):
                source = W[3 * part + d, l + 1] * free
                W[3 * part + d, l + 1] = source
                E[3 * part + d, l + 1] = source * damp
            stiff = diagonal * free
            for g, values in enumerate(turned([masses, stiff, stiff, stiff])):
                KW[d, 16 * g + l + 1] = values
        return state

    loop(16, coefficients, 0, unroll=2)

    for d in range(3):
        KW[d, 0] = jnp.zeros(shape, f32)

    def side_fluxes(part, l):
        e1, e2, e3 = (E[3 * part + d, l] for d in range(3))
        b2 = face_weight[1] * ((z_next(e1) - e1) - (E[3 * part + 2, l + 1] - e3))
        b3 = face_weight[2] * ((E[3 * part + 1, l + 1] - e2) - (y_next(e1) - e1))
        return b2, b3

    def curl(part, l, before):
        e1, e2, e3 = (E[3 * part + d, l] for d in range(3))
        b2, b3 = side_fluxes(part, l)
        b1 = face_weight[0] * ((y_next(e3) - e3) - (z_next(e2) - e2))
        b2_before, b3_before = before
        results = (
            (z_back(b2) - b2) - (y_back(b3) - b3) + M[0, l - 1] * e1,
            (b3_before - b3) - (z_back(b1) - b1) + M[1, l - 1] * e2,
            (y_back(b1) - b1) - (b2_before - b2) + M[2, l - 1] * e3,
        )
        return results, (b2, b3)

    for field in range(6):
        pad_low(E, field)
        pad_high(E, field)

    def first_remainder(l, state):
        after = []
        for part in range(2):
            results, fluxes = curl(part, l + 1, state[part])
            after.append(fluxes)
            for d in range(3):
                Rm[3 * part + d, l + 1] = (
                    W[3 * part + d, l + 1] - results[d] * W[7 + d, l + 1]
                )
        return tuple(after)

    loop(16, first_remainder, (side_fluxes(0, 0), side_fluxes(1, 0)), unroll=4)
    pad_low(Rm, 0)
    pad_low(Rm, 3)

    def to_nodes(l, state):
        for part in range(2):
            r1, r2, r3 = (Rm[3 * part + d, l + 1] for d in range(3))
            r1b = Rm[3 * part, l]
            r2b = y_back(r2)
            r3b = z_back(r3)
            members = [
                ((r1b - r1) + (r2b - r2)) + (r3b - r3),
                0.5 * (r1 + r1b),
                0.5 * (r2 + r2b),
                0.5 * (r3 + r3b),
            ]
            for g, values in enumerate(turned(members)):
                NS[part, 16 * g + l] = values
        return state

    loop(16, to_nodes, 0, unroll=4)

    def diagonals(x, cw1_before):
        w1b, w1, w2, w3 = KW[0, x], KW[0, x + 1], KW[1, x + 1], KW[2, x + 1]
        total = ((((w1 + w1b) + w3) + row_back(w3)) + w2) + lane_back(w2)
        FI[x] = (1.0 + shift_ratio) * total + shift_added
        cw = []
        for d, w in enumerate((w1, w2, w3)):
            pair = w + row_next(w)
            pair = jnp.where(even_row, pair, row_back(pair))
            cw.append(coarse_scale[d] * (pair + lane_next(pair)))
            CW[d, x + 1] = cw[d]
        total = (
            (((cw[0] + cw1_before) + cw[2]) + row_back(cw[2], 2)) + cw[1]
        ) + lane_back(cw[1], 2)
        CI[x] = (1.0 + shift_ratio) * total + shift_added
        return cw[0]

    nothing = jnp.zeros(shape, f32)
    CW[0, 0] = nothing
    loop(64, diagonals, nothing, unroll=4)

    def factors(x, state):
        fine_before, coarse_before = state
        w1b, c1b = KW[0, x], CW[0, x]
        inverse = inside / (FI[x] - w1b * fine_before)
        coarse_inverse = coarse_inside / (CI[x] - c1b * coarse_before)
        FI[x] = inverse
        CI[x] = coarse_inverse
        FB[x] = w1b * inverse
        CB[x] = c1b * coarse_inverse
        quotient = KW[0, x + 1] * inverse
        coarse_quotient = CW[0, x + 1] * coarse_inverse
        FQ[x] = quotient
        CQ[x] = coarse_quotient
        return quotient, coarse_quotient

    loop(64, factors, (nothing, nothing), unroll=2)

    def eliminate(source, inverse, back, parts):
        def step(x, state):
            scale, couple = inverse[x], back[x]
            after = []
            for part in range(parts):
                value = source[part, x] * scale + couple * state[part]
                TY[part, x] = value
                after.append(value)
            return tuple(after)

        loop(64, step, (nothing,) * parts, unroll=4)

    def substitute(quotient, parts, then, unroll):
        def step(x, state):
            factor = quotient[x]
            after = tuple(TY[part, x] + factor * state[part] for part in range(parts))
            then(x, *after)
            return after

        loop(64, step, (nothing,) * parts, unroll=unroll, reverse=True)

    def sides(v, w2, w3, by):
        return ((w3 * row_next(v, by) + row_back(w3 * v, by)) + w2 * lane_next(v, by)) + lane_back(
            w2 * v, by
        )

    def after_smoothing(x, *values):
        halved = []
        for part, value in enumerate(values):
            SM[part, x] = value
            residue = sides(value, KW[1, x + 1], KW[2, x + 1], 1)
            halved.append(residue + 0.5 * (row_back(residue) + row_next(residue)))
        merged = jnp.where(even_row, halved[0], row_back(halved[1]))
        CS[0, x] = merged + 0.5 * (lane_back(merged) + lane_next(merged))

    def after_coarse(x, value):
        CS[0, x] = CS[0, x] + sides(value, CW[1, x + 1], CW[2, x + 1], 2)

    def after_correction(x, value):
        wide = jnp.where(even_lane, value, 0.5 * (lane_back(value) + lane_next(value)))
        above = row_next(wide)
        corrections = (
            jnp.where(even_row, wide, 0.5 * (row_back(wide) + above)),
            jnp.where(even_row, above, 0.5 * (wide + row_next(wide, 2))),
        )
        for part in range(2):
            smoothed = SM[part, x] + corrections[part]
            RH[part, x] = NS[part, x] + sides(smoothed, KW[1, x + 1], KW[2, x + 1], 1)

    def after_potential(x, *values):
        for part in range(2):
            NS[part, x] = values[part]

    eliminate(NS, FI, FB, 2)
    substitute(FQ, 2, after_smoothing, 8)
    eliminate(CS, CI, CB, 1)
    substitute(CQ, 1, after_coarse, 8)
    eliminate(CS, CI, CB, 1)
    substitute(CQ, 1, after_correction, 8)
    eliminate(RH, FI, FB, 2)
    substitute(FQ, 2, after_potential, 4)

    def from_nodes(l, state):
        for part in range(2):
            p0, p1, p2, p3 = turned([NS[part, 16 * g + l] for g in range(4)])
            Rm[3 * part, l + 1] = p0
            Rm[3 * part + 1, l + 1] = p1
            for d, (g_part, h_part) in (
                (1, (y_next(p0) - p0, 0.5 * (p2 + y_next(p2)))),
                (2, (z_next(p0) - p0, 0.5 * (p3 + z_next(p3)))),
            ):
                E[3 * part + d, l + 1] = (
                    E[3 * part + d, l + 1] + (g_part + h_part) * W[7 + d, l + 1]
                )
        return state

    loop(16, from_nodes, 0, unroll=4)
    for part in range(2):
        pad_high(Rm, 3 * part)
        pad_high(Rm, 3 * part + 1)

    def second_first(l, state):
        for part in range(2):
            p0, p1 = Rm[3 * part, l + 1], Rm[3 * part + 1, l + 1]
            g_part = Rm[3 * part, l + 2] - p0
            h_part = 0.5 * (p1 + Rm[3 * part + 1, l + 2])
            E[3 * part, l + 1] = E[3 * part, l + 1] + (g_part + h_part) * W[7, l + 1]
        return state

    loop(16, second_first, 0, unroll=4)
    for field in range(6):
        pad_low(E, field)
        pad_high(E, field)

    def last_step(l, state):
        after = []
        for part in range(2):
            results, fluxes = curl(part, l + 1, state[part])
            after.append(fluxes)
            for d in range(3):
                field = 3 * part + d
                remainder = W[field, l + 1] - results[d] * W[7 + d, l + 1]
                value = E[field, l + 1] + Dm[d, l] * remainder
                OUT[field, l] = value[TILE : 2 * TILE]
        return tuple(after)

    loop(16, last_step, (side_fluxes(0, 0), side_fluxes(1, 0)), unroll=4)

    def gather_up(a, state):
        for part in range(2):
            pieces = []
            for slot in range(16):
                field, i = divmod(16 * part + slot, 4)
                pieces.append(OUT[field, 4 * a + i] if field < 6 else zero8)
            moved = jnp.concatenate(pieces, axis=0).T
            for g in range(4):
                start = TILE * (4 * g + 1)
                out[4 * g + a, TILE * part : TILE * part + TILE, :] = moved[start : start + TILE]
        return state

    loop(4, gather_up, 0)


def vmem():
    return pl.BlockSpec(memory_space=pltpu.VMEM)


def smem():
    return pl.BlockSpec(memory_space=pltpu.SMEM)


def pack(residual, classes, edge_mask, class_weight, **options):
    return pl.pallas_call(
        pack_body,
        out_shape=jax.ShapeDtypeStruct((16, ROWS, 128), f32),
        in_specs=[vmem(), vmem(), vmem(), smem()],
        out_specs=vmem(),
        name="pack",
        **options,
    )(residual, classes, edge_mask, class_weight)


def unpack(packed, shape, **options):
    return pl.pallas_call(
        unpack_body,
        out_shape=jax.ShapeDtypeStruct(shape, f32),
        in_specs=[vmem()],
        out_specs=vmem(),
        name="unpack",
        **options,
    )(packed)


def lines(place, middle, shallow, deep, **options):
    edge = lambda count, levels: pltpu.VMEM((count, levels, ROWS, 128), f32)
    line = pltpu.VMEM((64, ROWS, 128), f32)
    pair = pltpu.VMEM((2, 64, ROWS, 128), f32)
    return pl.pallas_call(
        line_body,
        out_shape=jax.ShapeDtypeStruct((16, 2 * TILE, 128), f32),
        in_specs=[smem(), vmem(), vmem(), vmem()],
        out_specs=vmem(),
        scratch_shapes=[
            edge(10, 18),
            edge(6, 18),
            edge(3, 16),
            edge(3, 16),
            edge(6, 18),
            pltpu.VMEM((3, 65, ROWS, 128), f32),
            pltpu.VMEM((3, 65, ROWS, 128), f32),
            line,
            line,
            line,
            line,
            line,
            line,
            pair,
            pair,
            pltpu.VMEM((1, 64, ROWS, 128), f32),
            pair,
            pair,
            pltpu.VMEM((6, 16, TILE, 128), f32),
        ],
        name="lines",
        **options,
    )(place, middle, shallow, deep)


def swap(values):
    return lax.all_to_all(values, "gx", 0, 0, tiled=True)


def per_device(residual, classes, edge_mask, class_weight):
    size_x, size_y, size_z = (lax.axis_size(name) for name in ("gx", "gy", "gz"))
    axes = ("gx", "gy", "gz")
    tiles = size_x * size_z

    def position(y, tile):
        z, x = divmod(tile, size_x)
        return (x * size_y + y) * size_z + z

    def from_side(values, step_y, step_tile):
        pairs = [
            (position(y, tile), position(y + step_y, tile + step_tile))
            for y in range(size_y)
            for tile in range(tiles)
            if 0 <= y + step_y < size_y and 0 <= tile + step_tile < tiles
        ]
        return lax.ppermute(values, axes, pairs)

    own = swap(
        pack(
            residual,
            classes,
            edge_mask,
            class_weight,
        )
    )
    middle = jnp.concatenate([from_side(own, 1, 0), own, from_side(own, -1, 0)], axis=0)
    shallow = from_side(middle, 0, 1)
    deep = from_side(middle, 0, -1)
    tile = lax.axis_index("gz") * size_x + lax.axis_index("gx")
    place = jnp.stack(
        [
            lax.axis_index("gy") * TILE - TILE,
            tile * TILE - TILE,
            jnp.int32(size_y * TILE),
            jnp.int32(tiles * TILE),
        ]
    ).astype(jnp.int32)
    options = dict(compiler_params=pltpu.CompilerParams(vmem_limit_bytes=50 * 2**20))
    result = swap(lines(place, middle, shallow, deep, **options))
    return unpack(result, residual.shape)


def solution(mesh):
    return jax.shard_map(
        per_device,
        mesh=mesh,
        in_specs=(
            P("period", None, "gx", "gy", "gz"),
            P("gx", "gy", "gz"),
            P(None, "gx", "gy", "gz"),
            P("period"),
        ),
        out_specs=P("period", None, "gx", "gy", "gz"),
        check_vma=False,
    )
```

```python
import jax
import jax.numpy as jnp
from jax import lax
from jax.experimental import pallas as pl
from jax.experimental.pallas import tpu as pltpu
from jax.sharding import PartitionSpec as P


aspect = 2.0
face_weight = (1.0 / (aspect * aspect), 1.0, 1.0)
mass_factor = (aspect * aspect, 1.0, 1.0)
stiff_weight = (
    2.0 * (face_weight[1] + face_weight[2]),
    2.0 * (face_weight[0] + face_weight[2]),
    2.0 * (face_weight[0] + face_weight[1]),
)
edge_damping = 0.6
shift_ratio = 0.0001
shift_added = 0.05
coarse_scale = (0.5625, 0.1875, 0.1875)

f32 = jnp.float32
TILE = 8
ROWS = 3 * TILE
DEPTH = 32


def lanes(shape):
    return lax.broadcasted_iota(jnp.int32, shape, 1)


def turned(values):
    gap = jnp.zeros((DEPTH - ROWS, 128), f32)
    stacked = jnp.concatenate([piece for value in values for piece in (value, gap)], axis=0).T
    return [stacked[DEPTH * g : DEPTH * g + ROWS] for g in range(4)]


def loop(count, body, carry, unroll=1, reverse=False):
    def step(turn, state):
        for part in range(unroll):
            index = turn * unroll + part
            state = body(count - 1 - index if reverse else index, state)
        return state

    return lax.fori_loop(0, count // unroll, step, carry)


def y_next(v, by=1):
    return pltpu.roll(v, v.shape[0] - by, 0)


def y_back(v, by=1):
    return pltpu.roll(v, by, 0)


def z_next(v, by=1):
    return pltpu.roll(v, 128 - by, 1)


def z_back(v, by=1):
    return pltpu.roll(v, by, 1)


row_next, row_back, lane_next, lane_back = y_next, y_back, z_next, z_back


def pack_body(residual, classes, edge_mask, class_weight, out):
    thick = classes.shape[0]
    slots = []
    for i in range(thick):
        labels = classes[i]
        cells = jnp.zeros(labels.shape, f32)
        for label in range(class_weight.shape[0]):
            cells = jnp.where(labels == label, class_weight[label], cells)
        slots.append(cells)
    for comp in range(3):
        slots += [(1 - edge_mask[comp, i]).astype(f32) for i in range(thick)]
    for part in range(2):
        for comp in range(3):
            slots += [residual[part, comp, i] for i in range(thick)]
    zero = jnp.zeros((TILE, 128), f32)
    while len(slots) % 16:
        slots.append(zero)
    for part in range(len(slots) // 16):
        moved = jnp.concatenate(slots[16 * part : 16 * part + 16], axis=0).T
        for target in range(16):
            out[target, TILE * part : TILE * part + TILE, :] = moved[
                TILE * target : TILE * target + TILE
            ]


def unpack_body(packed, out):
    for part in range(2):
        moved = jnp.concatenate(
            [packed[source, TILE * part : TILE * part + TILE, :] for source in range(16)], axis=0
        ).T
        for slot in range(16):
            field, i = divmod(16 * part + slot, 4)
            if field < 6:
                out[field // 3, field % 3, i] = moved[TILE * slot : TILE * slot + TILE]


def pad_low(ref, field):
    lane = lanes((ROWS, 128))
    ref[field, 0] = jnp.where(lane < DEPTH, 0.0, pltpu.roll(ref[field, 16], DEPTH, 1))


def pad_high(ref, field):
    lane = lanes((ROWS, 128))
    ref[field, 17] = jnp.where(
        lane >= 128 - DEPTH, 0.0, pltpu.roll(ref[field, 1], 128 - DEPTH, 1)
    )


def spread_out(windows, parts, put):
    zero8 = jnp.zeros((TILE, 128), f32)

    def step(a, state):
        for y in range(3):
            for part in range(parts):
                pieces = []
                for p in range(16):
                    g, t = divmod(p, 4)
                    if t == 3:
                        pieces.append(zero8)
                    else:
                        pieces.append(
                            windows[t][y * 16 + 4 * g + a, TILE * part : TILE * part + TILE, :]
                        )
                moved = jnp.concatenate(pieces, axis=0).T
                for slot in range(16):
                    field, i = divmod(16 * part + slot, 4)
                    put(field, 4 * a + i, y, moved[TILE * slot : TILE * slot + TILE])
        return state

    loop(4, step, 0, unroll=2)


def setup_body(
    place, middle, shallow, deep, free_out, M, Dm, KW, CW, FI, FB, FQ, CI, CB, CQ, cells
):
    extent_y, extent_z = place[2], place[3]
    shape = (ROWS, 128)
    lane = lanes(shape)
    row = lax.broadcasted_iota(jnp.int32, shape, 0)
    at_y = lane % DEPTH + place[0]
    at_z = row + place[1]
    inside = jnp.where(
        (at_y >= 0) & (at_y < extent_y) & (at_z >= 0) & (at_z < extent_z), 1.0, 0.0
    ).astype(f32)
    coarse_inside = jnp.where(row % 2 == 0, inside, row_back(inside))
    even_row = row % 2 == 0

    def put(field, level, y, values):
        if field == 0:
            cells[0, level + 1, TILE * y : TILE * y + TILE, :] = values
        else:
            free_out[field - 1, level, TILE * y : TILE * y + TILE, :] = values

    spread_out((shallow, middle, deep), 1, put)
    pad_low(cells, 0)

    def coefficients(l, state):
        c = cells[0, l + 1]
        cx = cells[0, l]
        cy = y_back(c)
        cz = z_back(c)
        averages = (
            0.25 * (((c + cy) + cz) + z_back(cy)),
            0.25 * (((c + cx) + cz) + z_back(cx)),
            0.25 * (((c + cx) + cy) + y_back(cx)),
        )
        for d in range(3):
            free = free_out[d, l]
            masses = mass_factor[d] * averages[d] * free
            diagonal = stiff_weight[d] + masses
            M[d, l] = masses
            Dm[d, l] = edge_damping * free / diagonal
            stiff = diagonal * free
            for g, values in enumerate(turned([masses, stiff, stiff, stiff])):
                KW[d, 16 * g + l + 1] = values
        return state

    loop(16, coefficients, 0, unroll=8)

    for d in range(3):
        KW[d, 0] = jnp.zeros(shape, f32)

    def diagonals(x, cw1_before):
        w1b, w1, w2, w3 = KW[0, x], KW[0, x + 1], KW[1, x + 1], KW[2, x + 1]
        total = ((((w1 + w1b) + w3) + row_back(w3)) + w2) + lane_back(w2)
        FI[x] = (1.0 + shift_ratio) * total + shift_added
        cw = []
        for d, w in enumerate((w1, w2, w3)):
            pair = w + row_next(w)
            pair = jnp.where(even_row, pair, row_back(pair))
            cw.append(coarse_scale[d] * (pair + lane_next(pair)))
            CW[d, x + 1] = cw[d]
        total = (
            (((cw[0] + cw1_before) + cw[2]) + row_back(cw[2], 2)) + cw[1]
        ) + lane_back(cw[1], 2)
        CI[x] = (1.0 + shift_ratio) * total + shift_added
        return cw[0]

    nothing = jnp.zeros(shape, f32)
    CW[0, 0] = nothing
    loop(64, diagonals, nothing, unroll=8)

    def factors(x, state):
        fine_before, coarse_before = state
        w1b, c1b = KW[0, x], CW[0, x]
        inverse = inside / (FI[x] - w1b * fine_before)
        coarse_inverse = coarse_inside / (CI[x] - c1b * coarse_before)
        FI[x] = inverse
        CI[x] = coarse_inverse
        FB[x] = w1b * inverse
        CB[x] = c1b * coarse_inverse
        quotient = KW[0, x + 1] * inverse
        coarse_quotient = CW[0, x + 1] * coarse_inverse
        FQ[x] = quotient
        CQ[x] = coarse_quotient
        return quotient, coarse_quotient

    loop(64, factors, (nothing, nothing), unroll=2)


def line_body(
    middle,
    shallow,
    deep,
    free,
    M,
    Dm,
    KW,
    CW,
    FI,
    FB,
    FQ,
    CI,
    CB,
    CQ,
    out,
    W,
    E,
    Rm,
    NS,
    SM,
    CS,
    TY,
    RH,
    OUT,
):
    shape = (ROWS, 128)
    even_row = lax.broadcasted_iota(jnp.int32, shape, 0) % 2 == 0
    even_lane = lanes(shape) % 2 == 0
    nothing = jnp.zeros(shape, f32)
    zero8 = jnp.zeros((TILE, 128), f32)

    def put(field, level, y, values):
        if field < 6:
            rows = slice(TILE * y, TILE * y + TILE)
            source = values * free[field % 3, level, rows, :]
            W[field, level, rows, :] = source
            E[field, level + 1, rows, :] = source * Dm[field % 3, level, rows, :]

    spread_out((shallow, middle, deep), 2, put)

    def side_fluxes(part, l):
        e1, e2, e3 = (E[3 * part + d, l] for d in range(3))
        b2 = face_weight[1] * ((z_next(e1) - e1) - (E[3 * part + 2, l + 1] - e3))
        b3 = face_weight[2] * ((E[3 * part + 1, l + 1] - e2) - (y_next(e1) - e1))
        return b2, b3

    def curl(part, l, before):
        e1, e2, e3 = (E[3 * part + d, l] for d in range(3))
        b2, b3 = side_fluxes(part, l)
        b1 = face_weight[0] * ((y_next(e3) - e3) - (z_next(e2) - e2))
        b2_before, b3_before = before
        results = (
            (z_back(b2) - b2) - (y_back(b3) - b3) + M[0, l - 1] * e1,
            (b3_before - b3) - (z_back(b1) - b1) + M[1, l - 1] * e2,
            (y_back(b1) - b1) - (b2_before - b2) + M[2, l - 1] * e3,
        )
        return results, (b2, b3)

    for field in range(6):
        pad_low(E, field)
        pad_high(E, field)

    def first_remainder(l, state):
        after = []
        for part in range(2):
            results, fluxes = curl(part, l + 1, state[part])
            after.append(fluxes)
            for d in range(3):
                Rm[3 * part + d, l + 1] = (
                    W[3 * part + d, l] - results[d] * free[d, l]
                )
        return tuple(after)

    loop(16, first_remainder, (side_fluxes(0, 0), side_fluxes(1, 0)), unroll=4)
    pad_low(Rm, 0)
    pad_low(Rm, 3)

    def to_nodes(l, state):
        for part in range(2):
            r1, r2, r3 = (Rm[3 * part + d, l + 1] for d in range(3))
            r1b = Rm[3 * part, l]
            r2b = y_back(r2)
            r3b = z_back(r3)
            members = [
                ((r1b - r1) + (r2b - r2)) + (r3b - r3),
                0.5 * (r1 + r1b),
                0.5 * (r2 + r2b),
                0.5 * (r3 + r3b),
            ]
            for g, values in enumerate(turned(members)):
                NS[part, 16 * g + l] = values
        return state

    loop(16, to_nodes, 0, unroll=8)

    def eliminate(source, inverse, back, parts):
        def step(x, state):
            scale, couple = inverse[x], back[x]
            after = []
            for part in range(parts):
                value = source[part, x] * scale + couple * state[part]
                TY[part, x] = value
                after.append(value)
            return tuple(after)

        loop(64, step, (nothing,) * parts, unroll=4)

    def substitute(quotient, parts, then, unroll):
        def step(x, state):
            factor = quotient[x]
            after = tuple(TY[part, x] + factor * state[part] for part in range(parts))
            then(x, *after)
            return after

        loop(64, step, (nothing,) * parts, unroll=unroll, reverse=True)

    def sides(v, w2, w3, by):
        return ((w3 * row_next(v, by) + row_back(w3 * v, by)) + w2 * lane_next(v, by)) + lane_back(
            w2 * v, by
        )

    def after_smoothing(x, *values):
        halved = []
        for part, value in enumerate(values):
            SM[part, x] = value
            residue = sides(value, KW[1, x + 1], KW[2, x + 1], 1)
            halved.append(residue + 0.5 * (row_back(residue) + row_next(residue)))
        merged = jnp.where(even_row, halved[0], row_back(halved[1]))
        CS[0, x] = merged + 0.5 * (lane_back(merged) + lane_next(merged))

    def after_coarse(x, value):
        CS[0, x] = CS[0, x] + sides(value, CW[1, x + 1], CW[2, x + 1], 2)

    def after_correction(x, value):
        wide = jnp.where(even_lane, value, 0.5 * (lane_back(value) + lane_next(value)))
        above = row_next(wide)
        corrections = (
            jnp.where(even_row, wide, 0.5 * (row_back(wide) + above)),
            jnp.where(even_row, above, 0.5 * (wide + row_next(wide, 2))),
        )
        for part in range(2):
            smoothed = SM[part, x] + corrections[part]
            RH[part, x] = NS[part, x] + sides(smoothed, KW[1, x + 1], KW[2, x + 1], 1)

    def after_potential(x, *values):
        for part in range(2):
            NS[part, x] = values[part]

    eliminate(NS, FI, FB, 2)
    substitute(FQ, 2, after_smoothing, 8)
    eliminate(CS, CI, CB, 1)
    substitute(CQ, 1, after_coarse, 16)
    eliminate(CS, CI, CB, 1)
    substitute(CQ, 1, after_correction, 8)
    eliminate(RH, FI, FB, 2)
    substitute(FQ, 2, after_potential, 4)

    def from_nodes(l, state):
        for part in range(2):
            p0, p1, p2, p3 = turned([NS[part, 16 * g + l] for g in range(4)])
            Rm[3 * part, l + 1] = p0
            Rm[3 * part + 1, l + 1] = p1
            for d, (g_part, h_part) in (
                (1, (y_next(p0) - p0, 0.5 * (p2 + y_next(p2)))),
                (2, (z_next(p0) - p0, 0.5 * (p3 + z_next(p3)))),
            ):
                E[3 * part + d, l + 1] = (
                    E[3 * part + d, l + 1] + (g_part + h_part) * free[d, l]
                )
        return state

    loop(16, from_nodes, 0, unroll=8)
    for part in range(2):
        pad_high(Rm, 3 * part)
        pad_high(Rm, 3 * part + 1)

    def second_first(l, state):
        for part in range(2):
            p0, p1 = Rm[3 * part, l + 1], Rm[3 * part + 1, l + 1]
            g_part = Rm[3 * part, l + 2] - p0
            h_part = 0.5 * (p1 + Rm[3 * part + 1, l + 2])
            E[3 * part, l + 1] = E[3 * part, l + 1] + (g_part + h_part) * free[0, l]
        return state

    loop(16, second_first, 0, unroll=4)
    for field in range(6):
        pad_low(E, field)
        pad_high(E, field)

    def last_step(l, state):
        after = []
        for part in range(2):
            results, fluxes = curl(part, l + 1, state[part])
            after.append(fluxes)
            for d in range(3):
                field = 3 * part + d
                remainder = W[field, l] - results[d] * free[d, l]
                value = E[field, l + 1] + Dm[d, l] * remainder
                OUT[field, l] = value[TILE : 2 * TILE]
        return tuple(after)

    loop(16, last_step, (side_fluxes(0, 0), side_fluxes(1, 0)), unroll=8)

    def gather_up(a, state):
        for part in range(2):
            pieces = []
            for slot in range(16):
                field, i = divmod(16 * part + slot, 4)
                pieces.append(OUT[field, 4 * a + i] if field < 6 else zero8)
            moved = jnp.concatenate(pieces, axis=0).T
            for g in range(4):
                start = TILE * (4 * g + 1)
                out[4 * g + a, TILE * part : TILE * part + TILE, :] = moved[start : start + TILE]
        return state

    loop(4, gather_up, 0)


def vmem():
    return pl.BlockSpec(memory_space=pltpu.VMEM)


def smem():
    return pl.BlockSpec(memory_space=pltpu.SMEM)


def pack(residual, classes, edge_mask, class_weight, **options):
    return pl.pallas_call(
        pack_body,
        out_shape=jax.ShapeDtypeStruct((16, ROWS, 128), f32),
        in_specs=[vmem(), vmem(), vmem(), smem()],
        out_specs=vmem(),
        name="pack",
        **options,
    )(residual, classes, edge_mask, class_weight)


def unpack(packed, shape, **options):
    return pl.pallas_call(
        unpack_body,
        out_shape=jax.ShapeDtypeStruct(shape, f32),
        in_specs=[vmem()],
        out_specs=vmem(),
        name="unpack",
        **options,
    )(packed)


def resident(*shape):
    return pltpu.VMEM(shape, f32)


def setup(place, middle, shallow, deep, **options):
    line = resident(64, ROWS, 128)
    edge = resident(3, 16, ROWS, 128)
    weights = resident(3, 65, ROWS, 128)
    return pl.pallas_call(
        setup_body,
        out_shape=[edge, edge, edge, weights, weights] + [line] * 6,
        in_specs=[smem(), vmem(), vmem(), vmem()],
        out_specs=[vmem()] * 11,
        scratch_shapes=[resident(1, 18, ROWS, 128)],
        name="setup",
        **options,
    )(place, middle, shallow, deep)


def lines(middle, shallow, deep, ready, **options):
    edge = lambda count, levels: resident(count, levels, ROWS, 128)
    pair = resident(2, 64, ROWS, 128)
    return pl.pallas_call(
        line_body,
        out_shape=jax.ShapeDtypeStruct((16, 2 * TILE, 128), f32),
        in_specs=[vmem()] * (3 + len(ready)),
        out_specs=vmem(),
        scratch_shapes=[
            edge(6, 16),
            edge(6, 18),
            edge(6, 18),
            pair,
            pair,
            resident(1, 64, ROWS, 128),
            pair,
            pair,
            resident(6, 16, TILE, 128),
        ],
        name="lines",
        **options,
    )(middle, shallow, deep, *ready)


def swap(values):
    return lax.all_to_all(values, "gx", 0, 0, tiled=True)


def per_device(residual, classes, edge_mask, class_weight):
    size_x, size_y, size_z = (lax.axis_size(name) for name in ("gx", "gy", "gz"))
    axes = ("gx", "gy", "gz")
    tiles = size_x * size_z

    def position(y, tile):
        z, x = divmod(tile, size_x)
        return (x * size_y + y) * size_z + z

    def from_side(values, step_y, step_tile):
        pairs = [
            (position(y, tile), position(y + step_y, tile + step_tile))
            for y in range(size_y)
            for tile in range(tiles)
            if 0 <= y + step_y < size_y and 0 <= tile + step_tile < tiles
        ]
        return lax.ppermute(values, axes, pairs)

    own = swap(
        pack(
            residual,
            classes,
            edge_mask,
            class_weight,
        )
    )
    middle = jnp.concatenate([from_side(own, 1, 0), own, from_side(own, -1, 0)], axis=0)
    material, source = middle[:, :TILE], middle[:, TILE:]
    shallow_material = from_side(material, 0, 1)
    deep_material = from_side(material, 0, -1)
    shallow_source = from_side(source, 0, 1)
    deep_source = from_side(source, 0, -1)
    tile = lax.axis_index("gz") * size_x + lax.axis_index("gx")
    place = jnp.stack(
        [
            lax.axis_index("gy") * TILE - TILE,
            tile * TILE - TILE,
            jnp.int32(size_y * TILE),
            jnp.int32(tiles * TILE),
        ]
    ).astype(jnp.int32)
    options = lambda size, cost: dict(
        compiler_params=pltpu.CompilerParams(vmem_limit_bytes=size * 2**20),
        cost_estimate=pl.CostEstimate(flops=cost, bytes_accessed=0, transcendentals=0),
    )
    ready = setup(
        place, material, shallow_material, deep_material, **options(20, 2**27)
    )
    result = swap(lines(source, shallow_source, deep_source, ready, **options(32, 2**27)))
    return unpack(result, residual.shape)


def solution(mesh):
    return jax.shard_map(
        per_device,
        mesh=mesh,
        in_specs=(
            P("period", None, "gx", "gy", "gz"),
            P("gx", "gy", "gz"),
            P(None, "gx", "gy", "gz"),
            P("period"),
        ),
        out_specs=P("period", None, "gx", "gy", "gz"),
        check_vma=False,
    )
```

```python
import jax
import jax.numpy as jnp
from jax import lax
from jax.experimental import pallas as pl
from jax.experimental.pallas import tpu as pltpu
from jax.sharding import PartitionSpec as P


aspect = 2.0
face_weight = (1.0 / (aspect * aspect), 1.0, 1.0)
mass_factor = (aspect * aspect, 1.0, 1.0)
stiff_weight = (
    2.0 * (face_weight[1] + face_weight[2]),
    2.0 * (face_weight[0] + face_weight[2]),
    2.0 * (face_weight[0] + face_weight[1]),
)
edge_damping = 0.6
shift_ratio = 0.0001
shift_added = 0.05
coarse_scale = (0.5625, 0.1875, 0.1875)

f32 = jnp.float32
TILE = 8
ROWS = 3 * TILE
DEPTH = 32
HALF = TILE // 2


def lanes(shape):
    return lax.broadcasted_iota(jnp.int32, shape, 1)


def turned(values):
    gap = jnp.zeros((DEPTH - ROWS, 128), f32)
    stacked = jnp.concatenate([piece for value in values for piece in (value, gap)], axis=0).T
    return [stacked[DEPTH * g : DEPTH * g + ROWS] for g in range(4)]


def loop(count, body, carry, unroll=1, reverse=False):
    def step(turn, state):
        for part in range(unroll):
            index = turn * unroll + part
            state = body(count - 1 - index if reverse else index, state)
        return state

    return lax.fori_loop(0, count // unroll, step, carry)


def y_next(v, by=1):
    return pltpu.roll(v, v.shape[0] - by, 0)


def y_back(v, by=1):
    return pltpu.roll(v, by, 0)


def z_next(v, by=1):
    return pltpu.roll(v, 128 - by, 1)


def z_back(v, by=1):
    return pltpu.roll(v, by, 1)


row_next, row_back, lane_next, lane_back = y_next, y_back, z_next, z_back


def pack_body(residual, classes, edge_mask, class_weight, out):
    thick = classes.shape[0]
    slots = []
    for i in range(thick):
        labels = classes[i]
        cells = jnp.zeros(labels.shape, f32)
        for label in range(class_weight.shape[0]):
            cells = jnp.where(labels == label, class_weight[label], cells)
        slots.append(cells)
    for comp in range(3):
        slots += [(1 - edge_mask[comp, i]).astype(f32) for i in range(thick)]
    for part in range(2):
        for comp in range(3):
            slots += [residual[part, comp, i] for i in range(thick)]
    block = 0
    for start in range(0, len(slots), 16):
        group = jnp.concatenate(slots[start : start + 16], axis=0)
        block = send_group(group, lambda target: target, out, block)


def send_group(group, device, out, block):
    half = HALF
    if group.shape[0] == 128:
        moved = group.T
        parts = 2
    else:
        moved = jnp.concatenate([group, pltpu.roll(group, 128 - half, 1)], axis=0).T
        parts = 1
    for target in range(16):
        place = device(target)
        if place is not None:
            for part in range(parts):
                row = TILE * target + half * part
                out[place, block + part] = moved[row : row + half]
    return block + parts


def receive_group(blocks, block, full):
    half = HALF
    gap = jnp.zeros((half, 128), f32)
    rows = []
    for source in range(16):
        rows.append(blocks(source, block))
        rows.append(blocks(source, block + 1) if full else gap)
    moved = jnp.concatenate(rows, axis=0).T
    if full:
        return moved
    upper = pltpu.roll(moved[64:], half, 1)
    return jnp.where(lanes((64, 128)) % TILE < half, moved[:64], upper)


def unpack_body(packed, out):
    for part in range(2):
        moved = receive_group(lambda source, block: packed[source, block], 2 * part, part == 0)
        for slot in range(moved.shape[0] // TILE):
            field, i = divmod(16 * part + slot, 4)
            out[field // 3, field % 3, i] = moved[TILE * slot : TILE * slot + TILE]


def pad_low(ref, field):
    lane = lanes((ROWS, 128))
    ref[field, 0] = jnp.where(lane < DEPTH, 0.0, pltpu.roll(ref[field, 16], DEPTH, 1))


def pad_high(ref, field):
    lane = lanes((ROWS, 128))
    ref[field, 17] = jnp.where(
        lane >= 128 - DEPTH, 0.0, pltpu.roll(ref[field, 1], 128 - DEPTH, 1)
    )


def spread_out(windows, groups, put):
    gap = jnp.zeros((HALF, 128), f32)

    def step(a, state):
        for y in range(3):
            for part, full in enumerate(groups):

                def blocks(p, block):
                    g, t = divmod(p, 4)
                    if t == 3:
                        return gap
                    ref, first = windows[t]
                    return ref[y * 16 + 4 * g + a, first + block]

                moved = receive_group(blocks, 2 * part, full)
                for slot in range(moved.shape[0] // TILE):
                    field, i = divmod(16 * part + slot, 4)
                    put(field, 4 * a + i, y, moved[TILE * slot : TILE * slot + TILE])
        return state

    loop(4, step, 0, unroll=2)


def setup_body(
    place, middle, shallow, deep, free_out, M, Dm, KW, CW, FI, FB, FQ, CI, CB, CQ, cells
):
    extent_y, extent_z = place[2], place[3]
    shape = (ROWS, 128)
    lane = lanes(shape)
    row = lax.broadcasted_iota(jnp.int32, shape, 0)
    at_y = lane % DEPTH + place[0]
    at_z = row + place[1]
    inside = jnp.where(
        (at_y >= 0) & (at_y < extent_y) & (at_z >= 0) & (at_z < extent_z), 1.0, 0.0
    ).astype(f32)
    coarse_inside = jnp.where(row % 2 == 0, inside, row_back(inside))
    even_row = row % 2 == 0

    def put(field, level, y, values):
        if field == 0:
            cells[0, level + 1, TILE * y : TILE * y + TILE, :] = values
        else:
            free_out[field - 1, level, TILE * y : TILE * y + TILE, :] = values

    spread_out(((shallow, 0), (middle, 0), (deep, 0)), (True,), put)
    pad_low(cells, 0)

    def coefficients(l, state):
        c = cells[0, l + 1]
        cx = cells[0, l]
        cy = y_back(c)
        cz = z_back(c)
        averages = (
            0.25 * (((c + cy) + cz) + z_back(cy)),
            0.25 * (((c + cx) + cz) + z_back(cx)),
            0.25 * (((c + cx) + cy) + y_back(cx)),
        )
        for d in range(3):
            free = free_out[d, l]
            masses = mass_factor[d] * averages[d] * free
            diagonal = stiff_weight[d] + masses
            M[d, l] = masses
            Dm[d, l] = edge_damping * free / diagonal
            stiff = diagonal * free
            for g, values in enumerate(turned([masses, stiff, stiff, stiff])):
                KW[d, 16 * g + l + 1] = values
        return state

    loop(16, coefficients, 0, unroll=8)

    for d in range(3):
        KW[d, 0] = jnp.zeros(shape, f32)

    def diagonals(x, cw1_before):
        w1b, w1, w2, w3 = KW[0, x], KW[0, x + 1], KW[1, x + 1], KW[2, x + 1]
        total = ((((w1 + w1b) + w3) + row_back(w3)) + w2) + lane_back(w2)
        FI[x] = (1.0 + shift_ratio) * total + shift_added
        cw = []
        for d, w in enumerate((w1, w2, w3)):
            pair = w + row_next(w)
            pair = jnp.where(even_row, pair, row_back(pair))
            cw.append(coarse_scale[d] * (pair + lane_next(pair)))
            CW[d, x + 1] = cw[d]
        total = (
            (((cw[0] + cw1_before) + cw[2]) + row_back(cw[2], 2)) + cw[1]
        ) + lane_back(cw[1], 2)
        CI[x] = (1.0 + shift_ratio) * total + shift_added
        return cw[0]

    nothing = jnp.zeros(shape, f32)
    CW[0, 0] = nothing
    loop(64, diagonals, nothing, unroll=8)

    def factors(x, state):
        fine_before, coarse_before = state
        w1b, c1b = KW[0, x], CW[0, x]
        inverse = inside / (FI[x] - w1b * fine_before)
        coarse_inverse = coarse_inside / (CI[x] - c1b * coarse_before)
        FI[x] = inverse
        CI[x] = coarse_inverse
        FB[x] = w1b * inverse
        CB[x] = c1b * coarse_inverse
        quotient = KW[0, x + 1] * inverse
        coarse_quotient = CW[0, x + 1] * coarse_inverse
        FQ[x] = quotient
        CQ[x] = coarse_quotient
        return quotient, coarse_quotient

    loop(64, factors, (nothing, nothing), unroll=2)


def line_body(
    middle,
    shallow,
    deep,
    free,
    M,
    Dm,
    KW,
    CW,
    FI,
    FB,
    FQ,
    CI,
    CB,
    CQ,
    out,
    W,
    E,
    Rm,
    NS,
    SM,
    CS,
    TY,
    RH,
    OUT,
):
    shape = (ROWS, 128)
    even_row = lax.broadcasted_iota(jnp.int32, shape, 0) % 2 == 0
    even_lane = lanes(shape) % 2 == 0
    nothing = jnp.zeros(shape, f32)

    def put(field, level, y, values):
        rows = slice(TILE * y, TILE * y + TILE)
        source = values * free[field % 3, level, rows, :]
        W[field, level, rows, :] = source
        E[field, level + 1, rows, :] = source * Dm[field % 3, level, rows, :]

    spread_out(((shallow, 0), (middle, 2), (deep, 0)), (True, False), put)

    def side_fluxes(part, l):
        e1, e2, e3 = (E[3 * part + d, l] for d in range(3))
        b2 = face_weight[1] * ((z_next(e1) - e1) - (E[3 * part + 2, l + 1] - e3))
        b3 = face_weight[2] * ((E[3 * part + 1, l + 1] - e2) - (y_next(e1) - e1))
        return b2, b3

    def curl(part, l, before):
        e1, e2, e3 = (E[3 * part + d, l] for d in range(3))
        b2, b3 = side_fluxes(part, l)
        b1 = face_weight[0] * ((y_next(e3) - e3) - (z_next(e2) - e2))
        b2_before, b3_before = before
        results = (
            (z_back(b2) - b2) - (y_back(b3) - b3) + M[0, l - 1] * e1,
            (b3_before - b3) - (z_back(b1) - b1) + M[1, l - 1] * e2,
            (y_back(b1) - b1) - (b2_before - b2) + M[2, l - 1] * e3,
        )
        return results, (b2, b3)

    for field in range(6):
        pad_low(E, field)
        pad_high(E, field)

    def first_remainder(l, state):
        after = []
        for part in range(2):
            results, fluxes = curl(part, l + 1, state[part])
            after.append(fluxes)
            for d in range(3):
                Rm[3 * part + d, l + 1] = (
                    W[3 * part + d, l] - results[d] * free[d, l]
                )
        return tuple(after)

    loop(16, first_remainder, (side_fluxes(0, 0), side_fluxes(1, 0)), unroll=4)
    pad_low(Rm, 0)
    pad_low(Rm, 3)

    def to_nodes(l, state):
        for part in range(2):
            r1, r2, r3 = (Rm[3 * part + d, l + 1] for d in range(3))
            r1b = Rm[3 * part, l]
            r2b = y_back(r2)
            r3b = z_back(r3)
            members = [
                ((r1b - r1) + (r2b - r2)) + (r3b - r3),
                0.5 * (r1 + r1b),
                0.5 * (r2 + r2b),
                0.5 * (r3 + r3b),
            ]
            for g, values in enumerate(turned(members)):
                NS[part, 16 * g + l] = values
        return state

    loop(16, to_nodes, 0, unroll=8)

    def eliminate(source, inverse, back, parts):
        def step(x, state):
            scale, couple = inverse[x], back[x]
            after = []
            for part in range(parts):
                value = source[part, x] * scale + couple * state[part]
                TY[part, x] = value
                after.append(value)
            return tuple(after)

        loop(64, step, (nothing,) * parts, unroll=4)

    def substitute(quotient, parts, then, unroll):
        def step(x, state):
            factor = quotient[x]
            after = tuple(TY[part, x] + factor * state[part] for part in range(parts))
            then(x, *after)
            return after

        loop(64, step, (nothing,) * parts, unroll=unroll, reverse=True)

    def sides(v, w2, w3, by):
        return ((w3 * row_next(v, by) + row_back(w3 * v, by)) + w2 * lane_next(v, by)) + lane_back(
            w2 * v, by
        )

    def after_smoothing(x, *values):
        halved = []
        for part, value in enumerate(values):
            SM[part, x] = value
            residue = sides(value, KW[1, x + 1], KW[2, x + 1], 1)
            halved.append(residue + 0.5 * (row_back(residue) + row_next(residue)))
        merged = jnp.where(even_row, halved[0], row_back(halved[1]))
        CS[0, x] = merged + 0.5 * (lane_back(merged) + lane_next(merged))

    def after_coarse(x, value):
        CS[0, x] = CS[0, x] + sides(value, CW[1, x + 1], CW[2, x + 1], 2)

    def after_correction(x, value):
        wide = jnp.where(even_lane, value, 0.5 * (lane_back(value) + lane_next(value)))
        above = row_next(wide)
        corrections = (
            jnp.where(even_row, wide, 0.5 * (row_back(wide) + above)),
            jnp.where(even_row, above, 0.5 * (wide + row_next(wide, 2))),
        )
        for part in range(2):
            smoothed = SM[part, x] + corrections[part]
            RH[part, x] = NS[part, x] + sides(smoothed, KW[1, x + 1], KW[2, x + 1], 1)

    def after_potential(x, *values):
        for part in range(2):
            NS[part, x] = values[part]

    eliminate(NS, FI, FB, 2)
    substitute(FQ, 2, after_smoothing, 8)
    eliminate(CS, CI, CB, 1)
    substitute(CQ, 1, after_coarse, 16)
    eliminate(CS, CI, CB, 1)
    substitute(CQ, 1, after_correction, 8)
    eliminate(RH, FI, FB, 2)
    substitute(FQ, 2, after_potential, 4)

    def from_nodes(l, state):
        for part in range(2):
            p0, p1, p2, p3 = turned([NS[part, 16 * g + l] for g in range(4)])
            Rm[3 * part, l + 1] = p0
            Rm[3 * part + 1, l + 1] = p1
            for d, (g_part, h_part) in (
                (1, (y_next(p0) - p0, 0.5 * (p2 + y_next(p2)))),
                (2, (z_next(p0) - p0, 0.5 * (p3 + z_next(p3)))),
            ):
                E[3 * part + d, l + 1] = (
                    E[3 * part + d, l + 1] + (g_part + h_part) * free[d, l]
                )
        return state

    loop(16, from_nodes, 0, unroll=8)
    for part in range(2):
        pad_high(Rm, 3 * part)
        pad_high(Rm, 3 * part + 1)

    def second_first(l, state):
        for part in range(2):
            p0, p1 = Rm[3 * part, l + 1], Rm[3 * part + 1, l + 1]
            g_part = Rm[3 * part, l + 2] - p0
            h_part = 0.5 * (p1 + Rm[3 * part + 1, l + 2])
            E[3 * part, l + 1] = E[3 * part, l + 1] + (g_part + h_part) * free[0, l]
        return state

    loop(16, second_first, 0, unroll=4)
    for field in range(6):
        pad_low(E, field)
        pad_high(E, field)

    def last_step(l, state):
        after = []
        for part in range(2):
            results, fluxes = curl(part, l + 1, state[part])
            after.append(fluxes)
            for d in range(3):
                field = 3 * part + d
                remainder = W[field, l] - results[d] * free[d, l]
                value = E[field, l + 1] + Dm[d, l] * remainder
                OUT[field, l] = value[TILE : 2 * TILE]
        return tuple(after)

    loop(16, last_step, (side_fluxes(0, 0), side_fluxes(1, 0)), unroll=8)

    def gather_up(a, state):
        slots = [OUT[field, 4 * a + i] for field in range(6) for i in range(4)]
        block = 0
        for start in (0, 16):
            group = jnp.concatenate(slots[start : start + 16], axis=0)
            block = send_group(
                group, lambda p: p // 4 * 4 + a if p % 4 == 1 else None, out, block
            )
        return state

    loop(4, gather_up, 0)


def vmem():
    return pl.BlockSpec(memory_space=pltpu.VMEM)


def smem():
    return pl.BlockSpec(memory_space=pltpu.SMEM)


def pack(residual, classes, edge_mask, class_weight, **options):
    return pl.pallas_call(
        pack_body,
        out_shape=resident(16, 5, HALF, 128),
        in_specs=[vmem(), vmem(), vmem(), smem()],
        out_specs=vmem(),
        name="pack",
        **options,
    )(residual, classes, edge_mask, class_weight)


def unpack(packed, shape, **options):
    return pl.pallas_call(
        unpack_body,
        out_shape=jax.ShapeDtypeStruct(shape, f32),
        in_specs=[vmem()],
        out_specs=vmem(),
        name="unpack",
        **options,
    )(packed)


def resident(*shape):
    return pltpu.VMEM(shape, f32)


def setup(place, middle, shallow, deep, **options):
    line = resident(64, ROWS, 128)
    edge = resident(3, 16, ROWS, 128)
    weights = resident(3, 65, ROWS, 128)
    return pl.pallas_call(
        setup_body,
        out_shape=[edge, edge, edge, weights, weights] + [line] * 6,
        in_specs=[smem(), vmem(), vmem(), vmem()],
        out_specs=[vmem()] * 11,
        scratch_shapes=[resident(1, 18, ROWS, 128)],
        name="setup",
        **options,
    )(place, middle, shallow, deep)


def lines(middle, shallow, deep, ready, **options):
    edge = lambda count, levels: resident(count, levels, ROWS, 128)
    pair = resident(2, 64, ROWS, 128)
    return pl.pallas_call(
        line_body,
        out_shape=resident(16, 3, HALF, 128),
        in_specs=[vmem()] * (3 + len(ready)),
        out_specs=vmem(),
        scratch_shapes=[
            edge(6, 16),
            edge(6, 18),
            edge(6, 18),
            pair,
            pair,
            resident(1, 64, ROWS, 128),
            pair,
            pair,
            resident(6, 16, TILE, 128),
        ],
        name="lines",
        **options,
    )(middle, shallow, deep, *ready)


def swap(values):
    return lax.all_to_all(values, "gx", 0, 0, tiled=True)


def per_device(residual, classes, edge_mask, class_weight):
    size_x, size_y, size_z = (lax.axis_size(name) for name in ("gx", "gy", "gz"))
    axes = ("gx", "gy", "gz")
    tiles = size_x * size_z

    def position(y, tile):
        z, x = divmod(tile, size_x)
        return (x * size_y + y) * size_z + z

    def from_side(values, step_y, step_tile):
        pairs = [
            (position(y, tile), position(y + step_y, tile + step_tile))
            for y in range(size_y)
            for tile in range(tiles)
            if 0 <= y + step_y < size_y and 0 <= tile + step_tile < tiles
        ]
        return lax.ppermute(values, axes, pairs)

    own = swap(
        pack(
            residual,
            classes,
            edge_mask,
            class_weight,
        )
    )
    middle = jnp.concatenate([from_side(own, 1, 0), own, from_side(own, -1, 0)], axis=0)
    material, source = middle[:, :2], middle[:, 2:]
    shallow_material = from_side(material, 0, 1)
    deep_material = from_side(material, 0, -1)
    shallow_source = from_side(source, 0, 1)
    deep_source = from_side(source, 0, -1)
    tile = lax.axis_index("gz") * size_x + lax.axis_index("gx")
    place = jnp.stack(
        [
            lax.axis_index("gy") * TILE - TILE,
            tile * TILE - TILE,
            jnp.int32(size_y * TILE),
            jnp.int32(tiles * TILE),
        ]
    ).astype(jnp.int32)
    options = lambda size, cost: dict(
        compiler_params=pltpu.CompilerParams(vmem_limit_bytes=size * 2**20),
        cost_estimate=pl.CostEstimate(flops=cost, bytes_accessed=0, transcendentals=0),
    )
    ready = setup(place, middle, shallow_material, deep_material, **options(20, 2**27))
    result = swap(lines(middle, shallow_source, deep_source, ready, **options(32, 2**27)))
    return unpack(result, residual.shape)


def solution(mesh):
    return jax.shard_map(
        per_device,
        mesh=mesh,
        in_specs=(
            P("period", None, "gx", "gy", "gz"),
            P("gx", "gy", "gz"),
            P(None, "gx", "gy", "gz"),
            P("period"),
        ),
        out_specs=P("period", None, "gx", "gy", "gz"),
        check_vma=False,
    )
```

```python
import jax
import jax.numpy as jnp
from jax import lax
from jax.experimental import pallas as pl
from jax.experimental.pallas import tpu as pltpu
from jax.sharding import PartitionSpec as P


aspect = 2.0
face_weight = (1.0 / (aspect * aspect), 1.0, 1.0)
mass_factor = (aspect * aspect, 1.0, 1.0)
stiff_weight = (
    2.0 * (face_weight[1] + face_weight[2]),
    2.0 * (face_weight[0] + face_weight[2]),
    2.0 * (face_weight[0] + face_weight[1]),
)
edge_damping = 0.6
shift_ratio = 0.0001
shift_added = 0.05
coarse_scale = (0.5625, 0.1875, 0.1875)

f32 = jnp.float32
TILE = 8
ROWS = 3 * TILE
DEPTH = 32
HALF = TILE // 2


def lanes(shape):
    return lax.broadcasted_iota(jnp.int32, shape, 1)


def turned(values):
    gap = jnp.zeros((DEPTH - ROWS, 128), f32)
    stacked = jnp.concatenate([piece for value in values for piece in (value, gap)], axis=0).T
    return [stacked[DEPTH * g : DEPTH * g + ROWS] for g in range(4)]


def loop(count, body, carry, unroll=1, reverse=False):
    def step(turn, state):
        for part in range(unroll):
            index = turn * unroll + part
            state = body(count - 1 - index if reverse else index, state)
        return state

    return lax.fori_loop(0, count // unroll, step, carry)


def y_next(v, by=1):
    return pltpu.roll(v, v.shape[0] - by, 0)


def y_back(v, by=1):
    return pltpu.roll(v, by, 0)


def z_next(v, by=1):
    return pltpu.roll(v, 128 - by, 1)


def z_back(v, by=1):
    return pltpu.roll(v, by, 1)


row_next, row_back, lane_next, lane_back = y_next, y_back, z_next, z_back


def pack_body(residual, classes, edge_mask, class_weight, out):
    thick = classes.shape[0]
    slots = []
    for i in range(thick):
        labels = classes[i]
        cells = jnp.zeros(labels.shape, f32)
        for label in range(class_weight.shape[0]):
            cells = jnp.where(labels == label, class_weight[label], cells)
        slots.append(cells)
    for comp in range(3):
        slots += [(1 - edge_mask[comp, i]).astype(f32) for i in range(thick)]
    for part in range(2):
        for comp in range(3):
            slots += [residual[part, comp, i] for i in range(thick)]
    block = 0
    for start in range(0, len(slots), 16):
        group = jnp.concatenate(slots[start : start + 16], axis=0)
        block = send_group(group, lambda target: target, out, block)


def send_group(group, device, out, block):
    half = HALF
    if group.shape[0] == 128:
        moved = group.T
        parts = 2
    else:
        moved = jnp.concatenate([group, pltpu.roll(group, 128 - half, 1)], axis=0).T
        parts = 1
    for target in range(16):
        place = device(target)
        if place is not None:
            for part in range(parts):
                row = TILE * target + half * part
                out[place, block + part] = moved[row : row + half]
    return block + parts


def receive_group(blocks, block, full):
    half = HALF
    gap = jnp.zeros((half, 128), f32)
    rows = []
    for source in range(16):
        rows.append(blocks(source, block))
        rows.append(blocks(source, block + 1) if full else gap)
    moved = jnp.concatenate(rows, axis=0).T
    if full:
        return moved
    upper = pltpu.roll(moved[64:], half, 1)
    return jnp.where(lanes((64, 128)) % TILE < half, moved[:64], upper)


def unpack_body(packed, out):
    for part in range(2):
        moved = receive_group(lambda source, block: packed[source, block], 2 * part, part == 0)
        for slot in range(moved.shape[0] // TILE):
            field, i = divmod(16 * part + slot, 4)
            out[field // 3, field % 3, i] = moved[TILE * slot : TILE * slot + TILE]


def pad_low(ref, field):
    lane = lanes((ROWS, 128))
    ref[field, 0] = jnp.where(lane < DEPTH, 0.0, pltpu.roll(ref[field, 16], DEPTH, 1))


def pad_high(ref, field):
    lane = lanes((ROWS, 128))
    ref[field, 17] = jnp.where(
        lane >= 128 - DEPTH, 0.0, pltpu.roll(ref[field, 1], 128 - DEPTH, 1)
    )


def spread_out(windows, groups, put):
    gap = jnp.zeros((HALF, 128), f32)

    def step(a, state):
        for y in range(3):
            for part, full in enumerate(groups):

                def blocks(p, block):
                    g, t = divmod(p, 4)
                    if t == 3:
                        return gap
                    ref, first = windows[t]
                    return ref[y * 16 + 4 * g + a, first + block]

                moved = receive_group(blocks, 2 * part, full)
                for slot in range(moved.shape[0] // TILE):
                    field, i = divmod(16 * part + slot, 4)
                    put(field, 4 * a + i, y, moved[TILE * slot : TILE * slot + TILE])
        return state

    loop(4, step, 0, unroll=2)


def setup_body(
    place, middle, shallow, deep, free_out, M, Dm, KW, CW, FI, FB, FQ, CI, CB, CQ, cells
):
    extent_y, extent_z = place[2], place[3]
    shape = (ROWS, 128)
    lane = lanes(shape)
    row = lax.broadcasted_iota(jnp.int32, shape, 0)
    at_y = lane % DEPTH + place[0]
    at_z = row + place[1]
    inside = jnp.where(
        (at_y >= 0) & (at_y < extent_y) & (at_z >= 0) & (at_z < extent_z), 1.0, 0.0
    ).astype(f32)
    coarse_inside = jnp.where(row % 2 == 0, inside, row_back(inside))
    even_row = row % 2 == 0

    def put(field, level, y, values):
        if field == 0:
            cells[0, level + 1, TILE * y : TILE * y + TILE, :] = values
        else:
            free_out[field - 1, level, TILE * y : TILE * y + TILE, :] = values

    spread_out(((shallow, 0), (middle, 0), (deep, 0)), (True,), put)
    pad_low(cells, 0)

    def coefficients(l, state):
        c = cells[0, l + 1]
        cx = cells[0, l]
        cy = y_back(c)
        cz = z_back(c)
        averages = (
            0.25 * (((c + cy) + cz) + z_back(cy)),
            0.25 * (((c + cx) + cz) + z_back(cx)),
            0.25 * (((c + cx) + cy) + y_back(cx)),
        )
        for d in range(3):
            free = free_out[d, l]
            masses = mass_factor[d] * averages[d] * free
            diagonal = stiff_weight[d] + masses
            M[d, l] = masses
            Dm[d, l] = edge_damping * free / diagonal
            stiff = diagonal * free
            for g, values in enumerate(turned([masses, stiff, stiff, stiff])):
                KW[d, 16 * g + l + 1] = values
        return state

    loop(16, coefficients, 0, unroll=8)

    for d in range(3):
        KW[d, 0] = jnp.zeros(shape, f32)

    nothing = jnp.zeros(shape, f32)
    CW[0, 0] = nothing

    def diagonals(x, state):
        w1b, w1, w2, w3 = KW[0, x], KW[0, x + 1], KW[1, x + 1], KW[2, x + 1]
        total = ((((w1 + w1b) + w3) + row_back(w3)) + w2) + lane_back(w2)
        FI[x] = (1.0 + shift_ratio) * total + shift_added
        for d, w in enumerate((w1, w2, w3)):
            pair = w + row_next(w)
            pair = jnp.where(even_row, pair, row_back(pair))
            CW[d, x + 1] = coarse_scale[d] * (pair + lane_next(pair))
        return state

    def coarse_diagonals(x, state):
        w1b, w1, w2, w3 = CW[0, x], CW[0, x + 1], CW[1, x + 1], CW[2, x + 1]
        total = ((((w1 + w1b) + w3) + row_back(w3, 2)) + w2) + lane_back(w2, 2)
        CI[x] = (1.0 + shift_ratio) * total + shift_added
        return state

    loop(64, diagonals, 0, unroll=16)
    loop(64, coarse_diagonals, 0, unroll=16)

    def factors(x, state):
        fine_before, coarse_before = state
        w1b, c1b = KW[0, x], CW[0, x]
        inverse = inside / (FI[x] - w1b * fine_before)
        coarse_inverse = coarse_inside / (CI[x] - c1b * coarse_before)
        FI[x] = inverse
        CI[x] = coarse_inverse
        FB[x] = w1b * inverse
        CB[x] = c1b * coarse_inverse
        quotient = KW[0, x + 1] * inverse
        coarse_quotient = CW[0, x + 1] * coarse_inverse
        FQ[x] = quotient
        CQ[x] = coarse_quotient
        return quotient, coarse_quotient

    loop(64, factors, (nothing, nothing), unroll=2)


def line_body(
    middle,
    shallow,
    deep,
    free,
    M,
    Dm,
    KW,
    CW,
    FI,
    FB,
    FQ,
    CI,
    CB,
    CQ,
    out,
    W,
    E,
    Rm,
    NS,
    SM,
    CS,
    TY,
    CM,
    OUT,
):
    shape = (ROWS, 128)
    even_row = lax.broadcasted_iota(jnp.int32, shape, 0) % 2 == 0
    even_lane = lanes(shape) % 2 == 0
    nothing = jnp.zeros(shape, f32)

    def put(field, level, y, values):
        rows = slice(TILE * y, TILE * y + TILE)
        source = values * free[field % 3, level, rows, :]
        W[field, level, rows, :] = source
        E[field, level + 1, rows, :] = source * Dm[field % 3, level, rows, :]

    spread_out(((shallow, 0), (middle, 2), (deep, 0)), (True, False), put)

    def side_fluxes(part, l):
        e1, e2, e3 = (E[3 * part + d, l] for d in range(3))
        b2 = face_weight[1] * ((z_next(e1) - e1) - (E[3 * part + 2, l + 1] - e3))
        b3 = face_weight[2] * ((E[3 * part + 1, l + 1] - e2) - (y_next(e1) - e1))
        return b2, b3

    def curl(part, l, before):
        e1, e2, e3 = (E[3 * part + d, l] for d in range(3))
        b2, b3 = side_fluxes(part, l)
        b1 = face_weight[0] * ((y_next(e3) - e3) - (z_next(e2) - e2))
        b2_before, b3_before = before
        results = (
            (z_back(b2) - b2) - (y_back(b3) - b3) + M[0, l - 1] * e1,
            (b3_before - b3) - (z_back(b1) - b1) + M[1, l - 1] * e2,
            (y_back(b1) - b1) - (b2_before - b2) + M[2, l - 1] * e3,
        )
        return results, (b2, b3)

    for field in range(6):
        pad_low(E, field)
        pad_high(E, field)

    def first_remainder(l, state):
        after = []
        for part in range(2):
            results, fluxes = curl(part, l + 1, state[part])
            after.append(fluxes)
            for d in range(3):
                Rm[3 * part + d, l + 1] = (
                    W[3 * part + d, l] - results[d] * free[d, l]
                )
        return tuple(after)

    loop(16, first_remainder, (side_fluxes(0, 0), side_fluxes(1, 0)), unroll=4)
    pad_low(Rm, 0)
    pad_low(Rm, 3)

    def to_nodes(l, state):
        for part in range(2):
            r1, r2, r3 = (Rm[3 * part + d, l + 1] for d in range(3))
            r1b = Rm[3 * part, l]
            r2b = y_back(r2)
            r3b = z_back(r3)
            members = [
                ((r1b - r1) + (r2b - r2)) + (r3b - r3),
                0.5 * (r1 + r1b),
                0.5 * (r2 + r2b),
                0.5 * (r3 + r3b),
            ]
            for g, values in enumerate(turned(members)):
                NS[part, 16 * g + l] = values
        return state

    loop(16, to_nodes, 0, unroll=8)

    def eliminate(source, inverse, back, parts, unroll=4):
        def step(x, state):
            scale, couple = inverse[x], back[x]
            sources = source(x)
            after = []
            for part in range(parts):
                value = sources[part] * scale + couple * state[part]
                TY[part, x] = value
                after.append(value)
            return tuple(after)

        loop(64, step, (nothing,) * parts, unroll=unroll)

    def substitute(quotient, parts, then, unroll):
        def step(x, state):
            factor = quotient[x]
            after = tuple(TY[part, x] + factor * state[part] for part in range(parts))
            then(x, *after)
            return after

        loop(64, step, (nothing,) * parts, unroll=unroll, reverse=True)

    def sides(v, w2, w3, by):
        return ((w3 * row_next(v, by) + row_back(w3 * v, by)) + w2 * lane_next(v, by)) + lane_back(
            w2 * v, by
        )

    def after_smoothing(x, *values):
        halved = []
        for part, value in enumerate(values):
            SM[part, x] = value
            residue = sides(value, KW[1, x + 1], KW[2, x + 1], 1)
            halved.append(residue + 0.5 * (row_back(residue) + row_next(residue)))
        CM[0, x] = jnp.where(even_row, halved[0], row_back(halved[1]))

    def coarse_source(x):
        merged = CM[0, x]
        value = merged + 0.5 * (lane_back(merged) + lane_next(merged))
        CS[0, x] = value
        return (value,)

    def after_coarse(x, value):
        CM[0, x] = CS[0, x] + sides(value, CW[1, x + 1], CW[2, x + 1], 2)

    def after_correction(x, value):
        CS[0, x] = jnp.where(even_lane, value, 0.5 * (lane_back(value) + lane_next(value)))

    def corrected_source(x):
        wide = CS[0, x]
        above = row_next(wide)
        corrections = (
            jnp.where(even_row, wide, 0.5 * (row_back(wide) + above)),
            jnp.where(even_row, above, 0.5 * (wide + row_next(wide, 2))),
        )
        return tuple(
            NS[part, x] + sides(SM[part, x] + corrections[part], KW[1, x + 1], KW[2, x + 1], 1)
            for part in range(2)
        )

    def after_potential(x, *values):
        for part in range(2):
            NS[part, x] = values[part]

    eliminate(lambda x: (NS[0, x], NS[1, x]), FI, FB, 2)
    substitute(FQ, 2, after_smoothing, 16)
    eliminate(coarse_source, CI, CB, 1, 16)
    substitute(CQ, 1, after_coarse, 16)
    eliminate(lambda x: (CM[0, x],), CI, CB, 1)
    substitute(CQ, 1, after_correction, 16)
    eliminate(corrected_source, FI, FB, 2, 16)
    substitute(FQ, 2, after_potential, 4)

    def from_nodes(l, state):
        for part in range(2):
            p0, p1, p2, p3 = turned([NS[part, 16 * g + l] for g in range(4)])
            Rm[3 * part, l + 1] = p0
            Rm[3 * part + 1, l + 1] = p1
            for d, (g_part, h_part) in (
                (1, (y_next(p0) - p0, 0.5 * (p2 + y_next(p2)))),
                (2, (z_next(p0) - p0, 0.5 * (p3 + z_next(p3)))),
            ):
                E[3 * part + d, l + 1] = (
                    E[3 * part + d, l + 1] + (g_part + h_part) * free[d, l]
                )
        return state

    loop(16, from_nodes, 0, unroll=8)
    for part in range(2):
        pad_high(Rm, 3 * part)
        pad_high(Rm, 3 * part + 1)

    def second_first(l, state):
        for part in range(2):
            p0, p1 = Rm[3 * part, l + 1], Rm[3 * part + 1, l + 1]
            g_part = Rm[3 * part, l + 2] - p0
            h_part = 0.5 * (p1 + Rm[3 * part + 1, l + 2])
            E[3 * part, l + 1] = E[3 * part, l + 1] + (g_part + h_part) * free[0, l]
        return state

    loop(16, second_first, 0, unroll=4)
    for field in range(6):
        pad_low(E, field)
        pad_high(E, field)

    def last_step(l, state):
        after = []
        for part in range(2):
            results, fluxes = curl(part, l + 1, state[part])
            after.append(fluxes)
            for d in range(3):
                field = 3 * part + d
                remainder = W[field, l] - results[d] * free[d, l]
                value = E[field, l + 1] + Dm[d, l] * remainder
                OUT[field, l] = value[TILE : 2 * TILE]
        return tuple(after)

    loop(16, last_step, (side_fluxes(0, 0), side_fluxes(1, 0)), unroll=8)

    def gather_up(a, state):
        slots = [OUT[field, 4 * a + i] for field in range(6) for i in range(4)]
        block = 0
        for start in (0, 16):
            group = jnp.concatenate(slots[start : start + 16], axis=0)
            block = send_group(
                group, lambda p: p // 4 * 4 + a if p % 4 == 1 else None, out, block
            )
        return state

    loop(4, gather_up, 0, unroll=4)


def vmem():
    return pl.BlockSpec(memory_space=pltpu.VMEM)


def smem():
    return pl.BlockSpec(memory_space=pltpu.SMEM)


def pack(residual, classes, edge_mask, class_weight, **options):
    return pl.pallas_call(
        pack_body,
        out_shape=resident(16, 5, HALF, 128),
        in_specs=[vmem(), vmem(), vmem(), smem()],
        out_specs=vmem(),
        name="pack",
        **options,
    )(residual, classes, edge_mask, class_weight)


def unpack(packed, shape, **options):
    return pl.pallas_call(
        unpack_body,
        out_shape=jax.ShapeDtypeStruct(shape, f32),
        in_specs=[vmem()],
        out_specs=vmem(),
        name="unpack",
        **options,
    )(packed)


def resident(*shape):
    return pltpu.VMEM(shape, f32)


def setup(place, middle, shallow, deep, **options):
    line = resident(64, ROWS, 128)
    edge = resident(3, 16, ROWS, 128)
    weights = resident(3, 65, ROWS, 128)
    return pl.pallas_call(
        setup_body,
        out_shape=[edge, edge, edge, weights, weights] + [line] * 6,
        in_specs=[smem(), vmem(), vmem(), vmem()],
        out_specs=[vmem()] * 11,
        scratch_shapes=[resident(1, 18, ROWS, 128)],
        name="setup",
        **options,
    )(place, middle, shallow, deep)


def lines(middle, shallow, deep, ready, **options):
    edge = lambda count, levels: resident(count, levels, ROWS, 128)
    pair = resident(2, 64, ROWS, 128)
    return pl.pallas_call(
        line_body,
        out_shape=resident(16, 3, HALF, 128),
        in_specs=[vmem()] * (3 + len(ready)),
        out_specs=vmem(),
        scratch_shapes=[
            edge(6, 16),
            edge(6, 18),
            edge(6, 18),
            pair,
            pair,
            resident(1, 64, ROWS, 128),
            pair,
            resident(1, 64, ROWS, 128),
            resident(6, 16, TILE, 128),
        ],
        name="lines",
        **options,
    )(middle, shallow, deep, *ready)


def swap(values):
    return lax.all_to_all(values, "gx", 0, 0, tiled=True)


def per_device(residual, classes, edge_mask, class_weight):
    size_x, size_y, size_z = (lax.axis_size(name) for name in ("gx", "gy", "gz"))
    axes = ("gx", "gy", "gz")
    tiles = size_x * size_z

    def position(y, tile):
        z, x = divmod(tile, size_x)
        return (x * size_y + y) * size_z + z

    def from_side(values, step_y, step_tile):
        pairs = [
            (position(y, tile), position(y + step_y, tile + step_tile))
            for y in range(size_y)
            for tile in range(tiles)
            if 0 <= y + step_y < size_y and 0 <= tile + step_tile < tiles
        ]
        return lax.ppermute(values, axes, pairs)

    own = swap(
        pack(
            residual,
            classes,
            edge_mask,
            class_weight,
        )
    )
    middle = jnp.concatenate([from_side(own, 1, 0), own, from_side(own, -1, 0)], axis=0)
    material, source = middle[:, :2], middle[:, 2:]
    shallow_material = from_side(material, 0, 1)
    deep_material = from_side(material, 0, -1)
    shallow_source = from_side(source, 0, 1)
    deep_source = from_side(source, 0, -1)
    tile = lax.axis_index("gz") * size_x + lax.axis_index("gx")
    place = jnp.stack(
        [
            lax.axis_index("gy") * TILE - TILE,
            tile * TILE - TILE,
            jnp.int32(size_y * TILE),
            jnp.int32(tiles * TILE),
        ]
    ).astype(jnp.int32)
    options = lambda size, cost: dict(
        compiler_params=pltpu.CompilerParams(vmem_limit_bytes=size * 2**20),
        cost_estimate=pl.CostEstimate(flops=cost, bytes_accessed=0, transcendentals=0),
    )
    ready = setup(place, middle, shallow_material, deep_material, **options(20, 2**27))
    result = swap(lines(middle, shallow_source, deep_source, ready, **options(32, 2**27)))
    result = pltpu.with_memory_space_constraint(result, pltpu.VMEM)
    return unpack(result, residual.shape)


def solution(mesh):
    return jax.shard_map(
        per_device,
        mesh=mesh,
        in_specs=(
            P("period", None, "gx", "gy", "gz"),
            P("gx", "gy", "gz"),
            P(None, "gx", "gy", "gz"),
            P("period"),
        ),
        out_specs=P("period", None, "gx", "gy", "gz"),
        check_vma=False,
    )
```

```python
import functools

import jax
import jax.numpy as jnp
from jax import lax
from jax.experimental import pallas as pl
from jax.experimental.pallas import tpu as pltpu
from jax.sharding import PartitionSpec as P


aspect = 2.0
face_weight = (1.0 / (aspect * aspect), 1.0, 1.0)
mass_factor = (aspect * aspect, 1.0, 1.0)
stiff_weight = (
    2.0 * (face_weight[1] + face_weight[2]),
    2.0 * (face_weight[0] + face_weight[2]),
    2.0 * (face_weight[0] + face_weight[1]),
)
edge_damping = 0.6
shift_ratio = 0.0001
shift_added = 0.05
coarse_scale = (0.5625, 0.1875, 0.1875)

f32 = jnp.float32
TILE = 8
ROWS = 3 * TILE
DEPTH = 32
HALF = TILE // 2


def lanes(shape):
    return lax.broadcasted_iota(jnp.int32, shape, 1)


def turned(values):
    gap = jnp.zeros((DEPTH - ROWS, 128), f32)
    stacked = jnp.concatenate([piece for value in values for piece in (value, gap)], axis=0).T
    return [stacked[DEPTH * g : DEPTH * g + ROWS] for g in range(4)]


def loop(count, body, carry, unroll=1, reverse=False):
    def step(turn, state):
        for part in range(unroll):
            index = turn * unroll + part
            state = body(count - 1 - index if reverse else index, state)
        return state

    return lax.fori_loop(0, count // unroll, step, carry)


def y_next(v, by=1):
    return pltpu.roll(v, v.shape[0] - by, 0)


def y_back(v, by=1):
    return pltpu.roll(v, by, 0)


def z_next(v, by=1):
    return pltpu.roll(v, 128 - by, 1)


def z_back(v, by=1):
    return pltpu.roll(v, by, 1)


row_next, row_back, lane_next, lane_back = y_next, y_back, z_next, z_back


def position_facts(place, sizes):
    x, y, z = place[0], place[1], place[2]
    flip = z % 2
    along = x + flip * (sizes[0] - 1 - 2 * x)
    before = jnp.where(along == 0, 1 - flip, flip)
    after = jnp.where(along == sizes[0] - 1, 1 - flip, flip)
    corner_y = y * TILE - TILE
    corner_z = (z * sizes[0] + along) * TILE - TILE
    return corner_y, corner_z, (before, flip, after)


def mirrored(place, index, count):
    return index + place[2] % 2 * (count - 1 - 2 * index)


def pack_body(place, residual, classes, edge_mask, class_weight, out):
    thick = classes.shape[0]
    slots = []
    for i in range(thick):
        labels = classes[i]
        cells = jnp.zeros(labels.shape, f32)
        for label in range(class_weight.shape[0]):
            cells = jnp.where(labels == label, class_weight[label], cells)
        slots.append(cells)
    for comp in range(3):
        slots += [(1 - edge_mask[comp, i]).astype(f32) for i in range(thick)]
    for part in range(2):
        for comp in range(3):
            slots += [residual[part, comp, i] for i in range(thick)]
    block = 0
    for start in range(0, len(slots), 16):
        group = jnp.concatenate(slots[start : start + 16], axis=0)
        block = send_group(group, lambda target: mirrored(place, target, 16), out, block)


def send_group(group, device, out, block):
    half = HALF
    if group.shape[0] == 128:
        moved = group.T
        parts = 2
    else:
        moved = jnp.concatenate([group, pltpu.roll(group, 128 - half, 1)], axis=0).T
        parts = 1
    for target in range(16):
        where = device(target)
        if where is not None:
            for part in range(parts):
                row = TILE * target + half * part
                out[where, block + part] = moved[row : row + half]
    return block + parts


def receive_group(blocks, block, full):
    half = HALF
    gap = jnp.zeros((half, 128), f32)
    rows = []
    for source in range(16):
        rows.append(blocks(source, block))
        rows.append(blocks(source, block + 1) if full else gap)
    moved = jnp.concatenate(rows, axis=0).T
    if full:
        return moved
    upper = pltpu.roll(moved[64:], half, 1)
    return jnp.where(lanes((64, 128)) % TILE < half, moved[:64], upper)


def unpack_body(place, packed, out):
    for part in range(2):
        moved = receive_group(
            lambda window, block: packed[mirrored(place, window, 16), block], 2 * part, part == 0
        )
        for slot in range(moved.shape[0] // TILE):
            field, i = divmod(16 * part + slot, 4)
            out[field // 3, field % 3, i] = moved[TILE * slot : TILE * slot + TILE]


def pad_low(ref, field):
    lane = lanes((ROWS, 128))
    ref[field, 0] = jnp.where(lane < DEPTH, 0.0, pltpu.roll(ref[field, 16], DEPTH, 1))


def pad_high(ref, field):
    lane = lanes((ROWS, 128))
    ref[field, 17] = jnp.where(
        lane >= 128 - DEPTH, 0.0, pltpu.roll(ref[field, 1], 128 - DEPTH, 1)
    )


def spread_out(windows, groups, put):
    gap = jnp.zeros((HALF, 128), f32)

    def step(a, state):
        for y in range(3):
            for part, full in enumerate(groups):

                def blocks(p, block):
                    g, t = divmod(p, 4)
                    if t == 3:
                        return gap
                    ref, first, flag = windows[t]
                    turn = y + flag * (2 - 2 * y)
                    return ref[turn * 16 + 4 * g + a, first + block]

                moved = receive_group(blocks, 2 * part, full)
                for slot in range(moved.shape[0] // TILE):
                    field, i = divmod(16 * part + slot, 4)
                    put(field, 4 * a + i, y, moved[TILE * slot : TILE * slot + TILE])
        return state

    loop(4, step, 0, unroll=2)


def setup_body(
    sizes,
    place,
    middle,
    shallow,
    deep,
    free_out,
    M,
    Dm,
    KW,
    CW,
    FI,
    FB,
    FQ,
    CI,
    CB,
    CQ,
    cells,
):
    corner_y, corner_z, orders = position_facts(place, sizes)
    extent_y, extent_z = sizes[1] * TILE, sizes[0] * sizes[2] * TILE
    shape = (ROWS, 128)
    lane = lanes(shape)
    row = lax.broadcasted_iota(jnp.int32, shape, 0)
    at_y = lane % DEPTH + corner_y
    at_z = row + corner_z
    inside = jnp.where(
        (at_y >= 0) & (at_y < extent_y) & (at_z >= 0) & (at_z < extent_z), 1.0, 0.0
    ).astype(f32)
    coarse_inside = jnp.where(row % 2 == 0, inside, row_back(inside))
    even_row = row % 2 == 0

    def put(field, level, y, values):
        if field == 0:
            cells[0, level + 1, TILE * y : TILE * y + TILE, :] = values
        else:
            free_out[field - 1, level, TILE * y : TILE * y + TILE, :] = values

    spread_out(
        ((shallow, 0, orders[0]), (middle, 0, orders[1]), (deep, 0, orders[2])), (True,), put
    )
    pad_low(cells, 0)

    def coefficients(l, state):
        c = cells[0, l + 1]
        cx = cells[0, l]
        cy = y_back(c)
        cz = z_back(c)
        averages = (
            0.25 * (((c + cy) + cz) + z_back(cy)),
            0.25 * (((c + cx) + cz) + z_back(cx)),
            0.25 * (((c + cx) + cy) + y_back(cx)),
        )
        for d in range(3):
            free = free_out[d, l]
            masses = mass_factor[d] * averages[d] * free
            diagonal = stiff_weight[d] + masses
            M[d, l] = masses
            Dm[d, l] = edge_damping * free / diagonal
            stiff = diagonal * free
            for g, values in enumerate(turned([masses, stiff, stiff, stiff])):
                KW[d, 16 * g + l + 1] = values
        return state

    loop(16, coefficients, 0, unroll=8)

    for d in range(3):
        KW[d, 0] = jnp.zeros(shape, f32)

    nothing = jnp.zeros(shape, f32)
    CW[0, 0] = nothing

    def diagonals(x, state):
        w1b, w1, w2, w3 = KW[0, x], KW[0, x + 1], KW[1, x + 1], KW[2, x + 1]
        total = ((((w1 + w1b) + w3) + row_back(w3)) + w2) + lane_back(w2)
        FI[x] = (1.0 + shift_ratio) * total + shift_added
        for d, w in enumerate((w1, w2, w3)):
            pair = w + row_next(w)
            pair = jnp.where(even_row, pair, row_back(pair))
            CW[d, x + 1] = coarse_scale[d] * (pair + lane_next(pair))
        return state

    def coarse_diagonals(x, state):
        w1b, w1, w2, w3 = CW[0, x], CW[0, x + 1], CW[1, x + 1], CW[2, x + 1]
        total = ((((w1 + w1b) + w3) + row_back(w3, 2)) + w2) + lane_back(w2, 2)
        CI[x] = (1.0 + shift_ratio) * total + shift_added
        return state

    loop(64, diagonals, 0, unroll=16)
    loop(64, coarse_diagonals, 0, unroll=16)

    def factors(x, state):
        fine_before, coarse_before = state
        w1b, c1b = KW[0, x], CW[0, x]
        inverse = inside / (FI[x] - w1b * fine_before)
        coarse_inverse = coarse_inside / (CI[x] - c1b * coarse_before)
        FI[x] = inverse
        CI[x] = coarse_inverse
        FB[x] = w1b * inverse
        CB[x] = c1b * coarse_inverse
        quotient = KW[0, x + 1] * inverse
        coarse_quotient = CW[0, x + 1] * coarse_inverse
        FQ[x] = quotient
        CQ[x] = coarse_quotient
        return quotient, coarse_quotient

    loop(64, factors, (nothing, nothing), unroll=2)


def line_body(
    sizes,
    place,
    middle,
    shallow,
    deep,
    free,
    M,
    Dm,
    KW,
    CW,
    FI,
    FB,
    FQ,
    CI,
    CB,
    CQ,
    out,
    W,
    E,
    Rm,
    NS,
    SM,
    CS,
    TY,
    CM,
    OUT,
):
    shape = (ROWS, 128)
    orders = position_facts(place, sizes)[2]
    even_row = lax.broadcasted_iota(jnp.int32, shape, 0) % 2 == 0
    even_lane = lanes(shape) % 2 == 0
    nothing = jnp.zeros(shape, f32)

    def put(field, level, y, values):
        rows = slice(TILE * y, TILE * y + TILE)
        source = values * free[field % 3, level, rows, :]
        W[field, level, rows, :] = source
        E[field, level + 1, rows, :] = source * Dm[field % 3, level, rows, :]

    spread_out(
        ((shallow, 0, orders[0]), (middle, 2, orders[1]), (deep, 0, orders[2])),
        (True, False),
        put,
    )

    def side_fluxes(part, l):
        e1, e2, e3 = (E[3 * part + d, l] for d in range(3))
        b2 = face_weight[1] * ((z_next(e1) - e1) - (E[3 * part + 2, l + 1] - e3))
        b3 = face_weight[2] * ((E[3 * part + 1, l + 1] - e2) - (y_next(e1) - e1))
        return b2, b3

    def curl(part, l, before):
        e1, e2, e3 = (E[3 * part + d, l] for d in range(3))
        b2, b3 = side_fluxes(part, l)
        b1 = face_weight[0] * ((y_next(e3) - e3) - (z_next(e2) - e2))
        b2_before, b3_before = before
        results = (
            (z_back(b2) - b2) - (y_back(b3) - b3) + M[0, l - 1] * e1,
            (b3_before - b3) - (z_back(b1) - b1) + M[1, l - 1] * e2,
            (y_back(b1) - b1) - (b2_before - b2) + M[2, l - 1] * e3,
        )
        return results, (b2, b3)

    for field in range(6):
        pad_low(E, field)
        pad_high(E, field)

    def first_remainder(l, state):
        after = []
        for part in range(2):
            results, fluxes = curl(part, l + 1, state[part])
            after.append(fluxes)
            for d in range(3):
                Rm[3 * part + d, l + 1] = (
                    W[3 * part + d, l] - results[d] * free[d, l]
                )
        return tuple(after)

    loop(16, first_remainder, (side_fluxes(0, 0), side_fluxes(1, 0)), unroll=4)
    pad_low(Rm, 0)
    pad_low(Rm, 3)

    def to_nodes(l, state):
        for part in range(2):
            r1, r2, r3 = (Rm[3 * part + d, l + 1] for d in range(3))
            r1b = Rm[3 * part, l]
            r2b = y_back(r2)
            r3b = z_back(r3)
            members = [
                ((r1b - r1) + (r2b - r2)) + (r3b - r3),
                0.5 * (r1 + r1b),
                0.5 * (r2 + r2b),
                0.5 * (r3 + r3b),
            ]
            for g, values in enumerate(turned(members)):
                NS[part, 16 * g + l] = values
        return state

    loop(16, to_nodes, 0, unroll=8)

    def eliminate(source, inverse, back, parts, unroll=4):
        def step(x, state):
            scale, couple = inverse[x], back[x]
            sources = source(x)
            after = []
            for part in range(parts):
                value = sources[part] * scale + couple * state[part]
                TY[part, x] = value
                after.append(value)
            return tuple(after)

        loop(64, step, (nothing,) * parts, unroll=unroll)

    def substitute(quotient, parts, then, unroll):
        def step(x, state):
            factor = quotient[x]
            after = tuple(TY[part, x] + factor * state[part] for part in range(parts))
            then(x, *after)
            return after

        loop(64, step, (nothing,) * parts, unroll=unroll, reverse=True)

    def sides(v, w2, w3, by):
        return ((w3 * row_next(v, by) + row_back(w3 * v, by)) + w2 * lane_next(v, by)) + lane_back(
            w2 * v, by
        )

    def after_smoothing(x, *values):
        halved = []
        for part, value in enumerate(values):
            SM[part, x] = value
            residue = sides(value, KW[1, x + 1], KW[2, x + 1], 1)
            halved.append(residue + 0.5 * (row_back(residue) + row_next(residue)))
        CM[0, x] = jnp.where(even_row, halved[0], row_back(halved[1]))

    def coarse_source(x):
        merged = CM[0, x]
        value = merged + 0.5 * (lane_back(merged) + lane_next(merged))
        CS[0, x] = value
        return (value,)

    def after_coarse(x, value):
        CM[0, x] = CS[0, x] + sides(value, CW[1, x + 1], CW[2, x + 1], 2)

    def after_correction(x, value):
        CS[0, x] = jnp.where(even_lane, value, 0.5 * (lane_back(value) + lane_next(value)))

    def corrected_source(x):
        wide = CS[0, x]
        above = row_next(wide)
        corrections = (
            jnp.where(even_row, wide, 0.5 * (row_back(wide) + above)),
            jnp.where(even_row, above, 0.5 * (wide + row_next(wide, 2))),
        )
        return tuple(
            NS[part, x] + sides(SM[part, x] + corrections[part], KW[1, x + 1], KW[2, x + 1], 1)
            for part in range(2)
        )

    def after_potential(x, *values):
        for part in range(2):
            NS[part, x] = values[part]

    eliminate(lambda x: (NS[0, x], NS[1, x]), FI, FB, 2)
    substitute(FQ, 2, after_smoothing, 16)
    eliminate(coarse_source, CI, CB, 1, 16)
    substitute(CQ, 1, after_coarse, 16)
    eliminate(lambda x: (CM[0, x],), CI, CB, 1)
    substitute(CQ, 1, after_correction, 16)
    eliminate(corrected_source, FI, FB, 2, 16)
    substitute(FQ, 2, after_potential, 4)

    def from_nodes(l, state):
        for part in range(2):
            p0, p1, p2, p3 = turned([NS[part, 16 * g + l] for g in range(4)])
            Rm[3 * part, l + 1] = p0
            Rm[3 * part + 1, l + 1] = p1
            for d, (g_part, h_part) in (
                (1, (y_next(p0) - p0, 0.5 * (p2 + y_next(p2)))),
                (2, (z_next(p0) - p0, 0.5 * (p3 + z_next(p3)))),
            ):
                E[3 * part + d, l + 1] = (
                    E[3 * part + d, l + 1] + (g_part + h_part) * free[d, l]
                )
        return state

    loop(16, from_nodes, 0, unroll=8)
    for part in range(2):
        pad_high(Rm, 3 * part)
        pad_high(Rm, 3 * part + 1)

    def second_first(l, state):
        for part in range(2):
            p0, p1 = Rm[3 * part, l + 1], Rm[3 * part + 1, l + 1]
            g_part = Rm[3 * part, l + 2] - p0
            h_part = 0.5 * (p1 + Rm[3 * part + 1, l + 2])
            E[3 * part, l + 1] = E[3 * part, l + 1] + (g_part + h_part) * free[0, l]
        return state

    loop(16, second_first, 0, unroll=4)
    for field in range(6):
        pad_low(E, field)
        pad_high(E, field)

    def last_step(l, state):
        after = []
        for part in range(2):
            results, fluxes = curl(part, l + 1, state[part])
            after.append(fluxes)
            for d in range(3):
                field = 3 * part + d
                remainder = W[field, l] - results[d] * free[d, l]
                value = E[field, l + 1] + Dm[d, l] * remainder
                OUT[field, l] = value[TILE : 2 * TILE]
        return tuple(after)

    loop(16, last_step, (side_fluxes(0, 0), side_fluxes(1, 0)), unroll=8)

    def gather_up(a, state):
        slots = [OUT[field, 4 * a + i] for field in range(6) for i in range(4)]
        block = 0
        for start in (0, 16):
            group = jnp.concatenate(slots[start : start + 16], axis=0)
            block = send_group(
                group, lambda p: p // 4 * 4 + a if p % 4 == 1 else None, out, block
            )
        return state

    loop(4, gather_up, 0, unroll=4)


def vmem():
    return pl.BlockSpec(memory_space=pltpu.VMEM)


def smem():
    return pl.BlockSpec(memory_space=pltpu.SMEM)


def pack(place, residual, classes, edge_mask, class_weight, **options):
    return pl.pallas_call(
        pack_body,
        out_shape=resident(16, 5, HALF, 128),
        in_specs=[smem(), vmem(), vmem(), vmem(), smem()],
        out_specs=vmem(),
        name="pack",
        **options,
    )(place, residual, classes, edge_mask, class_weight)


def unpack(place, packed, shape, **options):
    return pl.pallas_call(
        unpack_body,
        out_shape=jax.ShapeDtypeStruct(shape, f32),
        in_specs=[smem(), vmem()],
        out_specs=vmem(),
        name="unpack",
        **options,
    )(place, packed)


def resident(*shape):
    return pltpu.VMEM(shape, f32)


def setup(sizes, place, middle, shallow, deep, **options):
    line = resident(64, ROWS, 128)
    edge = resident(3, 16, ROWS, 128)
    weights = resident(3, 65, ROWS, 128)
    return pl.pallas_call(
        functools.partial(setup_body, sizes),
        out_shape=[edge, edge, edge, weights, weights] + [line] * 6,
        in_specs=[smem(), vmem(), vmem(), vmem()],
        out_specs=[vmem()] * 11,
        scratch_shapes=[resident(1, 18, ROWS, 128)],
        name="setup",
        **options,
    )(place, middle, shallow, deep)


def lines(sizes, place, middle, shallow, deep, ready, **options):
    edge = lambda count, levels: resident(count, levels, ROWS, 128)
    pair = resident(2, 64, ROWS, 128)
    return pl.pallas_call(
        functools.partial(line_body, sizes),
        out_shape=resident(16, 3, HALF, 128),
        in_specs=[smem()] + [vmem()] * (3 + len(ready)),
        out_specs=vmem(),
        scratch_shapes=[
            edge(6, 16),
            edge(6, 18),
            edge(6, 18),
            pair,
            pair,
            resident(1, 64, ROWS, 128),
            pair,
            resident(1, 64, ROWS, 128),
            resident(6, 16, TILE, 128),
        ],
        name="lines",
        **options,
    )(place, middle, shallow, deep, *ready)


def swap(values):
    return lax.all_to_all(values, "gx", 0, 0, tiled=True)


def per_device(residual, classes, edge_mask, class_weight):
    size_x, size_y, size_z = (lax.axis_size(name) for name in ("gx", "gy", "gz"))
    axes = ("gx", "gy", "gz")
    tiles = size_x * size_z

    def position(y, tile):
        z, x = divmod(tile, size_x)
        if z % 2:
            x = size_x - 1 - x
        return (x * size_y + y) * size_z + z

    def from_side(values, step_y, step_tile):
        pairs = []
        for y in range(size_y):
            for tile in range(tiles):
                next_y = y - step_y if tile // size_x % 2 else y + step_y
                if 0 <= next_y < size_y and 0 <= tile + step_tile < tiles:
                    pairs.append((position(y, tile), position(next_y, tile + step_tile)))
        return lax.ppermute(values, axes, pairs)

    sizes = (size_x, size_y, size_z)
    place = jnp.stack([lax.axis_index(name) for name in axes]).astype(jnp.int32)
    own = swap(pack(place, residual, classes, edge_mask, class_weight))
    middle = jnp.concatenate([from_side(own, 1, 0), own, from_side(own, -1, 0)], axis=0)
    material, source = middle[:, :2], middle[:, 2:]
    shallow_material = from_side(material, 0, 1)
    deep_material = from_side(material, 0, -1)
    shallow_source = from_side(source, 0, 1)
    deep_source = from_side(source, 0, -1)
    options = lambda size, cost: dict(
        compiler_params=pltpu.CompilerParams(vmem_limit_bytes=size * 2**20),
        cost_estimate=pl.CostEstimate(flops=cost, bytes_accessed=0, transcendentals=0),
    )
    ready = setup(sizes, place, middle, shallow_material, deep_material, **options(20, 2**27))
    result = swap(lines(sizes, place, middle, shallow_source, deep_source, ready, **options(32, 2**27)))
    result = pltpu.with_memory_space_constraint(result, pltpu.VMEM)
    return unpack(place, result, residual.shape)


def solution(mesh):
    return jax.shard_map(
        per_device,
        mesh=mesh,
        in_specs=(
            P("period", None, "gx", "gy", "gz"),
            P("gx", "gy", "gz"),
            P(None, "gx", "gy", "gz"),
            P("period"),
        ),
        out_specs=P("period", None, "gx", "gy", "gz"),
        check_vma=False,
    )
```

```python
import functools

import jax
import jax.numpy as jnp
from jax import lax
from jax.experimental import pallas as pl
from jax.experimental.pallas import tpu as pltpu
from jax.sharding import PartitionSpec as P


aspect = 2.0
face_weight = (1.0 / (aspect * aspect), 1.0, 1.0)
mass_factor = (aspect * aspect, 1.0, 1.0)
stiff_weight = (
    2.0 * (face_weight[1] + face_weight[2]),
    2.0 * (face_weight[0] + face_weight[2]),
    2.0 * (face_weight[0] + face_weight[1]),
)
edge_damping = 0.6
shift_ratio = 0.0001
shift_added = 0.05
coarse_scale = (0.5625, 0.1875, 0.1875)

f32 = jnp.float32
TILE = 8
ROWS = 3 * TILE
DEPTH = 32
HALF = TILE // 2
AXES = ("gx", "gy", "gz")


def lanes(shape):
    return lax.broadcasted_iota(jnp.int32, shape, 1)


def turned(values):
    gap = jnp.zeros((DEPTH - ROWS, 128), f32)
    stacked = jnp.concatenate([piece for value in values for piece in (value, gap)], axis=0).T
    return [stacked[DEPTH * g : DEPTH * g + ROWS] for g in range(4)]


def loop(count, body, carry, unroll=1, reverse=False):
    def step(turn, state):
        for part in range(unroll):
            index = turn * unroll + part
            state = body(count - 1 - index if reverse else index, state)
        return state

    return lax.fori_loop(0, count // unroll, step, carry)


def y_next(v, by=1):
    return pltpu.roll(v, v.shape[0] - by, 0)


def y_back(v, by=1):
    return pltpu.roll(v, by, 0)


def z_next(v, by=1):
    return pltpu.roll(v, 128 - by, 1)


def z_back(v, by=1):
    return pltpu.roll(v, by, 1)


row_next, row_back, lane_next, lane_back = y_next, y_back, z_next, z_back


def position_facts(sizes):
    x, y, z = (lax.axis_index(name) for name in AXES)
    flip = z % 2
    along = x + flip * (sizes[0] - 1 - 2 * x)
    before = jnp.where(along == 0, 1 - flip, flip)
    after = jnp.where(along == sizes[0] - 1, 1 - flip, flip)
    corner_y = y * TILE - TILE
    corner_z = (z * sizes[0] + along) * TILE - TILE
    return corner_y, corner_z, (before, flip, after)


def mirrored(flip, index, count):
    return index + flip * (count - 1 - 2 * index)


def pack_body(residual, classes, edge_mask, class_weight, out):
    thick = classes.shape[0]
    flip = lax.axis_index("gz") % 2
    slots = []
    for i in range(thick):
        labels = classes[i]
        cells = jnp.zeros(labels.shape, f32)
        for label in range(class_weight.shape[0]):
            cells = jnp.where(labels == label, class_weight[label], cells)
        slots.append(cells)
    for comp in range(3):
        slots += [(1 - edge_mask[comp, i]).astype(f32) for i in range(thick)]
    for part in range(2):
        for comp in range(3):
            slots += [residual[part, comp, i] for i in range(thick)]
    block = 0
    for start in range(0, len(slots), 16):
        group = jnp.concatenate(slots[start : start + 16], axis=0)
        block = send_group(group, lambda target: mirrored(flip, target, 16), out, block)


def send_group(group, device, out, block):
    half = HALF
    if group.shape[0] == 128:
        moved = group.T
        parts = 2
    else:
        moved = jnp.concatenate([group, pltpu.roll(group, 128 - half, 1)], axis=0).T
        parts = 1
    for target in range(16):
        where = device(target)
        if where is not None:
            for part in range(parts):
                row = TILE * target + half * part
                out[where, block + part] = moved[row : row + half]
    return block + parts


def receive_group(blocks, block, full):
    half = HALF
    gap = jnp.zeros((half, 128), f32)
    rows = []
    for source in range(16):
        rows.append(blocks(source, block))
        rows.append(blocks(source, block + 1) if full else gap)
    moved = jnp.concatenate(rows, axis=0).T
    if full:
        return moved
    upper = pltpu.roll(moved[64:], half, 1)
    return jnp.where(lanes((64, 128)) % TILE < half, moved[:64], upper)


def unpack_body(packed, out):
    flip = lax.axis_index("gz") % 2
    for part in range(2):
        moved = receive_group(
            lambda window, block: packed[mirrored(flip, window, 16), block], 2 * part, part == 0
        )
        for slot in range(moved.shape[0] // TILE):
            field, i = divmod(16 * part + slot, 4)
            out[field // 3, field % 3, i] = moved[TILE * slot : TILE * slot + TILE]


def pad_low(ref, field):
    lane = lanes((ROWS, 128))
    ref[field, 0] = jnp.where(lane < DEPTH, 0.0, pltpu.roll(ref[field, 16], DEPTH, 1))


def pad_high(ref, field):
    lane = lanes((ROWS, 128))
    ref[field, 17] = jnp.where(
        lane >= 128 - DEPTH, 0.0, pltpu.roll(ref[field, 1], 128 - DEPTH, 1)
    )


def spread_out(windows, groups, put):
    gap = jnp.zeros((HALF, 128), f32)

    def step(a, state):
        for y in range(3):
            for part, full in enumerate(groups):

                def blocks(p, block):
                    g, t = divmod(p, 4)
                    if t == 3:
                        return gap
                    ref, first, flag = windows[t]
                    turn = y + flag * (2 - 2 * y)
                    return ref[turn * 16 + 4 * g + a, first + block]

                moved = receive_group(blocks, 2 * part, full)
                for slot in range(moved.shape[0] // TILE):
                    field, i = divmod(16 * part + slot, 4)
                    put(field, 4 * a + i, y, moved[TILE * slot : TILE * slot + TILE])
        return state

    loop(4, step, 0, unroll=2)


def setup_body(
    sizes,
    middle,
    shallow,
    deep,
    free_out,
    M,
    Dm,
    KW,
    CW,
    FI,
    FB,
    FQ,
    CI,
    CB,
    CQ,
    cells,
):
    corner_y, corner_z, orders = position_facts(sizes)
    extent_y, extent_z = sizes[1] * TILE, sizes[0] * sizes[2] * TILE
    shape = (ROWS, 128)
    lane = lanes(shape)
    row = lax.broadcasted_iota(jnp.int32, shape, 0)
    at_y = lane % DEPTH + corner_y
    at_z = row + corner_z
    inside = jnp.where(
        (at_y >= 0) & (at_y < extent_y) & (at_z >= 0) & (at_z < extent_z), 1.0, 0.0
    ).astype(f32)
    coarse_inside = jnp.where(row % 2 == 0, inside, row_back(inside))
    even_row = row % 2 == 0

    def put(field, level, y, values):
        if field == 0:
            cells[0, level + 1, TILE * y : TILE * y + TILE, :] = values
        else:
            free_out[field - 1, level, TILE * y : TILE * y + TILE, :] = values

    spread_out(
        ((shallow, 0, orders[0]), (middle, 0, orders[1]), (deep, 0, orders[2])), (True,), put
    )
    pad_low(cells, 0)

    def coefficients(l, state):
        c = cells[0, l + 1]
        cx = cells[0, l]
        cy = y_back(c)
        cz = z_back(c)
        averages = (
            0.25 * (((c + cy) + cz) + z_back(cy)),
            0.25 * (((c + cx) + cz) + z_back(cx)),
            0.25 * (((c + cx) + cy) + y_back(cx)),
        )
        for d in range(3):
            free = free_out[d, l]
            masses = mass_factor[d] * averages[d] * free
            diagonal = stiff_weight[d] + masses
            M[d, l] = masses
            Dm[d, l] = edge_damping * free / diagonal
            stiff = diagonal * free
            for g, values in enumerate(turned([masses, stiff, stiff, stiff])):
                KW[d, 16 * g + l + 1] = values
        return state

    loop(16, coefficients, 0, unroll=8)

    for d in range(3):
        KW[d, 0] = jnp.zeros(shape, f32)

    nothing = jnp.zeros(shape, f32)
    CW[0, 0] = nothing

    def diagonals(x, state):
        w1b, w1, w2, w3 = KW[0, x], KW[0, x + 1], KW[1, x + 1], KW[2, x + 1]
        total = ((((w1 + w1b) + w3) + row_back(w3)) + w2) + lane_back(w2)
        FI[x] = (1.0 + shift_ratio) * total + shift_added
        for d, w in enumerate((w1, w2, w3)):
            pair = w + row_next(w)
            pair = jnp.where(even_row, pair, row_back(pair))
            CW[d, x + 1] = coarse_scale[d] * (pair + lane_next(pair))
        return state

    def coarse_diagonals(x, state):
        w1b, w1, w2, w3 = CW[0, x], CW[0, x + 1], CW[1, x + 1], CW[2, x + 1]
        total = ((((w1 + w1b) + w3) + row_back(w3, 2)) + w2) + lane_back(w2, 2)
        CI[x] = (1.0 + shift_ratio) * total + shift_added
        return state

    loop(64, diagonals, 0, unroll=16)
    loop(64, coarse_diagonals, 0, unroll=16)

    def factors(x, state):
        fine_before, coarse_before = state
        w1b, c1b = KW[0, x], CW[0, x]
        inverse = inside / (FI[x] - w1b * fine_before)
        coarse_inverse = coarse_inside / (CI[x] - c1b * coarse_before)
        FI[x] = inverse
        CI[x] = coarse_inverse
        FB[x] = w1b * inverse
        CB[x] = c1b * coarse_inverse
        quotient = KW[0, x + 1] * inverse
        coarse_quotient = CW[0, x + 1] * coarse_inverse
        FQ[x] = quotient
        CQ[x] = coarse_quotient
        return quotient, coarse_quotient

    loop(64, factors, (nothing, nothing), unroll=2)


def line_body(
    sizes,
    middle,
    shallow,
    deep,
    free,
    M,
    Dm,
    KW,
    CW,
    FI,
    FB,
    FQ,
    CI,
    CB,
    CQ,
    out,
    W,
    E,
    Rm,
    NS,
    SM,
    CS,
    TY,
    CM,
    OUT,
):
    shape = (ROWS, 128)
    orders = position_facts(sizes)[2]
    even_row = lax.broadcasted_iota(jnp.int32, shape, 0) % 2 == 0
    even_lane = lanes(shape) % 2 == 0
    nothing = jnp.zeros(shape, f32)

    def put(field, level, y, values):
        rows = slice(TILE * y, TILE * y + TILE)
        source = values * free[field % 3, level, rows, :]
        W[field, level, rows, :] = source
        E[field, level + 1, rows, :] = source * Dm[field % 3, level, rows, :]

    spread_out(
        ((shallow, 0, orders[0]), (middle, 2, orders[1]), (deep, 0, orders[2])),
        (True, False),
        put,
    )

    def side_fluxes(part, l):
        e1, e2, e3 = (E[3 * part + d, l] for d in range(3))
        b2 = face_weight[1] * ((z_next(e1) - e1) - (E[3 * part + 2, l + 1] - e3))
        b3 = face_weight[2] * ((E[3 * part + 1, l + 1] - e2) - (y_next(e1) - e1))
        return b2, b3

    def curl(part, l, before):
        e1, e2, e3 = (E[3 * part + d, l] for d in range(3))
        b2, b3 = side_fluxes(part, l)
        b1 = face_weight[0] * ((y_next(e3) - e3) - (z_next(e2) - e2))
        b2_before, b3_before = before
        results = (
            (z_back(b2) - b2) - (y_back(b3) - b3) + M[0, l - 1] * e1,
            (b3_before - b3) - (z_back(b1) - b1) + M[1, l - 1] * e2,
            (y_back(b1) - b1) - (b2_before - b2) + M[2, l - 1] * e3,
        )
        return results, (b2, b3)

    for field in range(6):
        pad_low(E, field)
        pad_high(E, field)

    def first_remainder(l, state):
        after = []
        for part in range(2):
            results, fluxes = curl(part, l + 1, state[part])
            after.append(fluxes)
            for d in range(3):
                Rm[3 * part + d, l + 1] = (
                    W[3 * part + d, l] - results[d] * free[d, l]
                )
        return tuple(after)

    loop(16, first_remainder, (side_fluxes(0, 0), side_fluxes(1, 0)), unroll=4)
    pad_low(Rm, 0)
    pad_low(Rm, 3)

    def to_nodes(l, state):
        for part in range(2):
            r1, r2, r3 = (Rm[3 * part + d, l + 1] for d in range(3))
            r1b = Rm[3 * part, l]
            r2b = y_back(r2)
            r3b = z_back(r3)
            members = [
                ((r1b - r1) + (r2b - r2)) + (r3b - r3),
                0.5 * (r1 + r1b),
                0.5 * (r2 + r2b),
                0.5 * (r3 + r3b),
            ]
            for g, values in enumerate(turned(members)):
                NS[part, 16 * g + l] = values
        return state

    loop(16, to_nodes, 0, unroll=8)

    def eliminate(source, inverse, back, parts, unroll=4):
        def step(x, state):
            scale, couple = inverse[x], back[x]
            sources = source(x)
            after = []
            for part in range(parts):
                value = sources[part] * scale + couple * state[part]
                TY[part, x] = value
                after.append(value)
            return tuple(after)

        loop(64, step, (nothing,) * parts, unroll=unroll)

    def substitute(quotient, parts, then, unroll):
        def step(x, state):
            factor = quotient[x]
            after = tuple(TY[part, x] + factor * state[part] for part in range(parts))
            then(x, *after)
            return after

        loop(64, step, (nothing,) * parts, unroll=unroll, reverse=True)

    def sides(v, w2, w3, by):
        return ((w3 * row_next(v, by) + row_back(w3 * v, by)) + w2 * lane_next(v, by)) + lane_back(
            w2 * v, by
        )

    def after_smoothing(x, *values):
        halved = []
        for part, value in enumerate(values):
            SM[part, x] = value
            residue = sides(value, KW[1, x + 1], KW[2, x + 1], 1)
            halved.append(residue + 0.5 * (row_back(residue) + row_next(residue)))
        CM[0, x] = jnp.where(even_row, halved[0], row_back(halved[1]))

    def coarse_source(x):
        merged = CM[0, x]
        value = merged + 0.5 * (lane_back(merged) + lane_next(merged))
        CS[0, x] = value
        return (value,)

    def after_coarse(x, value):
        CM[0, x] = CS[0, x] + sides(value, CW[1, x + 1], CW[2, x + 1], 2)

    def after_correction(x, value):
        CS[0, x] = jnp.where(even_lane, value, 0.5 * (lane_back(value) + lane_next(value)))

    def corrected_source(x):
        wide = CS[0, x]
        above = row_next(wide)
        corrections = (
            jnp.where(even_row, wide, 0.5 * (row_back(wide) + above)),
            jnp.where(even_row, above, 0.5 * (wide + row_next(wide, 2))),
        )
        return tuple(
            NS[part, x] + sides(SM[part, x] + corrections[part], KW[1, x + 1], KW[2, x + 1], 1)
            for part in range(2)
        )

    def after_potential(x, *values):
        for part in range(2):
            NS[part, x] = values[part]

    eliminate(lambda x: (NS[0, x], NS[1, x]), FI, FB, 2)
    substitute(FQ, 2, after_smoothing, 16)
    eliminate(coarse_source, CI, CB, 1, 16)
    substitute(CQ, 1, after_coarse, 16)
    eliminate(lambda x: (CM[0, x],), CI, CB, 1)
    substitute(CQ, 1, after_correction, 16)
    eliminate(corrected_source, FI, FB, 2, 16)
    substitute(FQ, 2, after_potential, 4)

    def from_nodes(l, state):
        for part in range(2):
            p0, p1, p2, p3 = turned([NS[part, 16 * g + l] for g in range(4)])
            Rm[3 * part, l + 1] = p0
            Rm[3 * part + 1, l + 1] = p1
            for d, (g_part, h_part) in (
                (1, (y_next(p0) - p0, 0.5 * (p2 + y_next(p2)))),
                (2, (z_next(p0) - p0, 0.5 * (p3 + z_next(p3)))),
            ):
                E[3 * part + d, l + 1] = (
                    E[3 * part + d, l + 1] + (g_part + h_part) * free[d, l]
                )
        return state

    loop(16, from_nodes, 0, unroll=8)
    for part in range(2):
        pad_high(Rm, 3 * part)
        pad_high(Rm, 3 * part + 1)

    def second_first(l, state):
        for part in range(2):
            p0, p1 = Rm[3 * part, l + 1], Rm[3 * part + 1, l + 1]
            g_part = Rm[3 * part, l + 2] - p0
            h_part = 0.5 * (p1 + Rm[3 * part + 1, l + 2])
            E[3 * part, l + 1] = E[3 * part, l + 1] + (g_part + h_part) * free[0, l]
        return state

    loop(16, second_first, 0, unroll=4)
    for field in range(6):
        pad_low(E, field)
        pad_high(E, field)

    def last_step(l, state):
        after = []
        for part in range(2):
            results, fluxes = curl(part, l + 1, state[part])
            after.append(fluxes)
            for d in range(3):
                field = 3 * part + d
                remainder = W[field, l] - results[d] * free[d, l]
                value = E[field, l + 1] + Dm[d, l] * remainder
                OUT[field, l] = value[TILE : 2 * TILE]
        return tuple(after)

    loop(16, last_step, (side_fluxes(0, 0), side_fluxes(1, 0)), unroll=8)

    def gather_up(a, state):
        slots = [OUT[field, 4 * a + i] for field in range(6) for i in range(4)]
        block = 0
        for start in (0, 16):
            group = jnp.concatenate(slots[start : start + 16], axis=0)
            block = send_group(
                group, lambda p: p // 4 * 4 + a if p % 4 == 1 else None, out, block
            )
        return state

    loop(4, gather_up, 0, unroll=4)


def vmem():
    return pl.BlockSpec(memory_space=pltpu.VMEM)


def smem():
    return pl.BlockSpec(memory_space=pltpu.SMEM)


def pack(residual, classes, edge_mask, class_weight, **options):
    return pl.pallas_call(
        pack_body,
        out_shape=resident(16, 5, HALF, 128),
        in_specs=[vmem(), vmem(), vmem(), smem()],
        out_specs=vmem(),
        name="pack",
        **options,
    )(residual, classes, edge_mask, class_weight)


def unpack(packed, shape, **options):
    return pl.pallas_call(
        unpack_body,
        out_shape=jax.ShapeDtypeStruct(shape, f32),
        in_specs=[vmem()],
        out_specs=vmem(),
        name="unpack",
        **options,
    )(packed)


def resident(*shape):
    return pltpu.VMEM(shape, f32)


def setup(sizes, middle, shallow, deep, **options):
    line = resident(64, ROWS, 128)
    edge = resident(3, 16, ROWS, 128)
    weights = resident(3, 65, ROWS, 128)
    return pl.pallas_call(
        functools.partial(setup_body, sizes),
        out_shape=[edge, edge, edge, weights, weights] + [line] * 6,
        in_specs=[vmem()] * 3,
        out_specs=[vmem()] * 11,
        scratch_shapes=[resident(1, 18, ROWS, 128)],
        name="setup",
        **options,
    )(middle, shallow, deep)


def lines(sizes, middle, shallow, deep, ready, **options):
    edge = lambda count, levels: resident(count, levels, ROWS, 128)
    pair = resident(2, 64, ROWS, 128)
    return pl.pallas_call(
        functools.partial(line_body, sizes),
        out_shape=resident(16, 3, HALF, 128),
        in_specs=[vmem()] * (3 + len(ready)),
        out_specs=vmem(),
        scratch_shapes=[
            edge(6, 16),
            edge(6, 18),
            edge(6, 18),
            pair,
            pair,
            resident(1, 64, ROWS, 128),
            pair,
            resident(1, 64, ROWS, 128),
            resident(6, 16, TILE, 128),
        ],
        name="lines",
        **options,
    )(middle, shallow, deep, *ready)


def swap(values):
    return lax.all_to_all(values, "gx", 0, 0, tiled=True)


def per_device(residual, classes, edge_mask, class_weight):
    size_x, size_y, size_z = (lax.axis_size(name) for name in AXES)
    tiles = size_x * size_z

    def position(y, tile):
        z, x = divmod(tile, size_x)
        if z % 2:
            x = size_x - 1 - x
        return (x * size_y + y) * size_z + z

    def from_side(values, step_y, step_tile):
        pairs = []
        for y in range(size_y):
            for tile in range(tiles):
                next_y = y - step_y if tile // size_x % 2 else y + step_y
                if 0 <= next_y < size_y and 0 <= tile + step_tile < tiles:
                    pairs.append((position(y, tile), position(next_y, tile + step_tile)))
        return lax.ppermute(values, AXES, pairs)

    sizes = (size_x, size_y, size_z)
    own = swap(pack(residual, classes, edge_mask, class_weight))
    middle = jnp.concatenate([from_side(own, 1, 0), own, from_side(own, -1, 0)], axis=0)
    material, source = middle[:, :2], middle[:, 2:]
    shallow_material = from_side(material, 0, 1)
    deep_material = from_side(material, 0, -1)
    shallow_source = from_side(source, 0, 1)
    deep_source = from_side(source, 0, -1)
    options = lambda size, cost: dict(
        compiler_params=pltpu.CompilerParams(vmem_limit_bytes=size * 2**20),
        cost_estimate=pl.CostEstimate(flops=cost, bytes_accessed=0, transcendentals=0),
    )
    ready = setup(sizes, middle, shallow_material, deep_material, **options(20, 2**27))
    result = swap(lines(sizes, middle, shallow_source, deep_source, ready, **options(32, 2**27)))
    result = pltpu.with_memory_space_constraint(result, pltpu.VMEM)
    return unpack(result, residual.shape)


def solution(mesh):
    return jax.shard_map(
        per_device,
        mesh=mesh,
        in_specs=(
            P("period", None, "gx", "gy", "gz"),
            P("gx", "gy", "gz"),
            P(None, "gx", "gy", "gz"),
            P("period"),
        ),
        out_specs=P("period", None, "gx", "gy", "gz"),
        check_vma=False,
    )
```

```python
import functools

import jax
import jax.numpy as jnp
from jax import lax
from jax.experimental import pallas as pl
from jax.experimental.pallas import tpu as pltpu
from jax.sharding import PartitionSpec as P

aspect = 2.0
face_weight = (1.0 / (aspect * aspect), 1.0, 1.0)
mass_factor = (aspect * aspect, 1.0, 1.0)
stiff_weight = (
    2.0 * (face_weight[1] + face_weight[2]),
    2.0 * (face_weight[0] + face_weight[2]),
    2.0 * (face_weight[0] + face_weight[1]),
)
edge_damping = 0.6
shift_ratio = 0.0001
shift_added = 0.05
coarse_scale = (0.5625, 0.1875, 0.1875)

f32 = jnp.float32
TILE = 8
ROWS = 3 * TILE
GROUPS = 4
DEPTH = 32
HALF = TILE // 2
AXES = ("gx", "gy", "gz")


def lanes(shape):
    return lax.broadcasted_iota(jnp.int32, shape, 1)


def turned(values):
    gap = jnp.zeros((DEPTH - ROWS, 128), f32)
    stacked = jnp.concatenate([piece for value in values for piece in (value, gap)], axis=0).T
    return [stacked[DEPTH * g : DEPTH * g + ROWS] for g in range(4)]


def loop(count, body, carry, unroll=1, reverse=False):
    def step(turn, state):
        for part in range(unroll):
            index = turn * unroll + part
            state = body(count - 1 - index if reverse else index, state)
        return state

    return lax.fori_loop(0, count // unroll, step, carry)


def y_next(v, by=1):
    return pltpu.roll(v, v.shape[0] - by, 0)


def y_back(v, by=1):
    return pltpu.roll(v, by, 0)


def z_next(v, by=1):
    return pltpu.roll(v, 128 - by, 1)


def z_back(v, by=1):
    return pltpu.roll(v, by, 1)


row_next, row_back, lane_next, lane_back = y_next, y_back, z_next, z_back


def position_facts(sizes):
    x, y, z = (lax.axis_index(name) for name in AXES)
    flip = z % 2
    along = x + flip * (sizes[0] - 1 - 2 * x)
    before = jnp.where(along == 0, 1 - flip, flip)
    after = jnp.where(along == sizes[0] - 1, 1 - flip, flip)
    corner_y = y * TILE - TILE
    corner_z = (z * sizes[0] + along) * TILE - TILE
    return corner_y, corner_z, (before, flip, after)


def mirrored(flip, index, count):
    return index + flip * (count - 1 - 2 * index)


def pack_body(residual, classes, edge_mask, class_weight, out):
    thick = classes.shape[0]
    flip = lax.axis_index("gz") % 2
    slots = []
    for i in range(thick):
        labels = classes[i]
        cells = jnp.zeros(labels.shape, f32)
        for label in range(class_weight.shape[0]):
            cells = jnp.where(labels == label, class_weight[label], cells)
        slots.append(cells)
    for comp in range(3):
        slots += [(1 - edge_mask[comp, i]).astype(f32) for i in range(thick)]
    for part in range(2):
        for comp in range(3):
            slots += [residual[part, comp, i] for i in range(thick)]
    block = 0
    for start in range(0, len(slots), 16):
        group = jnp.concatenate(slots[start : start + 16], axis=0)
        block = send_group(group, lambda target: mirrored(flip, target, 16), out, block)


def send_group(group, device, out, block):
    half = HALF
    if group.shape[0] == 128:
        moved = group.T
        parts = 2
    else:
        moved = jnp.concatenate([group, pltpu.roll(group, 128 - half, 1)], axis=0).T
        parts = 1
    for target in range(16):
        where = device(target)
        if where is not None:
            for part in range(parts):
                row = TILE * target + half * part
                out[where, block + part] = moved[row : row + half]
    return block + parts


def receive_group(blocks, block, full):
    half = HALF
    gap = jnp.zeros((half, 128), f32)
    rows = []
    for source in range(16):
        rows.append(blocks(source, block))
        rows.append(blocks(source, block + 1) if full else gap)
    moved = jnp.concatenate(rows, axis=0).T
    if full:
        return moved
    upper = pltpu.roll(moved[64:], half, 1)
    return jnp.where(lanes((64, 128)) % TILE < half, moved[:64], upper)


def unpack_body(packed, out):
    flip = lax.axis_index("gz") % 2
    for part in range(2):
        moved = receive_group(
            lambda window, block: packed[mirrored(flip, window, 16), block], 2 * part, part == 0
        )
        for slot in range(moved.shape[0] // TILE):
            field, i = divmod(16 * part + slot, 4)
            out[field // 3, field % 3, i] = moved[TILE * slot : TILE * slot + TILE]


def pad_low(ref, field):
    lane = lanes((ROWS, 128))
    ref[field, 0] = jnp.where(lane < DEPTH, 0.0, pltpu.roll(ref[field, 16], DEPTH, 1))


def pad_high(ref, field):
    lane = lanes((ROWS, 128))
    ref[field, 17] = jnp.where(
        lane >= 128 - DEPTH, 0.0, pltpu.roll(ref[field, 1], 128 - DEPTH, 1)
    )


def spread_out(windows, groups, put):
    gap = jnp.zeros((HALF, 128), f32)

    def step(a, state):
        for y in range(3):
            for part, full in enumerate(groups):

                def blocks(p, block):
                    g, t = divmod(p, 4)
                    if t == 3:
                        return gap
                    ref, first, flag = windows[t]
                    turn = y + flag * (2 - 2 * y)
                    return ref[turn * 16 + 4 * g + a, first + block]

                moved = receive_group(blocks, 2 * part, full)
                for slot in range(moved.shape[0] // TILE):
                    field, i = divmod(16 * part + slot, 4)
                    put(field, 4 * a + i, y, moved[TILE * slot : TILE * slot + TILE])
        return state

    loop(4, step, 0, unroll=2)


def setup_body(
    sizes,
    middle,
    shallow,
    deep,
    free_out,
    M,
    Dm,
    KW,
    CW,
    FI,
    FB,
    FQ,
    CI,
    CB,
    CQ,
    cells,
):
    corner_y, corner_z, orders = position_facts(sizes)
    extent_y, extent_z = sizes[1] * TILE, sizes[0] * sizes[2] * TILE
    shape = (ROWS, 128)
    lane = lanes(shape)
    row = lax.broadcasted_iota(jnp.int32, shape, 0)
    at_y = lane % DEPTH + corner_y
    at_z = row + corner_z
    inside = jnp.where(
        (at_y >= 0) & (at_y < extent_y) & (at_z >= 0) & (at_z < extent_z), 1.0, 0.0
    ).astype(f32)
    coarse_inside = jnp.where(row % 2 == 0, inside, row_back(inside))
    even_row = row % 2 == 0

    def put(field, level, y, values):
        if field == 0:
            cells[0, level + 1, TILE * y : TILE * y + TILE, :] = values
        else:
            free_out[field - 1, level, TILE * y : TILE * y + TILE, :] = values

    spread_out(
        ((shallow, 0, orders[0]), (middle, 0, orders[1]), (deep, 0, orders[2])), (True,), put
    )
    pad_low(cells, 0)

    def coefficients(l, state):
        c = cells[0, l + 1]
        cx = cells[0, l]
        cy = y_back(c)
        cz = z_back(c)
        averages = (
            0.25 * (((c + cy) + cz) + z_back(cy)),
            0.25 * (((c + cx) + cz) + z_back(cx)),
            0.25 * (((c + cx) + cy) + y_back(cx)),
        )
        for d in range(3):
            free = free_out[d, l]
            masses = mass_factor[d] * averages[d] * free
            diagonal = stiff_weight[d] + masses
            M[d, l] = masses
            Dm[d, l] = edge_damping * free / diagonal
            stiff = diagonal * free
            for g, values in enumerate(turned([masses, stiff, stiff, stiff])):
                KW[d, 16 * g + l + 1] = values
        return state

    loop(16, coefficients, 0, unroll=8)

    for d in range(3):
        KW[d, 0] = jnp.zeros(shape, f32)

    nothing = jnp.zeros(shape, f32)
    CW[0, 0] = nothing

    def diagonals(x, state):
        w1b, w1, w2, w3 = KW[0, x], KW[0, x + 1], KW[1, x + 1], KW[2, x + 1]
        total = ((((w1 + w1b) + w3) + row_back(w3)) + w2) + lane_back(w2)
        FI[x] = (1.0 + shift_ratio) * total + shift_added
        for d, w in enumerate((w1, w2, w3)):
            pair = w + row_next(w)
            pair = jnp.where(even_row, pair, row_back(pair))
            CW[d, x + 1] = coarse_scale[d] * (pair + lane_next(pair))
        return state

    def coarse_diagonals(x, state):
        w1b, w1, w2, w3 = CW[0, x], CW[0, x + 1], CW[1, x + 1], CW[2, x + 1]
        total = ((((w1 + w1b) + w3) + row_back(w3, 2)) + w2) + lane_back(w2, 2)
        CI[x] = (1.0 + shift_ratio) * total + shift_added
        return state

    loop(64, diagonals, 0, unroll=16)
    loop(64, coarse_diagonals, 0, unroll=16)

    def factors(x, state):
        fine_before, coarse_before = state
        w1b, c1b = KW[0, x], CW[0, x]
        inverse = inside / (FI[x] - w1b * fine_before)
        coarse_inverse = coarse_inside / (CI[x] - c1b * coarse_before)
        FI[x] = inverse
        CI[x] = coarse_inverse
        FB[x] = w1b * inverse
        CB[x] = c1b * coarse_inverse
        quotient = KW[0, x + 1] * inverse
        coarse_quotient = CW[0, x + 1] * coarse_inverse
        FQ[x] = quotient
        CQ[x] = coarse_quotient
        return quotient, coarse_quotient

    loop(64, factors, (nothing, nothing), unroll=2)


def line_body(
    sizes,
    middle,
    shallow,
    deep,
    free,
    M,
    Dm,
    KW,
    CW,
    FI,
    FB,
    FQ,
    CI,
    CB,
    CQ,
    out,
    W,
    E,
    Rm,
    NS,
    SM,
    CS,
    TY,
    CM,
    OUT,
):
    shape = (ROWS, 128)
    orders = position_facts(sizes)[2]
    even_row = lax.broadcasted_iota(jnp.int32, shape, 0) % 2 == 0
    even_lane = lanes(shape) % 2 == 0
    nothing = jnp.zeros(shape, f32)
    def put(field, level, y, values):
        rows = slice(TILE * y, TILE * y + TILE)
        source = values * free[field % 3, level, rows, :]
        W[field, level, rows, :] = source
        E[field, level + 1, rows, :] = source * Dm[field % 3, level, rows, :]

    spread_out(
        ((shallow, 2, orders[0]), (middle, 2, orders[1]), (deep, 2, orders[2])),
        (True, False),
        put,
    )

    def side_fluxes(part, l):
        e1, e2, e3 = (E[3 * part + d, l] for d in range(3))
        b2 = face_weight[1] * ((z_next(e1) - e1) - (E[3 * part + 2, l + 1] - e3))
        b3 = face_weight[2] * ((E[3 * part + 1, l + 1] - e2) - (y_next(e1) - e1))
        return b2, b3

    def curl(part, l, before):
        e1, e2, e3 = (E[3 * part + d, l] for d in range(3))
        b2, b3 = side_fluxes(part, l)
        b1 = face_weight[0] * ((y_next(e3) - e3) - (z_next(e2) - e2))
        b2_before, b3_before = before
        results = (
            (z_back(b2) - b2) - (y_back(b3) - b3) + M[0, l - 1] * e1,
            (b3_before - b3) - (z_back(b1) - b1) + M[1, l - 1] * e2,
            (y_back(b1) - b1) - (b2_before - b2) + M[2, l - 1] * e3,
        )
        return results, (b2, b3)

    for field in range(6):
        pad_low(E, field)
        pad_high(E, field)

    def first_remainder(l, state):
        after = []
        for part in range(2):
            results, fluxes = curl(part, l + 1, state[part])
            after.append(fluxes)
            for d in range(3):
                Rm[3 * part + d, l + 1] = (
                    W[3 * part + d, l] - results[d] * free[d, l]
                )
        return tuple(after)

    loop(16, first_remainder, (side_fluxes(0, 0), side_fluxes(1, 0)), unroll=4)
    pad_low(Rm, 0)
    pad_low(Rm, 3)

    def to_nodes(l, state):
        for part in range(2):
            r1, r2, r3 = (Rm[3 * part + d, l + 1] for d in range(3))
            r1b = Rm[3 * part, l]
            r2b = y_back(r2)
            r3b = z_back(r3)
            members = [
                ((r1b - r1) + (r2b - r2)) + (r3b - r3),
                0.5 * (r1 + r1b),
                0.5 * (r2 + r2b),
                0.5 * (r3 + r3b),
            ]
            for g, values in enumerate(turned(members)):
                NS[part, 16 * g + l] = values
        return state

    loop(16, to_nodes, 0, unroll=8)

    def eliminate(source, inverse, back, parts, unroll=4):
        def step(x, state):
            scale, couple = inverse[x], back[x]
            sources = source(x)
            after = []
            for part in range(parts):
                value = sources[part] * scale + couple * state[part]
                TY[part, x] = value
                after.append(value)
            return tuple(after)

        loop(64, step, (nothing,) * parts, unroll=unroll)

    def substitute(quotient, parts, then, unroll):
        def step(x, state):
            factor = quotient[x]
            after = tuple(TY[part, x] + factor * state[part] for part in range(parts))
            then(x, *after)
            return after

        loop(64, step, (nothing,) * parts, unroll=unroll, reverse=True)

    def sides(v, w2, w3, by):
        return ((w3 * row_next(v, by) + row_back(w3 * v, by)) + w2 * lane_next(v, by)) + lane_back(
            w2 * v, by
        )

    def after_smoothing(x, *values):
        halved = []
        for part, value in enumerate(values):
            SM[part, x] = value
            residue = sides(value, KW[1, x + 1], KW[2, x + 1], 1)
            halved.append(residue + 0.5 * (row_back(residue) + row_next(residue)))
        CM[0, x] = jnp.where(even_row, halved[0], row_back(halved[1]))

    def coarse_source(x):
        merged = CM[0, x]
        value = merged + 0.5 * (lane_back(merged) + lane_next(merged))
        CS[0, x] = value
        return (value,)

    def after_coarse(x, value):
        CM[0, x] = CS[0, x] + sides(value, CW[1, x + 1], CW[2, x + 1], 2)

    def after_correction(x, value):
        CS[0, x] = jnp.where(even_lane, value, 0.5 * (lane_back(value) + lane_next(value)))

    def corrected_source(x):
        wide = CS[0, x]
        above = row_next(wide)
        corrections = (
            jnp.where(even_row, wide, 0.5 * (row_back(wide) + above)),
            jnp.where(even_row, above, 0.5 * (wide + row_next(wide, 2))),
        )
        return tuple(
            NS[part, x] + sides(SM[part, x] + corrections[part], KW[1, x + 1], KW[2, x + 1], 1)
            for part in range(2)
        )

    def after_potential(x, *values):
        for part in range(2):
            NS[part, x] = values[part]

    eliminate(lambda x: (NS[0, x], NS[1, x]), FI, FB, 2)
    substitute(FQ, 2, after_smoothing, 16)
    eliminate(coarse_source, CI, CB, 1, 16)
    substitute(CQ, 1, after_coarse, 16)
    eliminate(lambda x: (CM[0, x],), CI, CB, 1)
    substitute(CQ, 1, after_correction, 16)
    eliminate(corrected_source, FI, FB, 2, 16)
    substitute(FQ, 2, after_potential, 4)

    def from_nodes(l, state):
        for part in range(2):
            p0, p1, p2, p3 = turned([NS[part, 16 * g + l] for g in range(4)])
            Rm[3 * part, l + 1] = p0
            Rm[3 * part + 1, l + 1] = p1
            for d, (g_part, h_part) in (
                (1, (y_next(p0) - p0, 0.5 * (p2 + y_next(p2)))),
                (2, (z_next(p0) - p0, 0.5 * (p3 + z_next(p3)))),
            ):
                E[3 * part + d, l + 1] = (
                    E[3 * part + d, l + 1] + (g_part + h_part) * free[d, l]
                )
        return state

    loop(16, from_nodes, 0, unroll=8)
    for part in range(2):
        pad_high(Rm, 3 * part)
        pad_high(Rm, 3 * part + 1)

    def second_first(l, state):
        for part in range(2):
            p0, p1 = Rm[3 * part, l + 1], Rm[3 * part + 1, l + 1]
            g_part = Rm[3 * part, l + 2] - p0
            h_part = 0.5 * (p1 + Rm[3 * part + 1, l + 2])
            E[3 * part, l + 1] = E[3 * part, l + 1] + (g_part + h_part) * free[0, l]
        return state

    loop(16, second_first, 0, unroll=4)
    for field in range(6):
        pad_low(E, field)
        pad_high(E, field)

    def last_step(l, state):
        after = []
        for part in range(2):
            results, fluxes = curl(part, l + 1, state[part])
            after.append(fluxes)
            for d in range(3):
                field = 3 * part + d
                remainder = W[field, l] - results[d] * free[d, l]
                value = E[field, l + 1] + Dm[d, l] * remainder
                OUT[field, l] = value[TILE : 2 * TILE]
        return tuple(after)

    loop(16, last_step, (side_fluxes(0, 0), side_fluxes(1, 0)), unroll=8)

    def gather_up(a, state):
        slots = [OUT[field, 4 * a + i] for field in range(6) for i in range(4)]
        block = 0
        for start in (0, 16):
            group = jnp.concatenate(slots[start : start + 16], axis=0)
            block = send_group(
                group, lambda p: p // 4 * 4 + a if p % 4 == 1 else None, out, block
            )
        return state

    loop(4, gather_up, 0, unroll=4)


def vmem():
    return pl.BlockSpec(memory_space=pltpu.VMEM)


def smem():
    return pl.BlockSpec(memory_space=pltpu.SMEM)


def pack(residual, classes, edge_mask, class_weight, **options):
    return pl.pallas_call(
        pack_body,
        out_shape=resident(16, 5, HALF, 128),
        in_specs=[vmem(), vmem(), vmem(), smem()],
        out_specs=vmem(),
        name="pack",
        **options,
    )(residual, classes, edge_mask, class_weight)


def unpack(packed, shape, **options):
    return pl.pallas_call(
        unpack_body,
        out_shape=jax.ShapeDtypeStruct(shape, f32),
        in_specs=[vmem()],
        out_specs=vmem(),
        name="unpack",
        **options,
    )(packed)


def resident(*shape):
    return pltpu.VMEM(shape, f32)


def setup(sizes, middle, shallow, deep, **options):
    line = resident(64, ROWS, 128)
    edge = resident(3, 16, ROWS, 128)
    weights = resident(3, 65, ROWS, 128)
    return pl.pallas_call(
        functools.partial(setup_body, sizes),
        out_shape=[edge, edge, edge, weights, weights] + [line] * 6,
        in_specs=[vmem()] * 3,
        out_specs=[vmem()] * 11,
        scratch_shapes=[resident(1, 18, ROWS, 128)],
        name="setup",
        **options,
    )(middle, shallow, deep)


def lines(sizes, middle, shallow, deep, ready, **options):
    edge = lambda count, levels: resident(count, levels, ROWS, 128)
    pair = resident(2, 64, ROWS, 128)
    return pl.pallas_call(
        functools.partial(line_body, sizes),
        out_shape=resident(16, 3, HALF, 128),
        in_specs=[vmem()] * (3 + len(ready)),
        out_specs=vmem(),
        scratch_shapes=[
            edge(6, 16),
            edge(6, 18),
            edge(6, 18),
            pair,
            pair,
            resident(1, 64, ROWS, 128),
            pair,
            resident(1, 64, ROWS, 128),
            resident(6, 16, TILE, 128),
        ],
        name="lines",
        **options,
    )(middle, shallow, deep, *ready)


def swap(values):
    return lax.all_to_all(values, "gx", 0, 0, tiled=True)


def per_device(residual, classes, edge_mask, class_weight):
    size_x, size_y, size_z = (lax.axis_size(name) for name in AXES)
    tiles = size_x * size_z

    def position(y, tile):
        z, x = divmod(tile, size_x)
        if z % 2:
            x = size_x - 1 - x
        return (x * size_y + y) * size_z + z

    def from_side(values, step_y, step_tile):
        pairs = []
        for y in range(size_y):
            for tile in range(tiles):
                next_y = y - step_y if tile // size_x % 2 else y + step_y
                if 0 <= next_y < size_y and 0 <= tile + step_tile < tiles:
                    pairs.append((position(y, tile), position(next_y, tile + step_tile)))
        return lax.ppermute(values, AXES, pairs)

    sizes = (size_x, size_y, size_z)
    own = swap(pack(residual, classes, edge_mask, class_weight))
    middle = jnp.concatenate([from_side(own, 1, 0), own, from_side(own, -1, 0)], axis=0)
    shallow, deep = from_side(middle, 0, 1), from_side(middle, 0, -1)
    options = lambda size, cost: dict(
        compiler_params=pltpu.CompilerParams(vmem_limit_bytes=size * 2**20),
        cost_estimate=pl.CostEstimate(flops=cost, bytes_accessed=0, transcendentals=0),
    )
    ready = setup(sizes, middle, shallow, deep, **options(20, 2**27))
    result = swap(lines(sizes, middle, shallow, deep, ready, **options(32, 2**27)))
    result = pltpu.with_memory_space_constraint(result, pltpu.VMEM)
    return unpack(result, residual.shape)


def solution(mesh):
    return jax.shard_map(
        per_device,
        mesh=mesh,
        in_specs=(
            P("period", None, "gx", "gy", "gz"),
            P("gx", "gy", "gz"),
            P(None, "gx", "gy", "gz"),
            P("period"),
        ),
        out_specs=P("period", None, "gx", "gy", "gz"),
        check_vma=False,
    )
```

```python
import functools

import jax
import jax.numpy as jnp
from jax import lax
from jax.experimental import pallas as pl
from jax.experimental.pallas import tpu as pltpu
from jax.sharding import PartitionSpec as P


aspect = 2.0
face_weight = (1.0 / (aspect * aspect), 1.0, 1.0)
mass_factor = (aspect * aspect, 1.0, 1.0)
stiff_weight = (
    2.0 * (face_weight[1] + face_weight[2]),
    2.0 * (face_weight[0] + face_weight[2]),
    2.0 * (face_weight[0] + face_weight[1]),
)
edge_damping = 0.6
shift_ratio = 0.0001
shift_added = 0.05
coarse_scale = (0.5625, 0.1875, 0.1875)

f32 = jnp.float32
TILE = 8
ROWS = 3 * TILE
DEPTH = 32
HALF = TILE // 2
AXES = ("gx", "gy", "gz")


def lanes(shape):
    return lax.broadcasted_iota(jnp.int32, shape, 1)


def turned(values):
    gap = jnp.zeros((DEPTH - ROWS, 128), f32)
    stacked = jnp.concatenate([piece for value in values for piece in (value, gap)], axis=0).T
    return [stacked[DEPTH * g : DEPTH * g + ROWS] for g in range(4)]


def loop(count, body, carry, unroll=1, reverse=False):
    def step(turn, state):
        for part in range(unroll):
            index = turn * unroll + part
            state = body(count - 1 - index if reverse else index, state)
        return state

    return lax.fori_loop(0, count // unroll, step, carry)


def y_next(v, by=1):
    return pltpu.roll(v, v.shape[0] - by, 0)


def y_back(v, by=1):
    return pltpu.roll(v, by, 0)


def z_next(v, by=1):
    return pltpu.roll(v, 128 - by, 1)


def z_back(v, by=1):
    return pltpu.roll(v, by, 1)


row_next, row_back, lane_next, lane_back = y_next, y_back, z_next, z_back


def position_facts(sizes):
    x, y, z = (lax.axis_index(name) for name in AXES)
    flip = z % 2
    along = x + flip * (sizes[0] - 1 - 2 * x)
    before = jnp.where(along == 0, 1 - flip, flip)
    after = jnp.where(along == sizes[0] - 1, 1 - flip, flip)
    corner_y = y * TILE - TILE
    corner_z = (z * sizes[0] + along) * TILE - TILE
    return corner_y, corner_z, (before, flip, after)


def mirrored(flip, index, count):
    return index + flip * (count - 1 - 2 * index)


def pack_body(residual, classes, edge_mask, class_weight, out):
    thick = classes.shape[0]
    flip = lax.axis_index("gz") % 2
    slots = []
    for i in range(thick):
        labels = classes[i]
        cells = jnp.zeros(labels.shape, f32)
        for label in range(class_weight.shape[0]):
            cells = jnp.where(labels == label, class_weight[label], cells)
        slots.append(cells)
    for comp in range(3):
        slots += [(1 - edge_mask[comp, i]).astype(f32) for i in range(thick)]
    for part in range(2):
        for comp in range(3):
            slots += [residual[part, comp, i] for i in range(thick)]
    block = 0
    for start in range(0, len(slots), 16):
        group = jnp.concatenate(slots[start : start + 16], axis=0)
        block = send_group(group, lambda target: mirrored(flip, target, 16), out, block)


def send_group(group, device, out, block):
    half = HALF
    if group.shape[0] == 128:
        moved = group.T
        parts = 2
    else:
        moved = jnp.concatenate([group, pltpu.roll(group, 128 - half, 1)], axis=0).T
        parts = 1
    for target in range(16):
        where = device(target)
        if where is not None:
            for part in range(parts):
                row = TILE * target + half * part
                out[where, block + part] = moved[row : row + half]
    return block + parts


def receive_group(blocks, block, full):
    half = HALF
    gap = jnp.zeros((half, 128), f32)
    rows = []
    for source in range(16):
        rows.append(blocks(source, block))
        rows.append(blocks(source, block + 1) if full else gap)
    moved = jnp.concatenate(rows, axis=0).T
    if full:
        return moved
    upper = pltpu.roll(moved[64:], half, 1)
    return jnp.where(lanes((64, 128)) % TILE < half, moved[:64], upper)


def unpack_body(packed, out):
    flip = lax.axis_index("gz") % 2
    for part in range(2):
        moved = receive_group(
            lambda window, block: packed[mirrored(flip, window, 16), block], 2 * part, part == 0
        )
        for slot in range(moved.shape[0] // TILE):
            field, i = divmod(16 * part + slot, 4)
            out[field // 3, field % 3, i] = moved[TILE * slot : TILE * slot + TILE]


def pad_low(ref, field):
    lane = lanes((ROWS, 128))
    ref[field, 0] = jnp.where(lane < DEPTH, 0.0, pltpu.roll(ref[field, 16], DEPTH, 1))


def pad_high(ref, field):
    lane = lanes((ROWS, 128))
    ref[field, 17] = jnp.where(
        lane >= 128 - DEPTH, 0.0, pltpu.roll(ref[field, 1], 128 - DEPTH, 1)
    )


def spread_out(windows, groups, put):
    gap = jnp.zeros((HALF, 128), f32)

    def step(a, state):
        for y in range(3):
            for part, full in enumerate(groups):

                def blocks(p, block):
                    g, t = divmod(p, 4)
                    if t == 3:
                        return gap
                    ref, first, flag = windows[t]
                    turn = y + flag * (2 - 2 * y)
                    return ref[turn * 16 + 4 * g + a, first + block]

                moved = receive_group(blocks, 2 * part, full)
                for slot in range(moved.shape[0] // TILE):
                    field, i = divmod(16 * part + slot, 4)
                    put(field, 4 * a + i, y, moved[TILE * slot : TILE * slot + TILE])
        return state

    loop(4, step, 0, unroll=2)


def setup_body(
    sizes,
    middle,
    shallow,
    deep,
    free_out,
    M,
    Dm,
    KW,
    CW,
    FI,
    FB,
    FQ,
    CI,
    CB,
    CQ,
    cells,
):
    corner_y, corner_z, orders = position_facts(sizes)
    extent_y, extent_z = sizes[1] * TILE, sizes[0] * sizes[2] * TILE
    shape = (ROWS, 128)
    lane = lanes(shape)
    row = lax.broadcasted_iota(jnp.int32, shape, 0)
    at_y = lane % DEPTH + corner_y
    at_z = row + corner_z
    inside = jnp.where(
        (at_y >= 0) & (at_y < extent_y) & (at_z >= 0) & (at_z < extent_z), 1.0, 0.0
    ).astype(f32)
    coarse_inside = jnp.where(row % 2 == 0, inside, row_back(inside))
    even_row = row % 2 == 0

    def put(field, level, y, values):
        if field == 0:
            cells[0, level + 1, TILE * y : TILE * y + TILE, :] = values
        else:
            free_out[field - 1, level, TILE * y : TILE * y + TILE, :] = values

    spread_out(
        ((shallow, 0, orders[0]), (middle, 0, orders[1]), (deep, 0, orders[2])), (True,), put
    )
    pad_low(cells, 0)

    def coefficients(l, state):
        c = cells[0, l + 1]
        cx = cells[0, l]
        cy = y_back(c)
        cz = z_back(c)
        averages = (
            0.25 * (((c + cy) + cz) + z_back(cy)),
            0.25 * (((c + cx) + cz) + z_back(cx)),
            0.25 * (((c + cx) + cy) + y_back(cx)),
        )
        for d in range(3):
            free = free_out[d, l]
            masses = mass_factor[d] * averages[d] * free
            diagonal = stiff_weight[d] + masses
            M[d, l] = masses
            Dm[d, l] = edge_damping * free / diagonal
            stiff = diagonal * free
            for g, values in enumerate(turned([masses, stiff, stiff, stiff])):
                KW[d, 16 * g + l + 1] = values
        return state

    loop(16, coefficients, 0, unroll=8)

    for d in range(3):
        KW[d, 0] = jnp.zeros(shape, f32)

    nothing = jnp.zeros(shape, f32)
    CW[0, 0] = nothing

    def diagonals(x, state):
        w1b, w1, w2, w3 = KW[0, x], KW[0, x + 1], KW[1, x + 1], KW[2, x + 1]
        total = ((((w1 + w1b) + w3) + row_back(w3)) + w2) + lane_back(w2)
        FI[x] = (1.0 + shift_ratio) * total + shift_added
        for d, w in enumerate((w1, w2, w3)):
            pair = w + row_next(w)
            pair = jnp.where(even_row, pair, row_back(pair))
            CW[d, x + 1] = coarse_scale[d] * (pair + lane_next(pair))
        return state

    def coarse_diagonals(x, state):
        w1b, w1, w2, w3 = CW[0, x], CW[0, x + 1], CW[1, x + 1], CW[2, x + 1]
        total = ((((w1 + w1b) + w3) + row_back(w3, 2)) + w2) + lane_back(w2, 2)
        CI[x] = (1.0 + shift_ratio) * total + shift_added
        return state

    loop(64, diagonals, 0, unroll=16)
    loop(64, coarse_diagonals, 0, unroll=16)

    def factors(x, state):
        fine_before, coarse_before = state
        w1b, c1b = KW[0, x], CW[0, x]
        inverse = inside / (FI[x] - w1b * fine_before)
        coarse_inverse = coarse_inside / (CI[x] - c1b * coarse_before)
        FI[x] = inverse
        CI[x] = coarse_inverse
        FB[x] = w1b * inverse
        CB[x] = c1b * coarse_inverse
        quotient = KW[0, x + 1] * inverse
        coarse_quotient = CW[0, x + 1] * coarse_inverse
        FQ[x] = quotient
        CQ[x] = coarse_quotient
        return quotient, coarse_quotient

    loop(64, factors, (nothing, nothing), unroll=2)


def line_body(
    sizes,
    middle,
    shallow,
    deep,
    free,
    M,
    Dm,
    KW,
    CW,
    FI,
    FB,
    FQ,
    CI,
    CB,
    CQ,
    out,
    W,
    E,
    Rm,
    NS,
    SM,
    CS,
    TY,
    CM,
    OUT,
):
    shape = (ROWS, 128)
    orders = position_facts(sizes)[2]
    even_row = lax.broadcasted_iota(jnp.int32, shape, 0) % 2 == 0
    even_lane = lanes(shape) % 2 == 0
    nothing = jnp.zeros(shape, f32)

    def put(field, level, y, values):
        rows = slice(TILE * y, TILE * y + TILE)
        source = values * free[field % 3, level, rows, :]
        W[field, level, rows, :] = source
        E[field, level + 1, rows, :] = source * Dm[field % 3, level, rows, :]

    spread_out(
        ((shallow, 2, orders[0]), (middle, 2, orders[1]), (deep, 0, orders[2])),
        (True, False),
        put,
    )

    def side_fluxes(part, l):
        e1, e2, e3 = (E[3 * part + d, l] for d in range(3))
        b2 = face_weight[1] * ((z_next(e1) - e1) - (E[3 * part + 2, l + 1] - e3))
        b3 = face_weight[2] * ((E[3 * part + 1, l + 1] - e2) - (y_next(e1) - e1))
        return b2, b3

    def curl(part, l, before):
        e1, e2, e3 = (E[3 * part + d, l] for d in range(3))
        b2, b3 = side_fluxes(part, l)
        b1 = face_weight[0] * ((y_next(e3) - e3) - (z_next(e2) - e2))
        b2_before, b3_before = before
        results = (
            (z_back(b2) - b2) - (y_back(b3) - b3) + M[0, l - 1] * e1,
            (b3_before - b3) - (z_back(b1) - b1) + M[1, l - 1] * e2,
            (y_back(b1) - b1) - (b2_before - b2) + M[2, l - 1] * e3,
        )
        return results, (b2, b3)

    for field in range(6):
        pad_low(E, field)
        pad_high(E, field)

    def first_remainder(l, state):
        after = []
        for part in range(2):
            results, fluxes = curl(part, l + 1, state[part])
            after.append(fluxes)
            for d in range(3):
                Rm[3 * part + d, l + 1] = (
                    W[3 * part + d, l] - results[d] * free[d, l]
                )
        return tuple(after)

    loop(16, first_remainder, (side_fluxes(0, 0), side_fluxes(1, 0)), unroll=4)
    pad_low(Rm, 0)
    pad_low(Rm, 3)

    def to_nodes(l, state):
        for part in range(2):
            r1, r2, r3 = (Rm[3 * part + d, l + 1] for d in range(3))
            r1b = Rm[3 * part, l]
            r2b = y_back(r2)
            r3b = z_back(r3)
            members = [
                ((r1b - r1) + (r2b - r2)) + (r3b - r3),
                0.5 * (r1 + r1b),
                0.5 * (r2 + r2b),
                0.5 * (r3 + r3b),
            ]
            for g, values in enumerate(turned(members)):
                NS[part, 16 * g + l] = values
        return state

    loop(16, to_nodes, 0, unroll=8)

    def eliminate(source, inverse, back, parts, unroll=4):
        def step(x, state):
            scale, couple = inverse[x], back[x]
            sources = source(x)
            after = []
            for part in range(parts):
                value = sources[part] * scale + couple * state[part]
                TY[part, x] = value
                after.append(value)
            return tuple(after)

        loop(64, step, (nothing,) * parts, unroll=unroll)

    def substitute(quotient, parts, then, unroll):
        def step(x, state):
            factor = quotient[x]
            after = tuple(TY[part, x] + factor * state[part] for part in range(parts))
            then(x, *after)
            return after

        loop(64, step, (nothing,) * parts, unroll=unroll, reverse=True)

    def sides(v, w2, w3, by):
        return ((w3 * row_next(v, by) + row_back(w3 * v, by)) + w2 * lane_next(v, by)) + lane_back(
            w2 * v, by
        )

    def after_smoothing(x, *values):
        halved = []
        for part, value in enumerate(values):
            SM[part, x] = value
            residue = sides(value, KW[1, x + 1], KW[2, x + 1], 1)
            halved.append(residue + 0.5 * (row_back(residue) + row_next(residue)))
        CM[0, x] = jnp.where(even_row, halved[0], row_back(halved[1]))

    def coarse_source(x):
        merged = CM[0, x]
        value = merged + 0.5 * (lane_back(merged) + lane_next(merged))
        CS[0, x] = value
        return (value,)

    def after_coarse(x, value):
        CM[0, x] = CS[0, x] + sides(value, CW[1, x + 1], CW[2, x + 1], 2)

    def after_correction(x, value):
        CS[0, x] = jnp.where(even_lane, value, 0.5 * (lane_back(value) + lane_next(value)))

    def corrected_source(x):
        wide = CS[0, x]
        above = row_next(wide)
        corrections = (
            jnp.where(even_row, wide, 0.5 * (row_back(wide) + above)),
            jnp.where(even_row, above, 0.5 * (wide + row_next(wide, 2))),
        )
        return tuple(
            NS[part, x] + sides(SM[part, x] + corrections[part], KW[1, x + 1], KW[2, x + 1], 1)
            for part in range(2)
        )

    def after_potential(x, *values):
        for part in range(2):
            NS[part, x] = values[part]

    eliminate(lambda x: (NS[0, x], NS[1, x]), FI, FB, 2)
    substitute(FQ, 2, after_smoothing, 16)
    eliminate(coarse_source, CI, CB, 1, 16)
    substitute(CQ, 1, after_coarse, 16)
    eliminate(lambda x: (CM[0, x],), CI, CB, 1)
    substitute(CQ, 1, after_correction, 16)
    eliminate(corrected_source, FI, FB, 2, 16)
    substitute(FQ, 2, after_potential, 4)

    def from_nodes(l, state):
        for part in range(2):
            p0, p1, p2, p3 = turned([NS[part, 16 * g + l] for g in range(4)])
            Rm[3 * part, l + 1] = p0
            Rm[3 * part + 1, l + 1] = p1
            for d, (g_part, h_part) in (
                (1, (y_next(p0) - p0, 0.5 * (p2 + y_next(p2)))),
                (2, (z_next(p0) - p0, 0.5 * (p3 + z_next(p3)))),
            ):
                E[3 * part + d, l + 1] = (
                    E[3 * part + d, l + 1] + (g_part + h_part) * free[d, l]
                )
        return state

    loop(16, from_nodes, 0, unroll=8)
    for part in range(2):
        pad_high(Rm, 3 * part)
        pad_high(Rm, 3 * part + 1)

    def second_first(l, state):
        for part in range(2):
            p0, p1 = Rm[3 * part, l + 1], Rm[3 * part + 1, l + 1]
            g_part = Rm[3 * part, l + 2] - p0
            h_part = 0.5 * (p1 + Rm[3 * part + 1, l + 2])
            E[3 * part, l + 1] = E[3 * part, l + 1] + (g_part + h_part) * free[0, l]
        return state

    loop(16, second_first, 0, unroll=4)
    for field in range(6):
        pad_low(E, field)
        pad_high(E, field)

    def last_step(l, state):
        after = []
        for part in range(2):
            results, fluxes = curl(part, l + 1, state[part])
            after.append(fluxes)
            for d in range(3):
                field = 3 * part + d
                remainder = W[field, l] - results[d] * free[d, l]
                value = E[field, l + 1] + Dm[d, l] * remainder
                OUT[field, l] = value[TILE : 2 * TILE]
        return tuple(after)

    loop(16, last_step, (side_fluxes(0, 0), side_fluxes(1, 0)), unroll=8)

    def gather_up(a, state):
        slots = [OUT[field, 4 * a + i] for field in range(6) for i in range(4)]
        block = 0
        for start in (0, 16):
            group = jnp.concatenate(slots[start : start + 16], axis=0)
            block = send_group(
                group, lambda p: p // 4 * 4 + a if p % 4 == 1 else None, out, block
            )
        return state

    loop(4, gather_up, 0, unroll=4)


def vmem():
    return pl.BlockSpec(memory_space=pltpu.VMEM)


def smem():
    return pl.BlockSpec(memory_space=pltpu.SMEM)


def pack(residual, classes, edge_mask, class_weight, **options):
    return pl.pallas_call(
        pack_body,
        out_shape=resident(16, 5, HALF, 128),
        in_specs=[vmem(), vmem(), vmem(), smem()],
        out_specs=vmem(),
        name="pack",
        **options,
    )(residual, classes, edge_mask, class_weight)


def unpack(packed, shape, **options):
    return pl.pallas_call(
        unpack_body,
        out_shape=jax.ShapeDtypeStruct(shape, f32),
        in_specs=[vmem()],
        out_specs=vmem(),
        name="unpack",
        **options,
    )(packed)


def resident(*shape):
    return pltpu.VMEM(shape, f32)


def setup(sizes, middle, shallow, deep, **options):
    line = resident(64, ROWS, 128)
    edge = resident(3, 16, ROWS, 128)
    weights = resident(3, 65, ROWS, 128)
    return pl.pallas_call(
        functools.partial(setup_body, sizes),
        out_shape=[edge, edge, edge, weights, weights] + [line] * 6,
        in_specs=[vmem()] * 3,
        out_specs=[vmem()] * 11,
        scratch_shapes=[resident(1, 18, ROWS, 128)],
        name="setup",
        **options,
    )(middle, shallow, deep)


def lines(sizes, middle, shallow, deep, ready, **options):
    edge = lambda count, levels: resident(count, levels, ROWS, 128)
    pair = resident(2, 64, ROWS, 128)
    return pl.pallas_call(
        functools.partial(line_body, sizes),
        out_shape=resident(16, 3, HALF, 128),
        in_specs=[vmem()] * (3 + len(ready)),
        out_specs=vmem(),
        scratch_shapes=[
            edge(6, 16),
            edge(6, 18),
            edge(6, 18),
            pair,
            pair,
            resident(1, 64, ROWS, 128),
            pair,
            resident(1, 64, ROWS, 128),
            resident(6, 16, TILE, 128),
        ],
        name="lines",
        **options,
    )(middle, shallow, deep, *ready)


def swap(values):
    return lax.all_to_all(values, "gx", 0, 0, tiled=True)


def per_device(residual, classes, edge_mask, class_weight):
    size_x, size_y, size_z = (lax.axis_size(name) for name in AXES)
    tiles = size_x * size_z

    def position(y, tile):
        z, x = divmod(tile, size_x)
        if z % 2:
            x = size_x - 1 - x
        return (x * size_y + y) * size_z + z

    def from_side(values, step_y, step_tile):
        pairs = []
        for y in range(size_y):
            for tile in range(tiles):
                next_y = y - step_y if tile // size_x % 2 else y + step_y
                if 0 <= next_y < size_y and 0 <= tile + step_tile < tiles:
                    pairs.append((position(y, tile), position(next_y, tile + step_tile)))
        return lax.ppermute(values, AXES, pairs)

    sizes = (size_x, size_y, size_z)
    own = swap(pack(residual, classes, edge_mask, class_weight))
    middle = jnp.concatenate([from_side(own, 1, 0), own, from_side(own, -1, 0)], axis=0)
    shallow = from_side(middle, 0, 1)
    deep_material = from_side(middle[:, :2], 0, -1)
    deep_source = from_side(middle[:, 2:], 0, -1)
    options = lambda size, cost: dict(
        compiler_params=pltpu.CompilerParams(vmem_limit_bytes=size * 2**20),
        cost_estimate=pl.CostEstimate(flops=cost, bytes_accessed=0, transcendentals=0),
    )
    ready = setup(sizes, middle, shallow, deep_material, **options(20, 2**27))
    result = swap(lines(sizes, middle, shallow, deep_source, ready, **options(32, 2**27)))
    result = pltpu.with_memory_space_constraint(result, pltpu.VMEM)
    return unpack(result, residual.shape)


def solution(mesh):
    return jax.shard_map(
        per_device,
        mesh=mesh,
        in_specs=(
            P("period", None, "gx", "gy", "gz"),
            P("gx", "gy", "gz"),
            P(None, "gx", "gy", "gz"),
            P("period"),
        ),
        out_specs=P("period", None, "gx", "gy", "gz"),
        check_vma=False,
    )
```

```python
import functools

import jax
import jax.numpy as jnp
from jax import lax
from jax.experimental import pallas as pl
from jax.experimental.pallas import tpu as pltpu
from jax.sharding import PartitionSpec as P

aspect = 2.0
face_weight = (1.0 / (aspect * aspect), 1.0, 1.0)
mass_factor = (aspect * aspect, 1.0, 1.0)
stiff_weight = (
    2.0 * (face_weight[1] + face_weight[2]),
    2.0 * (face_weight[0] + face_weight[2]),
    2.0 * (face_weight[0] + face_weight[1]),
)
edge_damping = 0.6
shift_ratio = 0.0001
shift_added = 0.05
coarse_scale = (0.5625, 0.1875, 0.1875)

f32 = jnp.float32
TILE = 8
ROWS = 3 * TILE
GROUPS = 4
DEPTH = 32
HALF = TILE // 2
AXES = ("gx", "gy", "gz")


def lanes(shape):
    return lax.broadcasted_iota(jnp.int32, shape, 1)


def turned(values):
    gap = jnp.zeros((DEPTH - ROWS, 128), f32)
    stacked = jnp.concatenate([piece for value in values for piece in (value, gap)], axis=0).T
    return [stacked[DEPTH * g : DEPTH * g + ROWS] for g in range(4)]


def loop(count, body, carry, unroll=1, reverse=False):
    def step(turn, state):
        for part in range(unroll):
            index = turn * unroll + part
            state = body(count - 1 - index if reverse else index, state)
        return state

    return lax.fori_loop(0, count // unroll, step, carry)


def y_next(v, by=1):
    return pltpu.roll(v, v.shape[0] - by, 0)


def y_back(v, by=1):
    return pltpu.roll(v, by, 0)


def z_next(v, by=1):
    return pltpu.roll(v, 128 - by, 1)


def z_back(v, by=1):
    return pltpu.roll(v, by, 1)


row_next, row_back, lane_next, lane_back = y_next, y_back, z_next, z_back


def position_facts(sizes):
    x, y, z = (lax.axis_index(name) for name in AXES)
    flip = z % 2
    along = x + flip * (sizes[0] - 1 - 2 * x)
    before = jnp.where(along == 0, 1 - flip, flip)
    after = jnp.where(along == sizes[0] - 1, 1 - flip, flip)
    corner_y = y * TILE - TILE
    corner_z = (z * sizes[0] + along) * TILE - TILE
    return corner_y, corner_z, (before, flip, after)


def mirrored(flip, index, count):
    return index + flip * (count - 1 - 2 * index)


def pack_body(residual, classes, edge_mask, class_weight, out):
    thick = classes.shape[0]
    flip = lax.axis_index("gz") % 2
    slots = []
    for i in range(thick):
        labels = classes[i]
        cells = jnp.zeros(labels.shape, f32)
        for label in range(class_weight.shape[0]):
            cells = jnp.where(labels == label, class_weight[label], cells)
        slots.append(cells)
    for comp in range(3):
        slots += [(1 - edge_mask[comp, i]).astype(f32) for i in range(thick)]
    for part in range(2):
        for comp in range(3):
            slots += [residual[part, comp, i] for i in range(thick)]
    block = 0
    for start in range(0, len(slots), 16):
        group = jnp.concatenate(slots[start : start + 16], axis=0)
        block = send_group(group, lambda target: mirrored(flip, target, 16), out, block)


def send_group(group, device, out, block):
    half = HALF
    if group.shape[0] == 128:
        moved = group.T
        parts = 2
    else:
        moved = jnp.concatenate([group, pltpu.roll(group, 128 - half, 1)], axis=0).T
        parts = 1
    for target in range(16):
        where = device(target)
        if where is not None:
            for part in range(parts):
                row = TILE * target + half * part
                out[where, block + part] = moved[row : row + half]
    return block + parts


def receive_group(blocks, block, full):
    half = HALF
    gap = jnp.zeros((half, 128), f32)
    rows = []
    for source in range(16):
        rows.append(blocks(source, block))
        rows.append(blocks(source, block + 1) if full else gap)
    moved = jnp.concatenate(rows, axis=0).T
    if full:
        return moved
    upper = pltpu.roll(moved[64:], half, 1)
    return jnp.where(lanes((64, 128)) % TILE < half, moved[:64], upper)


def unpack_body(packed, out):
    flip = lax.axis_index("gz") % 2
    for part in range(2):
        moved = receive_group(
            lambda window, block: packed[mirrored(flip, window, 16), block], 2 * part, part == 0
        )
        for slot in range(moved.shape[0] // TILE):
            field, i = divmod(16 * part + slot, 4)
            out[field // 3, field % 3, i] = moved[TILE * slot : TILE * slot + TILE]


def pad_low(ref, field):
    lane = lanes((ROWS, 128))
    ref[field, 0] = jnp.where(lane < DEPTH, 0.0, pltpu.roll(ref[field, 16], DEPTH, 1))


def pad_high(ref, field):
    lane = lanes((ROWS, 128))
    ref[field, 17] = jnp.where(
        lane >= 128 - DEPTH, 0.0, pltpu.roll(ref[field, 1], 128 - DEPTH, 1)
    )


def spread_out(windows, groups, put):
    gap = jnp.zeros((HALF, 128), f32)

    def step(a, state):
        for y in range(3):
            for part, full in enumerate(groups):

                def blocks(p, block):
                    g, t = divmod(p, 4)
                    if t == 3:
                        return gap
                    ref, first, flag = windows[t]
                    turn = y + flag * (2 - 2 * y)
                    return ref[turn * 16 + 4 * g + a, first + block]

                moved = receive_group(blocks, 2 * part, full)
                for slot in range(moved.shape[0] // TILE):
                    field, i = divmod(16 * part + slot, 4)
                    put(field, 4 * a + i, y, moved[TILE * slot : TILE * slot + TILE])
        return state

    loop(4, step, 0, unroll=4)


def setup_body(
    sizes,
    middle,
    shallow,
    deep,
    free_out,
    M,
    Dm,
    KW,
    CW,
    FI,
    FB,
    FQ,
    CI,
    CB,
    CQ,
    cells,
):
    corner_y, corner_z, orders = position_facts(sizes)
    extent_y, extent_z = sizes[1] * TILE, sizes[0] * sizes[2] * TILE
    shape = (ROWS, 128)
    lane = lanes(shape)
    row = lax.broadcasted_iota(jnp.int32, shape, 0)
    at_y = lane % DEPTH + corner_y
    at_z = row + corner_z
    inside = jnp.where(
        (at_y >= 0) & (at_y < extent_y) & (at_z >= 0) & (at_z < extent_z), 1.0, 0.0
    ).astype(f32)
    coarse_inside = jnp.where(row % 2 == 0, inside, row_back(inside))
    even_row = row % 2 == 0

    def put(field, level, y, values):
        if field == 0:
            cells[0, level + 1, TILE * y : TILE * y + TILE, :] = values
        else:
            free_out[field - 1, level, TILE * y : TILE * y + TILE, :] = values

    spread_out(
        ((shallow, 0, orders[0]), (middle, 0, orders[1]), (deep, 0, orders[2])), (True,), put
    )
    pad_low(cells, 0)

    def coefficients(l, state):
        c = cells[0, l + 1]
        cx = cells[0, l]
        cy = y_back(c)
        cz = z_back(c)
        averages = (
            0.25 * (((c + cy) + cz) + z_back(cy)),
            0.25 * (((c + cx) + cz) + z_back(cx)),
            0.25 * (((c + cx) + cy) + y_back(cx)),
        )
        for d in range(3):
            free = free_out[d, l]
            masses = mass_factor[d] * averages[d] * free
            diagonal = stiff_weight[d] + masses
            M[d, l] = masses
            Dm[d, l] = edge_damping * free / diagonal
            stiff = diagonal * free
            for g, values in enumerate(turned([masses, stiff, stiff, stiff])):
                KW[d, 16 * g + l + 1] = values
        return state

    loop(16, coefficients, 0, unroll=8)

    for d in range(3):
        KW[d, 0] = jnp.zeros(shape, f32)

    nothing = jnp.zeros(shape, f32)
    CW[0, 0] = nothing

    def diagonals(x, state):
        w1b, w1, w2, w3 = KW[0, x], KW[0, x + 1], KW[1, x + 1], KW[2, x + 1]
        total = ((((w1 + w1b) + w3) + row_back(w3)) + w2) + lane_back(w2)
        FI[x] = (1.0 + shift_ratio) * total + shift_added
        for d, w in enumerate((w1, w2, w3)):
            pair = w + row_next(w)
            pair = jnp.where(even_row, pair, row_back(pair))
            CW[d, x + 1] = coarse_scale[d] * (pair + lane_next(pair))
        return state

    def coarse_diagonals(x, state):
        w1b, w1, w2, w3 = CW[0, x], CW[0, x + 1], CW[1, x + 1], CW[2, x + 1]
        total = ((((w1 + w1b) + w3) + row_back(w3, 2)) + w2) + lane_back(w2, 2)
        CI[x] = (1.0 + shift_ratio) * total + shift_added
        return state

    loop(64, diagonals, 0, unroll=16)
    loop(64, coarse_diagonals, 0, unroll=16)

    def factors(x, state):
        fine_before, coarse_before = state
        w1b, c1b = KW[0, x], CW[0, x]
        inverse = inside / (FI[x] - w1b * fine_before)
        coarse_inverse = coarse_inside / (CI[x] - c1b * coarse_before)
        FI[x] = inverse
        CI[x] = coarse_inverse
        FB[x] = w1b * inverse
        CB[x] = c1b * coarse_inverse
        quotient = KW[0, x + 1] * inverse
        coarse_quotient = CW[0, x + 1] * coarse_inverse
        FQ[x] = quotient
        CQ[x] = coarse_quotient
        return quotient, coarse_quotient

    loop(64, factors, (nothing, nothing), unroll=2)


def line_body(
    sizes,
    middle,
    shallow,
    deep,
    free,
    M,
    Dm,
    KW,
    CW,
    FI,
    FB,
    FQ,
    CI,
    CB,
    CQ,
    out,
    W,
    E,
    Rm,
    NS,
    SM,
    CS,
    TY,
    CM,
    OUT,
):
    shape = (ROWS, 128)
    orders = position_facts(sizes)[2]
    even_row = lax.broadcasted_iota(jnp.int32, shape, 0) % 2 == 0
    even_lane = lanes(shape) % 2 == 0
    nothing = jnp.zeros(shape, f32)
    def put(field, level, y, values):
        rows = slice(TILE * y, TILE * y + TILE)
        source = values * free[field % 3, level, rows, :]
        W[field, level, rows, :] = source
        E[field, level + 1, rows, :] = source * Dm[field % 3, level, rows, :]

    spread_out(
        ((shallow, 2, orders[0]), (middle, 2, orders[1]), (deep, 2, orders[2])),
        (True, False),
        put,
    )

    def side_fluxes(part, l):
        e1, e2, e3 = (E[3 * part + d, l] for d in range(3))
        b2 = face_weight[1] * ((z_next(e1) - e1) - (E[3 * part + 2, l + 1] - e3))
        b3 = face_weight[2] * ((E[3 * part + 1, l + 1] - e2) - (y_next(e1) - e1))
        return b2, b3

    def curl(part, l, before):
        e1, e2, e3 = (E[3 * part + d, l] for d in range(3))
        b2, b3 = side_fluxes(part, l)
        b1 = face_weight[0] * ((y_next(e3) - e3) - (z_next(e2) - e2))
        b2_before, b3_before = before
        results = (
            (z_back(b2) - b2) - (y_back(b3) - b3) + M[0, l - 1] * e1,
            (b3_before - b3) - (z_back(b1) - b1) + M[1, l - 1] * e2,
            (y_back(b1) - b1) - (b2_before - b2) + M[2, l - 1] * e3,
        )
        return results, (b2, b3)

    for field in range(6):
        pad_low(E, field)
        pad_high(E, field)

    def first_remainder(l, state):
        after = []
        for part in range(2):
            results, fluxes = curl(part, l + 1, state[part])
            after.append(fluxes)
            for d in range(3):
                Rm[3 * part + d, l + 1] = (
                    W[3 * part + d, l] - results[d] * free[d, l]
                )
        return tuple(after)

    loop(16, first_remainder, (side_fluxes(0, 0), side_fluxes(1, 0)), unroll=4)
    pad_low(Rm, 0)
    pad_low(Rm, 3)

    def to_nodes(l, state):
        for part in range(2):
            r1, r2, r3 = (Rm[3 * part + d, l + 1] for d in range(3))
            r1b = Rm[3 * part, l]
            r2b = y_back(r2)
            r3b = z_back(r3)
            members = [
                ((r1b - r1) + (r2b - r2)) + (r3b - r3),
                0.5 * (r1 + r1b),
                0.5 * (r2 + r2b),
                0.5 * (r3 + r3b),
            ]
            for g, values in enumerate(turned(members)):
                NS[part, 16 * g + l] = values
        return state

    loop(16, to_nodes, 0, unroll=16)

    def eliminate(source, inverse, back, parts, unroll=4):
        def step(x, state):
            scale, couple = inverse[x], back[x]
            sources = source(x)
            after = []
            for part in range(parts):
                value = sources[part] * scale + couple * state[part]
                TY[part, x] = value
                after.append(value)
            return tuple(after)

        loop(64, step, (nothing,) * parts, unroll=unroll)

    def substitute(quotient, parts, then, unroll):
        def step(x, state):
            factor = quotient[x]
            after = tuple(TY[part, x] + factor * state[part] for part in range(parts))
            then(x, *after)
            return after

        loop(64, step, (nothing,) * parts, unroll=unroll, reverse=True)

    def sides(v, w2, w3, by):
        return ((w3 * row_next(v, by) + row_back(w3 * v, by)) + w2 * lane_next(v, by)) + lane_back(
            w2 * v, by
        )

    def after_smoothing(x, *values):
        halved = []
        for part, value in enumerate(values):
            SM[part, x] = value
            residue = sides(value, KW[1, x + 1], KW[2, x + 1], 1)
            halved.append(residue + 0.5 * (row_back(residue) + row_next(residue)))
        CM[0, x] = jnp.where(even_row, halved[0], row_back(halved[1]))

    def coarse_source(x):
        merged = CM[0, x]
        value = merged + 0.5 * (lane_back(merged) + lane_next(merged))
        CS[0, x] = value
        return (value,)

    def after_coarse(x, value):
        CM[0, x] = CS[0, x] + sides(value, CW[1, x + 1], CW[2, x + 1], 2)

    def after_correction(x, value):
        CS[0, x] = jnp.where(even_lane, value, 0.5 * (lane_back(value) + lane_next(value)))

    def corrected_source(x):
        wide = CS[0, x]
        above = row_next(wide)
        corrections = (
            jnp.where(even_row, wide, 0.5 * (row_back(wide) + above)),
            jnp.where(even_row, above, 0.5 * (wide + row_next(wide, 2))),
        )
        return tuple(
            NS[part, x] + sides(SM[part, x] + corrections[part], KW[1, x + 1], KW[2, x + 1], 1)
            for part in range(2)
        )

    def after_potential(x, *values):
        for part in range(2):
            NS[part, x] = values[part]

    eliminate(lambda x: (NS[0, x], NS[1, x]), FI, FB, 2)
    substitute(FQ, 2, after_smoothing, 16)
    eliminate(coarse_source, CI, CB, 1, 16)
    substitute(CQ, 1, after_coarse, 16)
    eliminate(lambda x: (CM[0, x],), CI, CB, 1)
    substitute(CQ, 1, after_correction, 16)
    eliminate(corrected_source, FI, FB, 2, 16)
    substitute(FQ, 2, after_potential, 4)

    def from_nodes(l, state):
        for part in range(2):
            p0, p1, p2, p3 = turned([NS[part, 16 * g + l] for g in range(4)])
            Rm[3 * part, l + 1] = p0
            Rm[3 * part + 1, l + 1] = p1
            for d, (g_part, h_part) in (
                (1, (y_next(p0) - p0, 0.5 * (p2 + y_next(p2)))),
                (2, (z_next(p0) - p0, 0.5 * (p3 + z_next(p3)))),
            ):
                E[3 * part + d, l + 1] = (
                    E[3 * part + d, l + 1] + (g_part + h_part) * free[d, l]
                )
        return state

    loop(16, from_nodes, 0, unroll=16)
    for part in range(2):
        pad_high(Rm, 3 * part)
        pad_high(Rm, 3 * part + 1)

    def second_first(l, state):
        for part in range(2):
            p0, p1 = Rm[3 * part, l + 1], Rm[3 * part + 1, l + 1]
            g_part = Rm[3 * part, l + 2] - p0
            h_part = 0.5 * (p1 + Rm[3 * part + 1, l + 2])
            E[3 * part, l + 1] = E[3 * part, l + 1] + (g_part + h_part) * free[0, l]
        return state

    loop(16, second_first, 0, unroll=4)
    for field in range(6):
        pad_low(E, field)
        pad_high(E, field)

    def last_step(l, state):
        after = []
        for part in range(2):
            results, fluxes = curl(part, l + 1, state[part])
            after.append(fluxes)
            for d in range(3):
                field = 3 * part + d
                remainder = W[field, l] - results[d] * free[d, l]
                value = E[field, l + 1] + Dm[d, l] * remainder
                OUT[field, l] = value[TILE : 2 * TILE]
        return tuple(after)

    loop(16, last_step, (side_fluxes(0, 0), side_fluxes(1, 0)), unroll=8)

    def gather_up(a, state):
        slots = [OUT[field, 4 * a + i] for field in range(6) for i in range(4)]
        block = 0
        for start in (0, 16):
            group = jnp.concatenate(slots[start : start + 16], axis=0)
            block = send_group(
                group, lambda p: p // 4 * 4 + a if p % 4 == 1 else None, out, block
            )
        return state

    loop(4, gather_up, 0, unroll=4)


def vmem():
    return pl.BlockSpec(memory_space=pltpu.VMEM)


def smem():
    return pl.BlockSpec(memory_space=pltpu.SMEM)


def pack(residual, classes, edge_mask, class_weight, **options):
    return pl.pallas_call(
        pack_body,
        out_shape=resident(16, 5, HALF, 128),
        in_specs=[vmem(), vmem(), vmem(), smem()],
        out_specs=vmem(),
        name="pack",
        **options,
    )(residual, classes, edge_mask, class_weight)


def unpack(packed, shape, **options):
    return pl.pallas_call(
        unpack_body,
        out_shape=jax.ShapeDtypeStruct(shape, f32),
        in_specs=[vmem()],
        out_specs=vmem(),
        name="unpack",
        **options,
    )(packed)


def resident(*shape):
    return pltpu.VMEM(shape, f32)


def setup(sizes, middle, shallow, deep, **options):
    line = resident(64, ROWS, 128)
    edge = resident(3, 16, ROWS, 128)
    weights = resident(3, 65, ROWS, 128)
    return pl.pallas_call(
        functools.partial(setup_body, sizes),
        out_shape=[edge, edge, edge, weights, weights] + [line] * 6,
        in_specs=[vmem()] * 3,
        out_specs=[vmem()] * 11,
        scratch_shapes=[resident(1, 18, ROWS, 128)],
        name="setup",
        **options,
    )(middle, shallow, deep)


def lines(sizes, middle, shallow, deep, ready, **options):
    edge = lambda count, levels: resident(count, levels, ROWS, 128)
    pair = resident(2, 64, ROWS, 128)
    return pl.pallas_call(
        functools.partial(line_body, sizes),
        out_shape=resident(16, 3, HALF, 128),
        in_specs=[vmem()] * (3 + len(ready)),
        out_specs=vmem(),
        scratch_shapes=[
            edge(6, 16),
            edge(6, 18),
            edge(6, 18),
            pair,
            pair,
            resident(1, 64, ROWS, 128),
            pair,
            resident(1, 64, ROWS, 128),
            resident(6, 16, TILE, 128),
        ],
        name="lines",
        **options,
    )(middle, shallow, deep, *ready)


def swap(values):
    return lax.all_to_all(values, "gx", 0, 0, tiled=True)


def per_device(residual, classes, edge_mask, class_weight):
    size_x, size_y, size_z = (lax.axis_size(name) for name in AXES)
    tiles = size_x * size_z

    def position(y, tile):
        z, x = divmod(tile, size_x)
        if z % 2:
            x = size_x - 1 - x
        return (x * size_y + y) * size_z + z

    def from_side(values, step_y, step_tile):
        pairs = []
        for y in range(size_y):
            for tile in range(tiles):
                next_y = y - step_y if tile // size_x % 2 else y + step_y
                if 0 <= next_y < size_y and 0 <= tile + step_tile < tiles:
                    pairs.append((position(y, tile), position(next_y, tile + step_tile)))
        return lax.ppermute(values, AXES, pairs)

    sizes = (size_x, size_y, size_z)
    own = swap(pack(residual, classes, edge_mask, class_weight))
    middle = jnp.concatenate([from_side(own, 1, 0), own, from_side(own, -1, 0)], axis=0)
    shallow, deep = from_side(middle, 0, 1), from_side(middle, 0, -1)
    options = lambda size, cost: dict(
        compiler_params=pltpu.CompilerParams(vmem_limit_bytes=size * 2**20),
        cost_estimate=pl.CostEstimate(flops=cost, bytes_accessed=0, transcendentals=0),
    )
    ready = setup(sizes, middle, shallow, deep, **options(20, 2**27))
    result = swap(lines(sizes, middle, shallow, deep, ready, **options(32, 2**27)))
    result = pltpu.with_memory_space_constraint(result, pltpu.VMEM)
    return unpack(result, residual.shape)


def solution(mesh):
    return jax.shard_map(
        per_device,
        mesh=mesh,
        in_specs=(
            P("period", None, "gx", "gy", "gz"),
            P("gx", "gy", "gz"),
            P(None, "gx", "gy", "gz"),
            P("period"),
        ),
        out_specs=P("period", None, "gx", "gy", "gz"),
        check_vma=False,
    )
```
